128 devices in a mesh: dom: 128 (over y, z, x, core).
Axes of the slice: x: 4, y: 4, z: 4, core: 2. Of those that a mesh axis runs over, the one named last changes fastest.
Arguments:
- concentration: float32 [4096, 128], P('dom'), may hold values from 0 to 1
- reaction_rate: float32 [4096, 128], P('dom'), may hold values from 0.5 to 4
- step_size: float32 [1], replicated, may hold values from 1 to 2
- block_values: float32 [4096, 5, 128, 128], P('dom'), may hold values from -40 to 48, as said below
- block_columns: int32 [4096, 5], P('dom'), may hold values from 0 to 95, as said below
- row_lengths: int32 [4096], P('dom'), may hold values from 2 to 5, as said below
- send_lists: int32 [128, 4, 16], P('dom'), may hold values from 0 to 31, as said below
Outputs:
- next_concentration: float32 [4096, 128], P('dom')
The draws below stay inside these ranges and needn't reach their ends.
Inputs may be any that keep to these rules, and one draw needn't show every extreme that they name: `send_lists`: for every partition and offset index q (offsets -2, -1, +1, +2), 16 distinct local block indices. `block_columns`: slot 0 of a block row is the row's own local block; live slots name a local block (below 32) or a ghost slot 32 + q * 16 + g of a block that the partition at offset index q sends; slot 1 of local block row q, for q = 0..3, is a ghost slot of offset index q; slots at or past the row's length repeat the row's own local block. `row_lengths`: some block row has all 5 slots live. `block_values`: slot 0 of every block row holds 8 times the identity plus a full random block; the other slots hold full random blocks.
All inputs are finite; a program needn't handle non-finite values.
Results may differ from the reference program's by a relative error of at most 0.00016.
Values sent between devices are 32-bit elements; how exact they have to be, the bound alone decides.
A program may use at most 64 MiB of HBM per device.

```python
import math
import jax
import jax.numpy as jnp
from jax import lax

BLK = 128
BDEV = 32
NNZB = 5
GMAX = 16
KRYLOV = 3
RESTARTS = 2
NDEV = 128
NB = 4096


def ghost_counts(key):
    first_key, second_key = jax.random.split(jax.random.fold_in(key, 11))
    counts = jax.random.randint(first_key, (NDEV, 4), max(GMAX // 4, 1), GMAX + 1)
    fullest = jax.random.randint(second_key, (4,), 0, NDEV)
    devices = jnp.arange(NDEV)[:, None]
    return jnp.where(devices == fullest[None, :], GMAX, counts).astype(jnp.int32)


def lengths_drawn(key):
    first_key, second_key = jax.random.split(jax.random.fold_in(key, 23))
    lengths = jax.random.randint(first_key, (NB,), 2, NNZB + 1)
    longest = jax.random.randint(second_key, (), 0, NB)
    return jnp.where(jnp.arange(NB) == longest, NNZB, lengths).astype(jnp.int32)


def draw_row_lengths(key, part):
    return lengths_drawn(key)


def draw_send_lists(key, part):
    scores = jax.random.randint(jax.random.fold_in(key, 37), (NDEV, 4, BDEV), 0, 1 << 20) * BDEV + jnp.arange(BDEV)
    ordering = jnp.argsort(scores, axis=-1)
    return ordering[:, :, :GMAX].astype(jnp.int32)


def draw_block_columns(key, part):
    counts = ghost_counts(key)
    lengths = lengths_drawn(key)
    subkeys = jax.random.split(jax.random.fold_in(key, 53), 4)
    row_ids = jnp.arange(NB)
    device = row_ids // BDEV
    local_row = row_ids % BDEV
    positions = jnp.arange(NNZB)[None, :]
    forced = (positions == 1) & (local_row[:, None] < 4)
    variety = jax.random.randint(subkeys[0], (NB, NNZB), 0, 2)
    variety = jnp.where(forced, 1, variety)
    owned = jax.random.randint(subkeys[1], (NB, NNZB), 0, BDEV)
    within = jax.random.randint(subkeys[2], (NB, NNZB), 0, 4)
    within = jnp.where(forced, jnp.broadcast_to((local_row % 4)[:, None], (NB, NNZB)), within)
    drawn_bits = jax.random.randint(subkeys[3], (NB, NNZB), 0, 1 << 20)
    offsets = jnp.array([-2, -1, 1, 2])
    sender = (device[:, None] - offsets[within]) % NDEV
    ghost_slot = drawn_bits % counts[sender, within]
    ghost = BDEV + within * GMAX + ghost_slot
    picked = jnp.where(variety == 1, ghost, owned)
    picked = jnp.where(positions == 0, local_row[:, None], picked)
    picked = jnp.where(positions < lengths[:, None], picked, local_row[:, None])
    return picked.astype(jnp.int32)


def draw_block_values(key, part):
    first_key = jax.random.fold_in(jax.random.fold_in(key, 71), 0)
    spread = 4.0 / math.sqrt(BLK * NNZB)
    shape = (NB, NNZB, BLK, BLK)
    entries = jax.random.normal(first_key, shape, jnp.float32)
    diagonal = (jnp.arange(NNZB) == 0).astype(jnp.float32)[None, :, None, None] * jnp.eye(BLK, dtype=jnp.float32)[None, None] * 8.0
    return (entries * spread + diagonal).astype(jnp.float32)


def block_scale(own_key, extent, shards, low, high):
    loudness = 1.0
    for dim, blocks in shards:
        draws = jax.random.uniform(jax.random.fold_in(jax.random.fold_in(own_key, 6), dim), (blocks,), jnp.float32, low / len(shards), high / len(shards))
        loudness = loudness * jnp.repeat(jnp.exp(draws), extent[dim] // blocks).reshape((-1,) + (1,) * (len(extent) - 1 - dim))
    return loudness


def setup_inputs(seed: int = 0) -> dict:
    key_of = jax.random.split(jax.random.key(seed), 8)
    return {
        "concentration": jnp.clip(1.0 * jax.random.uniform(key_of[0], (NB, BLK), jnp.float32) ** block_scale(key_of[0], (NB, BLK), ((0, 128),), -0.2, 0.2), 0.0, 1.0),
        "reaction_rate": jnp.clip(jnp.exp(math.log(4.0) - 2.0794415 * jax.random.uniform(key_of[1], (NB, BLK), jnp.float32) ** block_scale(key_of[1], (NB, BLK), ((0, 128),), -0.2, 0.2)), 0.5, 4.0),
        "step_size": jnp.clip(jax.random.uniform(key_of[2], (1,), jnp.float32, 1.0, 2.0), 1.0, 2.0),
        "block_values": draw_block_values(jax.random.fold_in(key_of[7], 71), 0),
        "block_columns": draw_block_columns(jax.random.fold_in(key_of[7], 71), 0),
        "row_lengths": draw_row_lengths(jax.random.fold_in(key_of[7], 71), 0),
        "send_lists": draw_send_lists(jax.random.fold_in(key_of[7], 71), 0),
    }


epsilon = 1e-06
OFFSETS = (-2, -1, 1, 2)

def column_map(block_columns, send_lists):
    device = (jnp.arange(NB, dtype=jnp.int32) // BDEV)[:, None]
    ghost_index = jnp.maximum(block_columns - BDEV, 0)
    neighbour = ghost_index // GMAX
    ghost_slot = ghost_index % GMAX
    offsets = jnp.array(OFFSETS, jnp.int32)
    sender = (device - offsets[neighbour]) % NDEV
    remote = send_lists[sender, neighbour, ghost_slot]
    owned = device * BDEV + block_columns
    return jnp.where(block_columns < BDEV, owned, sender * BDEV + remote).astype(jnp.int32)

def product(block_values, columns, active, field):
    gathered = field[columns] * active[:, :, None]
    return jnp.einsum('bsij,bsj->bi', block_values, gathered, precision=lax.Precision.HIGHEST)

def phi_column(hessenberg, substep):
    order = hessenberg.shape[0]
    augmented = jnp.zeros((order + 1, order + 1), jnp.float32)
    augmented = augmented.at[:order, :order].set(substep * hessenberg).at[0, order].set(1.0)
    reduced = augmented / 64.0
    identity = jnp.eye(order + 1, dtype=jnp.float32)
    series = identity
    for degree in range(12, 0, -1):
        series = identity + jnp.dot(reduced, series, precision=lax.Precision.HIGHEST) / degree
    for square_turn in range(6):
        series = jnp.dot(series, series, precision=lax.Precision.HIGHEST)
    return series[:order, order]

def krylov(start, apply):
    magnitude = jnp.sqrt(jnp.sum(start * start) + epsilon)
    vectors = jnp.zeros((KRYLOV,) + start.shape, jnp.float32).at[0].set(start / magnitude)
    hessenberg = jnp.zeros((KRYLOV, KRYLOV), jnp.float32)
    for column in range(KRYLOV):
        mapped = apply(vectors[column])
        projection = jnp.einsum('kbi,bi->k', vectors, mapped, precision=lax.Precision.HIGHEST)
        mapped = mapped - jnp.einsum('k,kbi->bi', projection, vectors, precision=lax.Precision.HIGHEST)
        hessenberg = hessenberg.at[:, column].set(projection)
        if column + 1 < KRYLOV:
            length = jnp.sqrt(jnp.sum(mapped * mapped) + epsilon)
            hessenberg = hessenberg.at[column + 1, column].set(length)
            vectors = vectors.at[column + 1].set(mapped / length)
    return (magnitude, vectors, hessenberg)

def reference(concentration, reaction_rate, step_size, block_values, block_columns, row_lengths, send_lists):
    columns = column_map(block_columns, send_lists)
    active = (jnp.arange(NNZB, dtype=jnp.int32)[None, :] < row_lengths[:, None]).astype(jnp.float32)
    slope = reaction_rate * (1.0 - 2.0 * concentration)

    def apply(field):
        return slope * field - product(block_values, columns, active, field)
    forcing = reaction_rate * concentration * (1.0 - concentration) - product(block_values, columns, active, concentration)
    substep = step_size[0] / RESTARTS
    increment = jnp.zeros_like(concentration)
    for restart in range(RESTARTS):
        start = forcing if restart == 0 else apply(increment) + forcing
        magnitude, vectors, hessenberg = krylov(start, apply)
        weights = phi_column(hessenberg, substep)
        increment = increment + substep * magnitude * jnp.einsum('k,kbi->bi', weights, vectors, precision=lax.Precision.HIGHEST)
    return concentration + increment
```

```python
import jax
import jax.numpy as jnp
from jax import lax
from jax.experimental import pallas as pl
from jax.experimental.pallas import tpu as pltpu
from jax.sharding import PartitionSpec as P

BLK = 128
BDEV = 32
NNZB = 5
GMAX = 16
OFFSETS = (-2, -1, 1, 2)
ORDER = (0, 3, 1, 2)
EPS = 1e-6
SHIFT = 8.0
SCALE = 0.25
ROUNDS = 7
GROUP = 8
CHUNK = 4
ZERO_ROW = BDEV + 4 * GMAX
XROWS = ZERO_ROW + 8
PAIRS = ((0, 0), (0, 1), (0, 2), (1, 1), (1, 2), (2, 2), (0, 3), (1, 3), (2, 3))
MESH = pl.DeviceIdType.MESH


def arnoldi_weights(gram, substep):
    G = {}
    for (i, j), g in gram.items():
        G[i, j] = g
        G[j, i] = g
    zero = jnp.zeros_like(substep)
    magnitude = jnp.sqrt(G[0, 0] + EPS)
    vectors = [[1.0 / magnitude]]
    H = [[None] * 3 for _ in range(3)]
    for col in range(3):
        v = vectors[col]
        n = len(v)
        mapped = [None] * (n + 1)
        for k in range(n + 1):
            term = None
            if k > 0:
                term = v[k - 1] * (1.0 / SCALE)
            if k < n:
                low = v[k] * SHIFT
                term = -low if term is None else term - low
            mapped[k] = term
        image = []
        for i in range(n):
            total = G[i, 0] * mapped[0]
            for k in range(1, n + 1):
                total = total + G[i, k] * mapped[k]
            image.append(total)
        projections = []
        for vec in vectors:
            total = vec[0] * image[0]
            for k in range(1, len(vec)):
                total = total + vec[k] * image[k]
            projections.append(total)
        for k, p in enumerate(projections):
            H[k][col] = p
        if col < 2:
            rest = list(mapped)
            for p, vec in zip(projections, vectors):
                for k in range(len(vec)):
                    rest[k] = rest[k] - p * vec[k]
            square = None
            for i in range(n + 1):
                total = G[i, 0] * rest[0]
                for k in range(1, n + 1):
                    total = total + G[i, k] * rest[k]
                total = total * rest[i]
                square = total if square is None else square + total
            length = jnp.sqrt(square + EPS)
            H[col + 1][col] = length
            inverse = 1.0 / length
            vectors.append([r * inverse for r in rest])
    small = substep * (1.0 / 64.0)
    A = [[None if H[i][j] is None else H[i][j] * small for j in range(3)] for i in range(3)]
    one = jnp.ones_like(substep)
    Pm = [[one if i == j else zero for j in range(3)] for i in range(3)]
    q = [zero] * 3
    for degree in range(12, 0, -1):
        inv = 1.0 / degree
        newP = [[None] * 3 for _ in range(3)]
        newq = [None] * 3
        for i in range(3):
            ks = [k for k in range(3) if A[i][k] is not None]
            for j in range(3):
                total = A[i][ks[0]] * Pm[ks[0]][j]
                for k in ks[1:]:
                    total = total + A[i][k] * Pm[k][j]
                total = total * inv
                newP[i][j] = total + 1.0 if i == j else total
            total = A[i][ks[0]] * q[ks[0]]
            for k in ks[1:]:
                total = total + A[i][k] * q[k]
            if i == 0:
                total = total + (1.0 / 64.0)
            newq[i] = total * inv
        Pm, q = newP, newq
    for _ in range(6):
        newP = [[Pm[i][0] * Pm[0][j] + Pm[i][1] * Pm[1][j] + Pm[i][2] * Pm[2][j] for j in range(3)] for i in range(3)]
        q = [Pm[i][0] * q[0] + Pm[i][1] * q[1] + Pm[i][2] * q[2] + q[i] for i in range(3)]
        Pm = newP
    out = []
    for k in range(3):
        total = None
        for col in range(k, 3):
            term = q[col] * vectors[col][k]
            total = term if total is None else total + term
        out.append(total * (substep * magnitude))
    return out


def kernel(ndev, conc_hbm, rate_hbm, step_hbm, blocks_hbm, cols_hbm, lens_hbm, lists_hbm, out_hbm, *scratch):
    (conc, rate, slope8, blocks, ys, sends, gram_row, arrivals, result, step_s, cols_s, lens_s, lists_s, index_s) = scratch[:14]
    xs = scratch[14 : 14 + ROUNDS]
    in_sems, block_sems, send_sems, recv_sems, ar_send, ar_recv, out_sem = scratch[14 + ROUNDS :]
    me = lax.axis_index("dom")

    small = [
        pltpu.make_async_copy(lists_hbm, lists_s, in_sems.at[0]),
        pltpu.make_async_copy(conc_hbm, conc, in_sems.at[1]),
        pltpu.make_async_copy(cols_hbm, cols_s, in_sems.at[2]),
        pltpu.make_async_copy(lens_hbm, lens_s, in_sems.at[3]),
        pltpu.make_async_copy(rate_hbm, rate, in_sems.at[4]),
        pltpu.make_async_copy(step_hbm, step_s, in_sems.at[5]),
    ]
    for copy in small:
        copy.start()
    chunks = []
    for c in range(BDEV // CHUNK):
        part = pl.ds(c * CHUNK, CHUNK)
        chunks.append(pltpu.make_async_copy(blocks_hbm.at[part], blocks.at[part], block_sems.at[c]))
        chunks[-1].start()

    barrier = pltpu.get_barrier_semaphore()

    def greet(k, carry):
        pl.semaphore_signal(barrier, inc=1, device_id=(lax.rem(me + k, ndev),), device_id_type=MESH)
        return carry

    lax.fori_loop(1, ndev, greet, 0)

    for x in xs:
        x[pl.ds(ZERO_ROW, 8), :] = jnp.zeros((8, BLK), jnp.float32)
    for copy in small:
        copy.wait()

    def remap(b, carry):
        length = lens_s[b]
        for t in range(NNZB):
            index_s[b * NNZB + t] = jnp.where(t < length, cols_s[b, t], ZERO_ROW)
        return carry

    lax.fori_loop(0, BDEV, remap, 0)

    def packet(r, q):
        o = OFFSETS[q]
        return pltpu.make_async_remote_copy(
            src_ref=sends.at[r, q],
            dst_ref=xs[r].at[pl.ds(BDEV + q * GMAX, GMAX), :],
            send_sem=send_sems.at[r, q],
            recv_sem=recv_sems.at[r, q],
            device_id=(lax.rem(me + (o + ndev), ndev),),
            device_id_type=MESH,
        )

    def pack(r, source):
        for q in ORDER:
            for g in range(GMAX):
                sends[r, q, pl.ds(g, 1), :] = source[pl.ds(lists_s[0, q, g], 1), :]
            if r > 0:
                packet(r, q).start()

    def await_ghosts(r):
        for q in ORDER:
            packet(r, q).wait_recv()

    def product(r, finish):
        x = xs[r]

        def group(i, carry):
            for s in range(GROUP):
                b = i * GROUP + s
                total = None
                for t in range(NNZB):
                    row = x[pl.ds(index_s[b * NNZB + t], 8, stride=0), :]
                    term = blocks[b, t].reshape(16, 8, BLK) * row[None]
                    total = term if total is None else total + term
                flipped = total.reshape(BLK, BLK).T
                finish(b, jnp.sum(flipped, axis=0, keepdims=True))
            return carry

        if r == 0:
            for i in range(BDEV // GROUP):
                for c in range(i * GROUP // CHUNK, (i + 1) * GROUP // CHUNK):
                    chunks[c].wait()
                group(i, 0)
        else:
            lax.fori_loop(0, BDEV // GROUP, group, 0)

    pack(0, conc)
    xs[0][pl.ds(0, BDEV), :] = conc[...]
    slope8[...] = rate[...] * (1.0 - 2.0 * conc[...]) + SHIFT
    pl.semaphore_wait(barrier, ndev - 1)
    for q in ORDER:
        packet(0, q).start()
    await_ghosts(0)

    def first(b, row):
        c = conc[pl.ds(b, 1), :]
        ys[0, pl.ds(b, 1), :] = rate[pl.ds(b, 1), :] * c * (1.0 - c) - row

    product(0, first)

    def broadcast_gram(slot, products):
        rows = [jnp.sum(p, axis=0, keepdims=True) for p in products]
        rows = rows + [jnp.zeros((BLK - len(rows), BLK), jnp.float32)]
        gram_row[slot] = jnp.sum(jnp.concatenate(rows, axis=0).T, axis=0, keepdims=True)

        def send(k, carry):
            pltpu.make_async_remote_copy(
                src_ref=gram_row.at[slot],
                dst_ref=arrivals.at[slot, me],
                send_sem=ar_send.at[slot],
                recv_sem=ar_recv.at[slot],
                device_id=(lax.rem(me + k, ndev),),
                device_id_type=MESH,
            ).start()
            return carry

        lax.fori_loop(1, ndev, send, 0)

    def collect_gram(slot):
        whole = arrivals.at[slot, pl.ds(0, ndev - 1)]
        pltpu.make_async_copy(whole, whole, ar_recv.at[slot]).wait()
        arrivals[slot, me] = gram_row[slot]
        total = jnp.sum(arrivals[slot], axis=0)
        return {
            pair: jnp.broadcast_to(total[:, e : e + 1], (1, BLK)) for e, pair in enumerate(PAIRS)
        }

    substep = jnp.full((1, BLK), step_s[0] * 0.5, jnp.float32)
    us = None
    for r in range(1, ROUNDS):
        pack(r, ys.at[r - 1])
        xs[r][pl.ds(0, BDEV), :] = ys[r - 1]
        if r == 4:
            w = [ys[k] for k in range(4)]
            broadcast_gram(0, [w[i] * w[j] for i, j in PAIRS])
        if r == ROUNDS - 1:
            w = [ys[k] for k in range(6)]
            first_weights = arnoldi_weights(collect_gram(0), substep)
            d = [None] * 4
            for k in range(4):
                term = None
                if k > 0:
                    term = first_weights[k - 1] * (1.0 / SCALE)
                if k < 3:
                    low = first_weights[k] * SHIFT
                    term = -low if term is None else term - low
                d[k] = term
            d[0] = d[0] + 1.0
            us = [d[0] * w[k] + d[1] * w[k + 1] + d[2] * w[k + 2] + d[3] * w[k + 3] for k in range(3)]
            tail = d[0] * w[3] + d[1] * w[4] + d[2] * w[5]
            partial = [us[i] * us[j] for i, j in PAIRS[:6]]
            base = (
                conc[...] + first_weights[0] * w[0] + first_weights[1] * w[1] + first_weights[2] * w[2]
            )
        await_ghosts(r)

        def later(b, row, r=r):
            ys[r, pl.ds(b, 1), :] = (
                slope8[pl.ds(b, 1), :] * ys[r - 1, pl.ds(b, 1), :] - row
            ) * SCALE

        product(r, later)
    last = tail + d[3] * ys[ROUNDS - 1]
    broadcast_gram(1, partial + [us[i] * last for i in range(3)])
    second = arnoldi_weights(collect_gram(1), substep)
    result[...] = base + second[0] * us[0] + second[1] * us[1] + second[2] * us[2]
    out = pltpu.make_async_copy(result, out_hbm, out_sem)
    out.start()
    for r in range(ROUNDS):
        for q in range(4):
            packet(r, q).wait_send()
    for slot in range(2):
        whole = arrivals.at[slot, pl.ds(0, ndev - 1)]
        pltpu.make_async_copy(whole, whole, ar_send.at[slot]).wait()
    out.wait()


def solution(mesh):
    ndev = mesh.shape["dom"]

    def step(conc, rate, size, blocks, cols, lens, lists):
        f32, i32 = jnp.float32, jnp.int32
        return pl.pallas_call(
            lambda *refs: kernel(ndev, *refs),
            out_shape=jax.ShapeDtypeStruct((BDEV, BLK), f32),
            in_specs=[pl.BlockSpec(memory_space=pl.ANY)] * 7,
            out_specs=pl.BlockSpec(memory_space=pl.ANY),
            scratch_shapes=[
                pltpu.VMEM((BDEV, BLK), f32),
                pltpu.VMEM((BDEV, BLK), f32),
                pltpu.VMEM((BDEV, BLK), f32),
                pltpu.VMEM((BDEV, NNZB, BLK, BLK), f32),
                pltpu.VMEM((ROUNDS, BDEV, BLK), f32),
                pltpu.VMEM((ROUNDS, 4, GMAX, BLK), f32),
                pltpu.VMEM((2, 1, BLK), f32),
                pltpu.VMEM((2, ndev, 1, BLK), f32),
                pltpu.VMEM((BDEV, BLK), f32),
                pltpu.SMEM((1,), f32),
                pltpu.SMEM((BDEV, NNZB), i32),
                pltpu.SMEM((BDEV,), i32),
                pltpu.SMEM((1, 4, GMAX), i32),
                pltpu.SMEM((BDEV * NNZB,), i32),
            ]
            + [pltpu.VMEM((XROWS, BLK), f32)] * ROUNDS
            + [
                pltpu.SemaphoreType.DMA((6,)),
                pltpu.SemaphoreType.DMA((BDEV // CHUNK,)),
                pltpu.SemaphoreType.DMA((ROUNDS, 4)),
                pltpu.SemaphoreType.DMA((ROUNDS, 4)),
                pltpu.SemaphoreType.DMA((2,)),
                pltpu.SemaphoreType.DMA((2,)),
                pltpu.SemaphoreType.DMA,
            ],
            compiler_params=pltpu.CompilerParams(collective_id=0, has_side_effects=True),
            name="rosenbrock",
        )(conc, rate, size, blocks, cols, lens, lists)

    dom = "dom"
    return jax.shard_map(
        step,
        mesh=mesh,
        in_specs=(P(dom), P(dom), P(), P(dom), P(dom), P(dom), P(dom)),
        out_specs=P(dom),
        check_vma=False,
    )
```

```python
import jax
import jax.numpy as jnp
from jax import lax
from jax.experimental import pallas as pl
from jax.experimental.pallas import tpu as pltpu
from jax.sharding import PartitionSpec as P

BLK = 128
BDEV = 32
NNZB = 5
GMAX = 16
OFFSETS = (-2, -1, 1, 2)
ORDER = (0, 3, 1, 2)
EPS = 1e-6
SHIFT = 8.0
SCALE = 0.25
ROUNDS = 7
GROUP = 8
CHUNK = 4
ZERO_ROW = BDEV + 4 * GMAX
XROWS = ZERO_ROW + 8
PAIRS = ((0, 0), (0, 1), (0, 2), (1, 1), (1, 2), (2, 2), (0, 3), (1, 3), (2, 3))
MESH = pl.DeviceIdType.MESH


def arnoldi_weights(gram, substep):
    G = {}
    for (i, j), g in gram.items():
        G[i, j] = g
        G[j, i] = g
    zero = jnp.zeros_like(substep)
    magnitude = jnp.sqrt(G[0, 0] + EPS)
    vectors = [[1.0 / magnitude]]
    H = [[None] * 3 for _ in range(3)]
    for col in range(3):
        v = vectors[col]
        n = len(v)
        mapped = [None] * (n + 1)
        for k in range(n + 1):
            term = None
            if k > 0:
                term = v[k - 1] * (1.0 / SCALE)
            if k < n:
                low = v[k] * SHIFT
                term = -low if term is None else term - low
            mapped[k] = term
        image = []
        for i in range(n):
            total = G[i, 0] * mapped[0]
            for k in range(1, n + 1):
                total = total + G[i, k] * mapped[k]
            image.append(total)
        projections = []
        for vec in vectors:
            total = vec[0] * image[0]
            for k in range(1, len(vec)):
                total = total + vec[k] * image[k]
            projections.append(total)
        for k, p in enumerate(projections):
            H[k][col] = p
        if col < 2:
            rest = list(mapped)
            for p, vec in zip(projections, vectors):
                for k in range(len(vec)):
                    rest[k] = rest[k] - p * vec[k]
            square = None
            for i in range(n + 1):
                total = G[i, 0] * rest[0]
                for k in range(1, n + 1):
                    total = total + G[i, k] * rest[k]
                total = total * rest[i]
                square = total if square is None else square + total
            length = jnp.sqrt(square + EPS)
            H[col + 1][col] = length
            inverse = 1.0 / length
            vectors.append([r * inverse for r in rest])
    small = substep * (1.0 / 64.0)
    A = [[None if H[i][j] is None else H[i][j] * small for j in range(3)] for i in range(3)]
    one = jnp.ones_like(substep)
    Pm = [[one if i == j else zero for j in range(3)] for i in range(3)]
    q = [zero] * 3
    for degree in range(12, 0, -1):
        inv = 1.0 / degree
        newP = [[None] * 3 for _ in range(3)]
        newq = [None] * 3
        for i in range(3):
            ks = [k for k in range(3) if A[i][k] is not None]
            for j in range(3):
                total = A[i][ks[0]] * Pm[ks[0]][j]
                for k in ks[1:]:
                    total = total + A[i][k] * Pm[k][j]
                total = total * inv
                newP[i][j] = total + 1.0 if i == j else total
            total = A[i][ks[0]] * q[ks[0]]
            for k in ks[1:]:
                total = total + A[i][k] * q[k]
            if i == 0:
                total = total + (1.0 / 64.0)
            newq[i] = total * inv
        Pm, q = newP, newq
    for _ in range(6):
        newP = [[Pm[i][0] * Pm[0][j] + Pm[i][1] * Pm[1][j] + Pm[i][2] * Pm[2][j] for j in range(3)] for i in range(3)]
        q = [Pm[i][0] * q[0] + Pm[i][1] * q[1] + Pm[i][2] * q[2] + q[i] for i in range(3)]
        Pm = newP
    out = []
    for k in range(3):
        total = None
        for col in range(k, 3):
            term = q[col] * vectors[col][k]
            total = term if total is None else total + term
        out.append(total * (substep * magnitude))
    return out


def far_first():
    steps = (0, 1, 2, 1)
    every = [(y, z, x, c) for y in range(4) for z in range(4) for x in range(4) for c in range(2)]
    every.remove((0, 0, 0, 0))
    return sorted(every, key=lambda o: (-(steps[o[0]] + steps[o[1]] + steps[o[2]]), o))


def kernel(ndev, conc_hbm, rate_hbm, step_hbm, blocks_hbm, cols_hbm, lens_hbm, lists_hbm, result, *scratch):
    (conc, rate, slope8, fixed, blocks, ys, sends, gram_row, arrivals, step_s, cols_s, lens_s, lists_s, index_s) = scratch[:14]
    xs = scratch[14 : 14 + ROUNDS]
    in_sems, block_sems, send_sems, recv_sems, ar_send, ar_recv, known_z, known_y = scratch[14 + ROUNDS :]
    me = lax.axis_index("dom")

    def near(o):
        return lax.rem(me + (o + ndev), ndev)

    my_core, my_x = lax.rem(me, 2), lax.rem(me // 2, 4)
    my_z, my_y = lax.rem(me // 8, 4), me // 32
    at_y = [lax.rem(my_y + d, 4) * 32 for d in range(4)]
    at_z = [lax.rem(my_z + d, 4) * 8 for d in range(4)]
    at_x = [lax.rem(my_x + d, 4) * 2 for d in range(4)]
    at_core = [my_core, 1 - my_core]

    def at(o):
        return at_y[o[0]] + at_z[o[1]] + at_x[o[2]] + at_core[o[3]]

    row_line = [(0, 0, x, c) for x in range(4) for c in range(2) if (x, c) != (0, 0)]
    z_line = [(0, d, 0, 0) for d in (1, 2, 3)]
    y_line = [(d, 0, 0, 0) for d in (1, 2, 3)]

    barrier = pltpu.get_barrier_semaphore()
    greeted = [near(OFFSETS[q]) for q in ORDER] + [at(o) for o in z_line + y_line + row_line]
    for device in greeted:
        pl.semaphore_signal(barrier, inc=1, device_id=(device,), device_id_type=MESH)

    small = [
        pltpu.make_async_copy(lists_hbm, lists_s, in_sems.at[0]),
        pltpu.make_async_copy(conc_hbm, conc, in_sems.at[1]),
        pltpu.make_async_copy(cols_hbm, cols_s, in_sems.at[2]),
        pltpu.make_async_copy(lens_hbm, lens_s, in_sems.at[3]),
        pltpu.make_async_copy(rate_hbm, rate, in_sems.at[4]),
        pltpu.make_async_copy(step_hbm, step_s, in_sems.at[5]),
    ]
    for copy in small:
        copy.start()
    chunks = []
    for c in range(BDEV // CHUNK):
        part = pl.ds(c * CHUNK, CHUNK)
        chunks.append(pltpu.make_async_copy(blocks_hbm.at[part], blocks.at[part], block_sems.at[c]))
        chunks[-1].start()

    def packet(r, q):
        return pltpu.make_async_remote_copy(
            src_ref=sends.at[r, q],
            dst_ref=xs[r].at[pl.ds(BDEV + q * GMAX, GMAX), :],
            send_sem=send_sems.at[r, q],
            recv_sem=recv_sems.at[r, q],
            device_id=(near(OFFSETS[q]),),
            device_id_type=MESH,
        )

    def pack(r, source):
        for q in ORDER:
            for g in range(GMAX):
                sends[r, q, pl.ds(g, 1), :] = source[pl.ds(lists_s[0, q, g], 1), :]
            if r > 0:
                packet(r, q).start()

    def await_ghosts(r):
        for q in ORDER:
            packet(r, q).wait_recv()

    def lane_sums(total):
        return jnp.sum(total.T, axis=0, keepdims=True)

    def own_part(r):
        source = conc if r == 0 else ys.at[r - 1]

        def group(i, carry):
            for s in range(GROUP):
                b = i * GROUP + s
                mine = source[pl.ds(b, 1), :]
                here = lane_sums(blocks[b, 0] * mine)
                if r == 0:
                    kept = rate[pl.ds(b, 1), :] * mine * (1.0 - mine)
                else:
                    kept = slope8[pl.ds(b, 1), :] * mine
                fixed[pl.ds(b, 1), :] = kept - here
            return carry

        lax.fori_loop(0, BDEV // GROUP, group, 0)

    def product(r):
        x = xs[r]
        for b in range(BDEV):
            total = None
            for t in range(1, NNZB):
                row = x[pl.ds(index_s[b * NNZB + t], 8, stride=0), :]
                term = blocks[b, t].reshape(16, 8, BLK) * row[None]
                total = term if total is None else total + term
            whole = fixed[pl.ds(b, 1), :] - lane_sums(total.reshape(BLK, BLK))
            ys[r, pl.ds(b, 1), :] = whole if r == 0 else whole * SCALE

    small[0].wait()
    small[1].wait()
    pack(0, conc)
    pl.semaphore_wait(barrier, len(greeted))
    for q in ORDER:
        packet(0, q).start()
    for o in z_line:
        pl.semaphore_signal(known_z, inc=1, device_id=(at(o),), device_id_type=MESH)
    xs[0][pl.ds(0, BDEV), :] = conc[...]
    for x in xs:
        x[pl.ds(ZERO_ROW, 8), :] = jnp.zeros((8, BLK), jnp.float32)
    for copy in small[2:]:
        copy.wait()
    slope8[...] = rate[...] * (1.0 - 2.0 * conc[...]) + SHIFT

    def remap(b, carry):
        length = lens_s[b]
        for t in range(1, NNZB):
            index_s[b * NNZB + t] = jnp.where(t < length, cols_s[t, b], ZERO_ROW)
        return carry

    lax.fori_loop(0, BDEV, remap, 0)
    for chunk in chunks:
        chunk.wait()
    own_part(0)
    await_ghosts(0)
    product(0)

    def broadcast_gram(slot, products):
        rows = [jnp.sum(p, axis=0, keepdims=True) for p in products]
        rows = rows + [jnp.zeros((BLK - len(rows), BLK), jnp.float32)]
        gram_row[slot] = jnp.sum(jnp.concatenate(rows, axis=0).T, axis=0, keepdims=True)
        for o in far_first():
            pltpu.make_async_remote_copy(
                src_ref=gram_row.at[slot],
                dst_ref=arrivals.at[slot, me],
                send_sem=ar_send.at[slot],
                recv_sem=ar_recv.at[slot],
                device_id=(at(o),),
                device_id_type=MESH,
            ).start()

    def collect_gram(slot):
        whole = arrivals.at[slot, pl.ds(0, ndev - 1)]
        pltpu.make_async_copy(whole, whole, ar_recv.at[slot]).wait()
        arrivals[slot, me] = gram_row[slot]
        total = jnp.sum(arrivals[slot], axis=0)
        return {
            pair: jnp.broadcast_to(total[:, e : e + 1], (1, BLK)) for e, pair in enumerate(PAIRS)
        }

    substep = jnp.full((1, BLK), step_s[0] * 0.5, jnp.float32)
    us = None
    for r in range(1, ROUNDS):
        pack(r, ys.at[r - 1])
        xs[r][pl.ds(0, BDEV), :] = ys[r - 1]
        if r == 1:
            pl.semaphore_wait(known_z, 3)
            for o in y_line:
                pl.semaphore_signal(known_y, inc=1, device_id=(at(o),), device_id_type=MESH)
        own_part(r)
        if r == 4:
            pl.semaphore_wait(known_y, 3)
            w = [ys[k] for k in range(4)]
            broadcast_gram(0, [w[i] * w[j] for i, j in PAIRS])
        if r == ROUNDS - 1:
            w = [ys[k] for k in range(6)]
            first_weights = arnoldi_weights(collect_gram(0), substep)
            d = [None] * 4
            for k in range(4):
                term = None
                if k > 0:
                    term = first_weights[k - 1] * (1.0 / SCALE)
                if k < 3:
                    low = first_weights[k] * SHIFT
                    term = -low if term is None else term - low
                d[k] = term
            d[0] = d[0] + 1.0
            us = [d[0] * w[k] + d[1] * w[k + 1] + d[2] * w[k + 2] + d[3] * w[k + 3] for k in range(3)]
            tail = d[0] * w[3] + d[1] * w[4] + d[2] * w[5]
            partial = [us[i] * us[j] for i, j in PAIRS[:6]]
            base = (
                conc[...] + first_weights[0] * w[0] + first_weights[1] * w[1] + first_weights[2] * w[2]
            )
        await_ghosts(r)
        product(r)
    last = tail + d[3] * ys[ROUNDS - 1]
    broadcast_gram(1, partial + [us[i] * last for i in range(3)])
    second = arnoldi_weights(collect_gram(1), substep)
    result[...] = base + second[0] * us[0] + second[1] * us[1] + second[2] * us[2]
    for r in range(ROUNDS):
        for q in range(4):
            packet(r, q).wait_send()
    for slot in range(2):
        whole = arrivals.at[slot, pl.ds(0, ndev - 1)]
        pltpu.make_async_copy(whole, whole, ar_send.at[slot]).wait()


def solution(mesh):
    ndev = mesh.shape["dom"]

    def step(conc, rate, size, blocks, cols, lens, lists):
        f32, i32 = jnp.float32, jnp.int32
        return pl.pallas_call(
            lambda *refs: kernel(ndev, *refs),
            out_shape=pltpu.VMEM((BDEV, BLK), f32),
            in_specs=[pl.BlockSpec(memory_space=pl.ANY)] * 7,
            out_specs=pl.BlockSpec(memory_space=pltpu.VMEM),
            scratch_shapes=[
                pltpu.VMEM((BDEV, BLK), f32),
                pltpu.VMEM((BDEV, BLK), f32),
                pltpu.VMEM((BDEV, BLK), f32),
                pltpu.VMEM((BDEV, BLK), f32),
                pltpu.VMEM((BDEV, NNZB, BLK, BLK), f32),
                pltpu.VMEM((ROUNDS, BDEV, BLK), f32),
                pltpu.VMEM((ROUNDS, 4, GMAX, BLK), f32),
                pltpu.VMEM((2, 1, BLK), f32),
                pltpu.VMEM((2, ndev, 1, BLK), f32),
                pltpu.SMEM((1,), f32),
                pltpu.SMEM((NNZB, BDEV), i32),
                pltpu.SMEM((BDEV,), i32),
                pltpu.SMEM((1, 4, GMAX), i32),
                pltpu.SMEM((BDEV * NNZB,), i32),
            ]
            + [pltpu.VMEM((XROWS, BLK), f32)] * ROUNDS
            + [
                pltpu.SemaphoreType.DMA((6,)),
                pltpu.SemaphoreType.DMA((BDEV // CHUNK,)),
                pltpu.SemaphoreType.DMA((ROUNDS, 4)),
                pltpu.SemaphoreType.DMA((ROUNDS, 4)),
                pltpu.SemaphoreType.DMA((2,)),
                pltpu.SemaphoreType.DMA((2,)),
                pltpu.SemaphoreType.REGULAR,
                pltpu.SemaphoreType.REGULAR,
            ],
            compiler_params=pltpu.CompilerParams(collective_id=0, has_side_effects=True),
            name="rosenbrock",
        )(conc, rate, size, blocks, cols.T, lens, lists)

    dom = "dom"
    return jax.shard_map(
        step,
        mesh=mesh,
        in_specs=(P(dom), P(dom), P(), P(dom), P(dom), P(dom), P(dom)),
        out_specs=P(dom),
        check_vma=False,
    )
```

```python
import jax
import jax.numpy as jnp
from jax import lax
from jax.experimental import pallas as pl
from jax.experimental.pallas import tpu as pltpu
from jax.sharding import PartitionSpec as P

BLK = 128
BDEV = 32
NNZB = 5
GMAX = 16
OFFSETS = (-2, -1, 1, 2)
ORDER = (0, 3, 1, 2)
EPS = 1e-6
SHIFT = 8.0
SCALE = 0.25
ROUNDS = 7
GROUP = 8
CHUNK = 4
ZERO_ROW = BDEV + 4 * GMAX
XROWS = ZERO_ROW + 8
PAIRS = ((0, 0), (0, 1), (0, 2), (1, 1), (1, 2), (2, 2), (0, 3), (1, 3), (2, 3))
MESH = pl.DeviceIdType.MESH


def arnoldi_weights(gram, substep):
    G = {}
    for (i, j), g in gram.items():
        G[i, j] = g
        G[j, i] = g
    zero = jnp.zeros_like(substep)
    magnitude = jnp.sqrt(G[0, 0] + EPS)
    vectors = [[1.0 / magnitude]]
    H = [[None] * 3 for _ in range(3)]
    for col in range(3):
        v = vectors[col]
        n = len(v)
        mapped = [None] * (n + 1)
        for k in range(n + 1):
            term = None
            if k > 0:
                term = v[k - 1] * (1.0 / SCALE)
            if k < n:
                low = v[k] * SHIFT
                term = -low if term is None else term - low
            mapped[k] = term
        image = []
        for i in range(n):
            total = G[i, 0] * mapped[0]
            for k in range(1, n + 1):
                total = total + G[i, k] * mapped[k]
            image.append(total)
        projections = []
        for vec in vectors:
            total = vec[0] * image[0]
            for k in range(1, len(vec)):
                total = total + vec[k] * image[k]
            projections.append(total)
        for k, p in enumerate(projections):
            H[k][col] = p
        if col < 2:
            rest = list(mapped)
            for p, vec in zip(projections, vectors):
                for k in range(len(vec)):
                    rest[k] = rest[k] - p * vec[k]
            square = None
            for i in range(n + 1):
                total = G[i, 0] * rest[0]
                for k in range(1, n + 1):
                    total = total + G[i, k] * rest[k]
                total = total * rest[i]
                square = total if square is None else square + total
            length = jnp.sqrt(square + EPS)
            H[col + 1][col] = length
            inverse = 1.0 / length
            vectors.append([r * inverse for r in rest])
    small = substep * (1.0 / 64.0)
    A = [[None if H[i][j] is None else H[i][j] * small for j in range(3)] for i in range(3)]
    one = jnp.ones_like(substep)
    Pm = [[one if i == j else zero for j in range(3)] for i in range(3)]
    q = [zero] * 3
    for degree in range(12, 0, -1):
        inv = 1.0 / degree
        newP = [[None] * 3 for _ in range(3)]
        newq = [None] * 3
        for i in range(3):
            ks = [k for k in range(3) if A[i][k] is not None]
            for j in range(3):
                total = A[i][ks[0]] * Pm[ks[0]][j]
                for k in ks[1:]:
                    total = total + A[i][k] * Pm[k][j]
                total = total * inv
                newP[i][j] = total + 1.0 if i == j else total
            total = A[i][ks[0]] * q[ks[0]]
            for k in ks[1:]:
                total = total + A[i][k] * q[k]
            if i == 0:
                total = total + (1.0 / 64.0)
            newq[i] = total * inv
        Pm, q = newP, newq
    for _ in range(6):
        newP = [[Pm[i][0] * Pm[0][j] + Pm[i][1] * Pm[1][j] + Pm[i][2] * Pm[2][j] for j in range(3)] for i in range(3)]
        q = [Pm[i][0] * q[0] + Pm[i][1] * q[1] + Pm[i][2] * q[2] + q[i] for i in range(3)]
        Pm = newP
    out = []
    for k in range(3):
        total = None
        for col in range(k, 3):
            term = q[col] * vectors[col][k]
            total = term if total is None else total + term
        out.append(total * (substep * magnitude))
    return out


def kernel(ndev, conc_hbm, rate_hbm, step_hbm, blocks_hbm, cols_hbm, lens_hbm, lists_hbm, result, *scratch):
    (conc_in, rate_in, conc, rate, slope8, fixed, blocks, ys, sends, gram_row, arrivals, ordered) = scratch[:12]
    (step_s, cols_s, lens_s, lists_s, index_s, place_s, row_s, pick_s) = scratch[12:20]
    xs = scratch[20 : 20 + ROUNDS]
    in_sems, block_sems, send_sems, recv_sems, ar_send, ar_recv, known_z, known_y = scratch[20 + ROUNDS :]
    me = lax.axis_index("dom")

    def near(o):
        return lax.rem(me + (o + ndev), ndev)

    my_core, my_x = lax.rem(me, 2), lax.rem(me // 2, 4)
    my_z, my_y = lax.rem(me // 8, 4), me // 32
    at_y = [lax.rem(my_y + d, 4) * 32 for d in range(4)]
    at_z = [lax.rem(my_z + d, 4) * 8 for d in range(4)]
    at_x = [lax.rem(my_x + d, 4) * 2 for d in range(4)]
    at_core = [my_core, 1 - my_core]
    urgent = jnp.where(my_x < 2, 0, 3 - my_core)

    def at(o):
        return at_y[o[0]] + at_z[o[1]] + at_x[o[2]] + at_core[o[3]]

    row_line = [(0, 0, x, c) for x in range(4) for c in range(2) if (x, c) != (0, 0)]
    z_line = [(0, d, 0, 0) for d in (1, 2, 3)]
    y_line = [(d, 0, 0, 0) for d in (1, 2, 3)]

    barrier = pltpu.get_barrier_semaphore()
    greeted = [near(OFFSETS[q]) for q in ORDER] + [at(o) for o in z_line + y_line + row_line]
    for device in greeted:
        pl.semaphore_signal(barrier, inc=1, device_id=(device,), device_id_type=MESH)

    small = [
        pltpu.make_async_copy(lists_hbm, lists_s, in_sems.at[0]),
        pltpu.make_async_copy(conc_hbm, conc_in, in_sems.at[1]),
        pltpu.make_async_copy(cols_hbm, cols_s, in_sems.at[2]),
        pltpu.make_async_copy(lens_hbm, lens_s, in_sems.at[3]),
        pltpu.make_async_copy(rate_hbm, rate_in, in_sems.at[4]),
        pltpu.make_async_copy(step_hbm, step_s, in_sems.at[5]),
    ]
    for copy in small:
        copy.start()
    chunks = []
    for c in range(BDEV // CHUNK):
        part = pl.ds(c * CHUNK, CHUNK)
        chunks.append(pltpu.make_async_copy(blocks_hbm.at[part], blocks.at[part], block_sems.at[c]))
        chunks[-1].start()

    def packet(r, q, source):
        offset = jnp.where(q < 2, q - 2, q - 1)
        return pltpu.make_async_remote_copy(
            src_ref=source,
            dst_ref=xs[r].at[pl.ds(pl.multiple_of(BDEV + q * GMAX, 8), GMAX), :],
            send_sem=send_sems.at[r, q],
            recv_sem=recv_sems.at[r, q],
            device_id=(lax.rem(me + offset + ndev, ndev),),
            device_id_type=MESH,
        )

    def await_ghosts(r):
        for q in ORDER:
            packet(r, q, sends.at[0, 0]).wait_recv()

    def lane_sums(total):
        return jnp.sum(total.T, axis=0, keepdims=True)

    def own_part(r):
        source = conc if r == 0 else ys.at[r - 1]

        def group(i, carry):
            for s in range(GROUP):
                p = i * GROUP + s
                mine = source[pl.ds(p, 1), :]
                here = lane_sums(blocks[row_s[p], 0] * mine)
                if r == 0:
                    kept = rate[pl.ds(p, 1), :] * mine * (1.0 - mine)
                else:
                    kept = slope8[pl.ds(p, 1), :] * mine
                fixed[pl.ds(p, 1), :] = kept - here
            return carry

        lax.fori_loop(0, BDEV // GROUP, group, 0)

    def product(r, low, high):
        x = xs[r]
        for p in range(low, high):
            total = None
            b = row_s[p]
            for t in range(1, NNZB):
                row = x[pl.ds(index_s[p * NNZB + t], 8, stride=0), :]
                term = blocks[b, t].reshape(16, 8, BLK) * row[None]
                total = term if total is None else total + term
            whole = fixed[pl.ds(p, 1), :] - lane_sums(total.reshape(BLK, BLK))
            whole = whole if r == 0 else whole * SCALE
            ys[r, pl.ds(p, 1), :] = whole
            if r + 1 < ROUNDS:
                xs[r + 1][pl.ds(p, 1), :] = whole

    def turn(r):
        product(r, 0, GMAX)
        n = r + 1
        if n < ROUNDS:
            packet(n, urgent, ys.at[r, pl.ds(0, GMAX), :]).start()
        product(r, GMAX, BDEV)
        if n < ROUNDS:
            for k in range(1, 4):
                q = lax.rem(urgent + k, 4)
                for g in range(GMAX):
                    sends[n, k, pl.ds(g, 1), :] = ys[r, pl.ds(pick_s[q * GMAX + g], 1), :]
                packet(n, q, sends.at[n, k]).start()

    small[0].wait()
    small[1].wait()
    for q in ORDER:
        for g in range(GMAX):
            sends[0, q, pl.ds(g, 1), :] = conc_in[pl.ds(lists_s[0, q, g], 1), :]
    pl.semaphore_wait(barrier, len(greeted))
    for q in ORDER:
        packet(0, q, sends.at[0, q]).start()
    for o in z_line:
        pl.semaphore_signal(known_z, inc=1, device_id=(at(o),), device_id_type=MESH)
    for x in xs:
        x[pl.ds(ZERO_ROW, 8), :] = jnp.zeros((8, BLK), jnp.float32)
    for copy in small[2:]:
        copy.wait()

    def find(b, others):
        found = 0
        for g in range(GMAX):
            found = jnp.where(lists_s[0, urgent, g] == b, g + 1, found)
        place_s[b] = jnp.where(found > 0, found - 1, jnp.minimum(GMAX + others, BDEV - 1))
        return others + jnp.where(found > 0, 0, 1)

    lax.fori_loop(0, BDEV, find, 0)

    def order(p, carry):
        b = 0
        for i in range(BDEV):
            b = jnp.where(place_s[i] == p, i, b)
        row_s[p] = b
        conc[pl.ds(p, 1), :] = conc_in[pl.ds(b, 1), :]
        rate[pl.ds(p, 1), :] = rate_in[pl.ds(b, 1), :]
        xs[0][pl.ds(p, 1), :] = conc_in[pl.ds(b, 1), :]
        length = lens_s[b]
        for t in range(1, NNZB):
            col = cols_s[t, b]
            moved = jnp.where(col < BDEV, place_s[jnp.clip(col, 0, BDEV - 1)], jnp.minimum(col, ZERO_ROW))
            index_s[p * NNZB + t] = jnp.where(t < length, moved, ZERO_ROW)
        return carry

    lax.fori_loop(0, BDEV, order, 0)

    def choose(g, carry):
        for q in range(4):
            pick_s[q * GMAX + g] = place_s[lists_s[0, q, g]]
        return carry

    lax.fori_loop(0, GMAX, choose, 0)
    slope8[...] = rate[...] * (1.0 - 2.0 * conc[...]) + SHIFT
    for chunk in chunks:
        chunk.wait()
    own_part(0)
    await_ghosts(0)
    turn(0)

    def broadcast_gram(slot, products):
        rows = [jnp.sum(p, axis=0, keepdims=True) for p in products]
        rows = rows + [jnp.zeros((BLK - len(rows), BLK), jnp.float32)]
        gram_row[slot] = jnp.sum(jnp.concatenate(rows, axis=0).T, axis=0, keepdims=True)
        for k in range(ndev - 1):
            pltpu.make_async_remote_copy(
                src_ref=gram_row.at[slot],
                dst_ref=arrivals.at[slot, me],
                send_sem=ar_send.at[slot],
                recv_sem=ar_recv.at[slot],
                device_id=(jnp.where(me <= k, k + 1, k),),
                device_id_type=MESH,
            ).start()

    def collect_gram(slot):
        whole = arrivals.at[slot, pl.ds(0, ndev - 1)]
        pltpu.make_async_copy(whole, whole, ar_recv.at[slot]).wait()
        arrivals[slot, me] = gram_row[slot]
        total = jnp.sum(arrivals[slot], axis=0)
        return {
            pair: jnp.broadcast_to(total[:, e : e + 1], (1, BLK)) for e, pair in enumerate(PAIRS)
        }

    substep = jnp.full((1, BLK), step_s[0] * 0.5, jnp.float32)
    us = None
    for r in range(1, ROUNDS):
        if r == 1:
            pl.semaphore_wait(known_z, 3)
            for o in y_line:
                pl.semaphore_signal(known_y, inc=1, device_id=(at(o),), device_id_type=MESH)
        own_part(r)
        if r == 4:
            pl.semaphore_wait(known_y, 3)
            w = [ys[k] for k in range(4)]
            broadcast_gram(0, [w[i] * w[j] for i, j in PAIRS])
        if r == ROUNDS - 1:
            w = [ys[k] for k in range(6)]
            first_weights = arnoldi_weights(collect_gram(0), substep)
            d = [None] * 4
            for k in range(4):
                term = None
                if k > 0:
                    term = first_weights[k - 1] * (1.0 / SCALE)
                if k < 3:
                    low = first_weights[k] * SHIFT
                    term = -low if term is None else term - low
                d[k] = term
            d[0] = d[0] + 1.0
            us = [d[0] * w[k] + d[1] * w[k + 1] + d[2] * w[k + 2] + d[3] * w[k + 3] for k in range(3)]
            tail = d[0] * w[3] + d[1] * w[4] + d[2] * w[5]
            partial = [us[i] * us[j] for i, j in PAIRS[:6]]
            base = (
                conc[...] + first_weights[0] * w[0] + first_weights[1] * w[1] + first_weights[2] * w[2]
            )
        await_ghosts(r)
        turn(r)
    last = tail + d[3] * ys[ROUNDS - 1]
    broadcast_gram(1, partial + [us[i] * last for i in range(3)])
    second = arnoldi_weights(collect_gram(1), substep)
    ordered[...] = base + second[0] * us[0] + second[1] * us[1] + second[2] * us[2]
    for b in range(BDEV):
        result[pl.ds(b, 1), :] = ordered[pl.ds(place_s[b], 1), :]
    for r in range(ROUNDS):
        for q in range(4):
            packet(r, q, sends.at[0, 0]).wait_send()
    for slot in range(2):
        whole = arrivals.at[slot, pl.ds(0, ndev - 1)]
        pltpu.make_async_copy(whole, whole, ar_send.at[slot]).wait()


def solution(mesh):
    ndev = mesh.shape["dom"]

    def step(conc, rate, size, blocks, cols, lens, lists):
        f32, i32 = jnp.float32, jnp.int32
        return pl.pallas_call(
            lambda *refs: kernel(ndev, *refs),
            out_shape=pltpu.VMEM((BDEV, BLK), f32),
            in_specs=[pl.BlockSpec(memory_space=pl.ANY)] * 7,
            out_specs=pl.BlockSpec(memory_space=pltpu.VMEM),
            scratch_shapes=[
                pltpu.VMEM((BDEV, BLK), f32),
                pltpu.VMEM((BDEV, BLK), f32),
                pltpu.VMEM((BDEV, BLK), f32),
                pltpu.VMEM((BDEV, BLK), f32),
                pltpu.VMEM((BDEV, BLK), f32),
                pltpu.VMEM((BDEV, BLK), f32),
                pltpu.VMEM((BDEV, NNZB, BLK, BLK), f32),
                pltpu.VMEM((ROUNDS, BDEV, BLK), f32),
                pltpu.VMEM((ROUNDS, 4, GMAX, BLK), f32),
                pltpu.VMEM((2, 1, BLK), f32),
                pltpu.VMEM((2, ndev, 1, BLK), f32),
                pltpu.VMEM((BDEV, BLK), f32),
                pltpu.SMEM((1,), f32),
                pltpu.SMEM((NNZB, BDEV), i32),
                pltpu.SMEM((BDEV,), i32),
                pltpu.SMEM((1, 4, GMAX), i32),
                pltpu.SMEM((BDEV * NNZB,), i32),
                pltpu.SMEM((BDEV,), i32),
                pltpu.SMEM((BDEV,), i32),
                pltpu.SMEM((4 * GMAX,), i32),
            ]
            + [pltpu.VMEM((XROWS, BLK), f32)] * ROUNDS
            + [
                pltpu.SemaphoreType.DMA((6,)),
                pltpu.SemaphoreType.DMA((BDEV // CHUNK,)),
                pltpu.SemaphoreType.DMA((ROUNDS, 4)),
                pltpu.SemaphoreType.DMA((ROUNDS, 4)),
                pltpu.SemaphoreType.DMA((2,)),
                pltpu.SemaphoreType.DMA((2,)),
                pltpu.SemaphoreType.REGULAR,
                pltpu.SemaphoreType.REGULAR,
            ],
            compiler_params=pltpu.CompilerParams(collective_id=0, has_side_effects=True),
            name="rosenbrock",
        )(conc, rate, size, blocks, cols.T, lens, lists)

    dom = "dom"
    return jax.shard_map(
        step,
        mesh=mesh,
        in_specs=(P(dom), P(dom), P(), P(dom), P(dom), P(dom), P(dom)),
        out_specs=P(dom),
        check_vma=False,
    )
```

```python
import jax
import jax.numpy as jnp
from jax import lax
from jax.experimental import pallas as pl
from jax.experimental.pallas import tpu as pltpu
from jax.sharding import PartitionSpec as P

BLK = 128
BDEV = 32
NNZB = 5
GMAX = 16
OFFSETS = (-2, -1, 1, 2)
ORDER = (0, 3, 1, 2)
EPS = 1e-6
SHIFT = 8.0
SCALE = 0.25
ROUNDS = 7
GROUP = 8
CHUNK = 4
ZERO_ROW = BDEV + 4 * GMAX
XROWS = ZERO_ROW + 8
RELAY_ROW = XROWS
RELAY_A = 7
RELAY_B = 103
RELAYED = ((2, 0), (1, 1), (1, 0))
PAIRS = ((0, 0), (0, 1), (0, 2), (1, 1), (1, 2), (2, 2), (0, 3), (1, 3), (2, 3))
MESH = pl.DeviceIdType.MESH


def arnoldi_weights(gram, substep):
    G = {}
    for (i, j), g in gram.items():
        G[i, j] = g
        G[j, i] = g
    zero = jnp.zeros_like(substep)
    magnitude = jnp.sqrt(G[0, 0] + EPS)
    vectors = [[1.0 / magnitude]]
    H = [[None] * 3 for _ in range(3)]
    for col in range(3):
        v = vectors[col]
        n = len(v)
        mapped = [None] * (n + 1)
        for k in range(n + 1):
            term = None
            if k > 0:
                term = v[k - 1] * (1.0 / SCALE)
            if k < n:
                low = v[k] * SHIFT
                term = -low if term is None else term - low
            mapped[k] = term
        image = []
        for i in range(n):
            total = G[i, 0] * mapped[0]
            for k in range(1, n + 1):
                total = total + G[i, k] * mapped[k]
            image.append(total)
        projections = []
        for vec in vectors:
            total = vec[0] * image[0]
            for k in range(1, len(vec)):
                total = total + vec[k] * image[k]
            projections.append(total)
        for k, p in enumerate(projections):
            H[k][col] = p
        if col < 2:
            rest = list(mapped)
            for p, vec in zip(projections, vectors):
                for k in range(len(vec)):
                    rest[k] = rest[k] - p * vec[k]
            square = None
            for i in range(n + 1):
                total = G[i, 0] * rest[0]
                for k in range(1, n + 1):
                    total = total + G[i, k] * rest[k]
                total = total * rest[i]
                square = total if square is None else square + total
            length = jnp.sqrt(square + EPS)
            H[col + 1][col] = length
            inverse = 1.0 / length
            vectors.append([r * inverse for r in rest])
    small = substep * (1.0 / 64.0)
    A = [[None if H[i][j] is None else H[i][j] * small for j in range(3)] for i in range(3)]
    one = jnp.ones_like(substep)
    Pm = [[one if i == j else zero for j in range(3)] for i in range(3)]
    q = [zero] * 3
    for degree in range(12, 0, -1):
        inv = 1.0 / degree
        newP = [[None] * 3 for _ in range(3)]
        newq = [None] * 3
        for i in range(3):
            ks = [k for k in range(3) if A[i][k] is not None]
            for j in range(3):
                total = A[i][ks[0]] * Pm[ks[0]][j]
                for k in ks[1:]:
                    total = total + A[i][k] * Pm[k][j]
                total = total * inv
                newP[i][j] = total + 1.0 if i == j else total
            total = A[i][ks[0]] * q[ks[0]]
            for k in ks[1:]:
                total = total + A[i][k] * q[k]
            if i == 0:
                total = total + (1.0 / 64.0)
            newq[i] = total * inv
        Pm, q = newP, newq
    for _ in range(6):
        newP = [[Pm[i][0] * Pm[0][j] + Pm[i][1] * Pm[1][j] + Pm[i][2] * Pm[2][j] for j in range(3)] for i in range(3)]
        q = [Pm[i][0] * q[0] + Pm[i][1] * q[1] + Pm[i][2] * q[2] + q[i] for i in range(3)]
        Pm = newP
    out = []
    for k in range(3):
        total = None
        for col in range(k, 3):
            term = q[col] * vectors[col][k]
            total = term if total is None else total + term
        out.append(total * (substep * magnitude))
    return out


def kernel(ndev, conc_hbm, rate_hbm, step_hbm, blocks_hbm, cols_hbm, lens_hbm, lists_hbm, result, *scratch):
    (conc_in, rate_in, conc, rate, slope8, fixed, blocks, ys, sends, gram_row, arrivals, ordered) = scratch[:12]
    (step_s, cols_s, lens_s, lists_s, index_s, place_s, row_s, pick_s) = scratch[12:20]
    xs = scratch[20 : 20 + ROUNDS]
    in_sems, block_sems, send_sems, recv_sems, ar_send, ar_recv, relay_sems, known_z, known_y = scratch[20 + ROUNDS :]
    me = lax.axis_index("dom")

    def near(o):
        return lax.rem(me + (o + ndev), ndev)

    my_core, my_x = lax.rem(me, 2), lax.rem(me // 2, 4)
    my_z, my_y = lax.rem(me // 8, 4), me // 32
    at_y = [lax.rem(my_y + d, 4) * 32 for d in range(4)]
    at_z = [lax.rem(my_z + d, 4) * 8 for d in range(4)]
    at_x = [lax.rem(my_x + d, 4) * 2 for d in range(4)]
    at_core = [my_core, 1 - my_core]
    urgent = jnp.where(my_x < 2, 0, 3 - my_core)

    def at(o):
        return at_y[o[0]] + at_z[o[1]] + at_x[o[2]] + at_core[o[3]]

    row_line = [(0, 0, x, c) for x in range(4) for c in range(2) if (x, c) != (0, 0)]
    z_line = [(0, d, 0, 0) for d in (1, 2, 3)]
    y_line = [(d, 0, 0, 0) for d in (1, 2, 3)]

    small = [
        pltpu.make_async_copy(lists_hbm, lists_s, in_sems.at[0]),
        pltpu.make_async_copy(conc_hbm, conc_in, in_sems.at[1]),
        pltpu.make_async_copy(cols_hbm, cols_s, in_sems.at[2]),
        pltpu.make_async_copy(lens_hbm, lens_s, in_sems.at[3]),
        pltpu.make_async_copy(rate_hbm, rate_in, in_sems.at[4]),
        pltpu.make_async_copy(step_hbm, step_s, in_sems.at[5]),
    ]
    small[0].start()
    small[1].start()

    barrier = pltpu.get_barrier_semaphore()
    greeted = [
        jnp.where(me + OFFSETS[q] >= ndev, RELAY_B, near(OFFSETS[q])) for q in ORDER
    ] + [at(o) for o in z_line + y_line + row_line]
    for device in greeted:
        pl.semaphore_signal(barrier, inc=1, device_id=(device,), device_id_type=MESH)
    greetings = len(greeted) + jnp.where(me == RELAY_B, 3, 0) - jnp.maximum(2 - me, 0)

    for copy in small[2:]:
        copy.start()
    chunks = []
    for c in range(BDEV // CHUNK):
        part = pl.ds(c * CHUNK, CHUNK)
        chunks.append(pltpu.make_async_copy(blocks_hbm.at[part], blocks.at[part], block_sems.at[c]))
        chunks[-1].start()

    def packet(r, q, source):
        offset = jnp.where(q < 2, q - 2, q - 1)
        return pltpu.make_async_remote_copy(
            src_ref=source,
            dst_ref=xs[r].at[pl.ds(pl.multiple_of(BDEV + q * GMAX, 8), GMAX), :],
            send_sem=send_sems.at[r, q],
            recv_sem=recv_sems.at[r, q],
            device_id=(lax.rem(me + offset + ndev, ndev),),
            device_id_type=MESH,
        )

    def await_ghosts(r):
        for q in ORDER:
            packet(r, q, sends.at[0, 0]).wait_recv()

    def lane_sums(total):
        return jnp.sum(total.T, axis=0, keepdims=True)

    def own_part(r):
        source = conc if r == 0 else ys.at[r - 1]

        def group(i, carry):
            for s in range(GROUP):
                p = i * GROUP + s
                mine = source[pl.ds(p, 1), :]
                here = lane_sums(blocks[row_s[p], 0] * mine)
                if r == 0:
                    kept = rate[pl.ds(p, 1), :] * mine * (1.0 - mine)
                else:
                    kept = slope8[pl.ds(p, 1), :] * mine
                fixed[pl.ds(p, 1), :] = kept - here
            return carry

        lax.fori_loop(0, BDEV // GROUP, group, 0)

    def product(r, low, high):
        x = xs[r]
        for p in range(low, high):
            total = None
            b = row_s[p]
            for t in range(1, NNZB):
                row = x[pl.ds(index_s[p * NNZB + t], 8, stride=0), :]
                term = blocks[b, t].reshape(16, 8, BLK) * row[None]
                total = term if total is None else total + term
            whole = fixed[pl.ds(p, 1), :] - lane_sums(total.reshape(BLK, BLK))
            whole = whole if r == 0 else whole * SCALE
            ys[r, pl.ds(p, 1), :] = whole
            if r + 1 < ROUNDS:
                xs[r + 1][pl.ds(p, 1), :] = whole

    def turn(r):
        product(r, 0, GMAX)
        n = r + 1
        if n < ROUNDS:
            packet(n, urgent, ys.at[r, pl.ds(0, GMAX), :]).start()
        product(r, GMAX, BDEV)
        if n < ROUNDS:
            for k in range(1, 4):
                q = lax.rem(urgent + k, 4)
                for g in range(GMAX):
                    sends[n, k, pl.ds(g, 1), :] = ys[r, pl.ds(pick_s[q * GMAX + g], 1), :]
                packet(n, q, sends.at[n, k]).start()

    small[0].wait()
    small[1].wait()
    for q in ORDER:
        for g in range(GMAX):
            sends[0, q, pl.ds(g, 1), :] = conc_in[pl.ds(lists_s[0, q, g], 1), :]
    pl.semaphore_wait(barrier, greetings)
    for q in ORDER:
        relayed = me + OFFSETS[q] < 0
        slot = q + 2 * me
        pltpu.make_async_remote_copy(
            src_ref=sends.at[0, q],
            dst_ref=xs[0].at[
                pl.ds(
                    pl.multiple_of(
                        jnp.where(relayed, RELAY_ROW + slot * GMAX, BDEV + q * GMAX), 8
                    ),
                    GMAX,
                ),
                :,
            ],
            send_sem=send_sems.at[0, q],
            recv_sem=recv_sems.at[jnp.where(relayed, ROUNDS, 0), jnp.where(relayed, slot, q)],
            device_id=(jnp.where(relayed, RELAY_A, near(OFFSETS[q])),),
            device_id_type=MESH,
        ).start()

    def forward(i):
        before_end, q = RELAYED[i]
        first = me == RELAY_A
        here = xs[0].at[pl.ds(RELAY_ROW + i * GMAX, GMAX), :]
        row = jnp.where(first, RELAY_ROW + i * GMAX, BDEV + q * GMAX)
        return pltpu.make_async_remote_copy(
            src_ref=here,
            dst_ref=xs[0].at[pl.ds(pl.multiple_of(row, 8), GMAX), :],
            send_sem=relay_sems.at[i],
            recv_sem=recv_sems.at[jnp.where(first, ROUNDS, 0), jnp.where(first, i, q)],
            device_id=(jnp.where(first, RELAY_B, ndev - before_end),),
            device_id_type=MESH,
        )

    is_relay = (me == RELAY_A) | (me == RELAY_B)

    @pl.when(is_relay)
    def _():
        for i in range(len(RELAYED)):
            here = xs[0].at[pl.ds(RELAY_ROW + i * GMAX, GMAX), :]
            pltpu.make_async_copy(here, here, recv_sems.at[ROUNDS, i]).wait()
            forward(i).start()

    for o in z_line:
        pl.semaphore_signal(known_z, inc=1, device_id=(at(o),), device_id_type=MESH)
    for x in xs:
        x[pl.ds(ZERO_ROW, 8), :] = jnp.zeros((8, BLK), jnp.float32)
    for copy in small[2:]:
        copy.wait()

    def find(b, others):
        found = 0
        for g in range(GMAX):
            found = jnp.where(lists_s[0, urgent, g] == b, g + 1, found)
        place_s[b] = jnp.where(found > 0, found - 1, jnp.minimum(GMAX + others, BDEV - 1))
        return others + jnp.where(found > 0, 0, 1)

    lax.fori_loop(0, BDEV, find, 0)

    def order(p, carry):
        b = 0
        for i in range(BDEV):
            b = jnp.where(place_s[i] == p, i, b)
        row_s[p] = b
        conc[pl.ds(p, 1), :] = conc_in[pl.ds(b, 1), :]
        rate[pl.ds(p, 1), :] = rate_in[pl.ds(b, 1), :]
        xs[0][pl.ds(p, 1), :] = conc_in[pl.ds(b, 1), :]
        length = lens_s[b]
        for t in range(1, NNZB):
            col = cols_s[t, b]
            moved = jnp.where(col < BDEV, place_s[jnp.clip(col, 0, BDEV - 1)], jnp.minimum(col, ZERO_ROW))
            index_s[p * NNZB + t] = jnp.where(t < length, moved, ZERO_ROW)
        return carry

    lax.fori_loop(0, BDEV, order, 0)

    def choose(g, carry):
        for q in range(4):
            pick_s[q * GMAX + g] = place_s[lists_s[0, q, g]]
        return carry

    lax.fori_loop(0, GMAX, choose, 0)
    slope8[...] = rate[...] * (1.0 - 2.0 * conc[...]) + SHIFT
    for chunk in chunks:
        chunk.wait()
    own_part(0)
    await_ghosts(0)
    turn(0)

    def broadcast_gram(slot, products):
        rows = [jnp.sum(p, axis=0, keepdims=True) for p in products]
        rows = rows + [jnp.zeros((BLK - len(rows), BLK), jnp.float32)]
        gram_row[slot] = jnp.sum(jnp.concatenate(rows, axis=0).T, axis=0, keepdims=True)
        for k in range(ndev - 1):
            pltpu.make_async_remote_copy(
                src_ref=gram_row.at[slot],
                dst_ref=arrivals.at[slot, me],
                send_sem=ar_send.at[slot],
                recv_sem=ar_recv.at[slot],
                device_id=(jnp.where(me <= k, k + 1, k),),
                device_id_type=MESH,
            ).start()

    def collect_gram(slot):
        whole = arrivals.at[slot, pl.ds(0, ndev - 1)]
        pltpu.make_async_copy(whole, whole, ar_recv.at[slot]).wait()
        arrivals[slot, me] = gram_row[slot]
        total = jnp.sum(arrivals[slot], axis=0)
        return {
            pair: jnp.broadcast_to(total[:, e : e + 1], (1, BLK)) for e, pair in enumerate(PAIRS)
        }

    substep = jnp.full((1, BLK), step_s[0] * 0.5, jnp.float32)
    us = None
    for r in range(1, ROUNDS):
        if r == 1:
            pl.semaphore_wait(known_z, 3)
            for o in y_line:
                pl.semaphore_signal(known_y, inc=1, device_id=(at(o),), device_id_type=MESH)
        own_part(r)
        if r == 4:
            pl.semaphore_wait(known_y, 3)
            w = [ys[k] for k in range(4)]
            broadcast_gram(0, [w[i] * w[j] for i, j in PAIRS])
        if r == ROUNDS - 1:
            w = [ys[k] for k in range(6)]
            first_weights = arnoldi_weights(collect_gram(0), substep)
            d = [None] * 4
            for k in range(4):
                term = None
                if k > 0:
                    term = first_weights[k - 1] * (1.0 / SCALE)
                if k < 3:
                    low = first_weights[k] * SHIFT
                    term = -low if term is None else term - low
                d[k] = term
            d[0] = d[0] + 1.0
            us = [d[0] * w[k] + d[1] * w[k + 1] + d[2] * w[k + 2] + d[3] * w[k + 3] for k in range(3)]
            tail = d[0] * w[3] + d[1] * w[4] + d[2] * w[5]
            partial = [us[i] * us[j] for i, j in PAIRS[:6]]
            base = (
                conc[...] + first_weights[0] * w[0] + first_weights[1] * w[1] + first_weights[2] * w[2]
            )
        await_ghosts(r)
        turn(r)
    last = tail + d[3] * ys[ROUNDS - 1]
    broadcast_gram(1, partial + [us[i] * last for i in range(3)])
    second = arnoldi_weights(collect_gram(1), substep)
    ordered[...] = base + second[0] * us[0] + second[1] * us[1] + second[2] * us[2]
    for b in range(BDEV):
        result[pl.ds(b, 1), :] = ordered[pl.ds(place_s[b], 1), :]
    for r in range(ROUNDS):
        for q in range(4):
            packet(r, q, sends.at[0, 0]).wait_send()

    @pl.when(is_relay)
    def _():
        for i in range(len(RELAYED)):
            forward(i).wait_send()

    for slot in range(2):
        whole = arrivals.at[slot, pl.ds(0, ndev - 1)]
        pltpu.make_async_copy(whole, whole, ar_send.at[slot]).wait()


def solution(mesh):
    ndev = mesh.shape["dom"]

    def step(conc, rate, size, blocks, cols, lens, lists):
        f32, i32 = jnp.float32, jnp.int32
        return pl.pallas_call(
            lambda *refs: kernel(ndev, *refs),
            out_shape=pltpu.VMEM((BDEV, BLK), f32),
            in_specs=[pl.BlockSpec(memory_space=pl.ANY)] * 7,
            out_specs=pl.BlockSpec(memory_space=pltpu.VMEM),
            scratch_shapes=[
                pltpu.VMEM((BDEV, BLK), f32),
                pltpu.VMEM((BDEV, BLK), f32),
                pltpu.VMEM((BDEV, BLK), f32),
                pltpu.VMEM((BDEV, BLK), f32),
                pltpu.VMEM((BDEV, BLK), f32),
                pltpu.VMEM((BDEV, BLK), f32),
                pltpu.VMEM((BDEV, NNZB, BLK, BLK), f32),
                pltpu.VMEM((ROUNDS, BDEV, BLK), f32),
                pltpu.VMEM((ROUNDS, 4, GMAX, BLK), f32),
                pltpu.VMEM((2, 1, BLK), f32),
                pltpu.VMEM((2, ndev, 1, BLK), f32),
                pltpu.VMEM((BDEV, BLK), f32),
                pltpu.SMEM((1,), f32),
                pltpu.SMEM((NNZB, BDEV), i32),
                pltpu.SMEM((BDEV,), i32),
                pltpu.SMEM((1, 4, GMAX), i32),
                pltpu.SMEM((BDEV * NNZB,), i32),
                pltpu.SMEM((BDEV,), i32),
                pltpu.SMEM((BDEV,), i32),
                pltpu.SMEM((4 * GMAX,), i32),
            ]
            + [pltpu.VMEM((XROWS + len(RELAYED) * GMAX, BLK), f32)]
            + [pltpu.VMEM((XROWS, BLK), f32)] * (ROUNDS - 1)
            + [
                pltpu.SemaphoreType.DMA((6,)),
                pltpu.SemaphoreType.DMA((BDEV // CHUNK,)),
                pltpu.SemaphoreType.DMA((ROUNDS, 4)),
                pltpu.SemaphoreType.DMA((ROUNDS + 1, 4)),
                pltpu.SemaphoreType.DMA((2,)),
                pltpu.SemaphoreType.DMA((2,)),
                pltpu.SemaphoreType.DMA((len(RELAYED),)),
                pltpu.SemaphoreType.REGULAR,
                pltpu.SemaphoreType.REGULAR,
            ],
            compiler_params=pltpu.CompilerParams(collective_id=0, has_side_effects=True),
            name="rosenbrock",
        )(conc, rate, size, blocks, cols.T, lens, lists)

    dom = "dom"
    return jax.shard_map(
        step,
        mesh=mesh,
        in_specs=(P(dom), P(dom), P(), P(dom), P(dom), P(dom), P(dom)),
        out_specs=P(dom),
        check_vma=False,
    )
```

```python
import jax
import jax.numpy as jnp
from jax import lax
from jax.experimental import pallas as pl
from jax.experimental.pallas import tpu as pltpu
from jax.sharding import PartitionSpec as P

BLK = 128
BDEV = 32
NNZB = 5
GMAX = 16
OFFSETS = (-2, -1, 1, 2)
ORDER = (0, 3, 1, 2)
EPS = 1e-6
SHIFT = 8.0
SCALE = 0.25
ROUNDS = 7
GROUP = 8
CHUNK = 4
ZERO_ROW = BDEV + 4 * GMAX
XROWS = ZERO_ROW + 8
RELAY_ROW = XROWS
RELAY_A = 7
RELAY_B = 103
RELAYED = ((2, 0), (1, 1), (1, 0))
PAIRS = ((0, 0), (0, 1), (0, 2), (1, 1), (1, 2), (2, 2), (0, 3), (1, 3), (2, 3))
MESH = pl.DeviceIdType.MESH


def arnoldi_weights(gram, substep):
    G = {}
    for (i, j), g in gram.items():
        G[i, j] = g
        G[j, i] = g
    zero = jnp.zeros_like(substep)
    magnitude = jnp.sqrt(G[0, 0] + EPS)
    vectors = [[1.0 / magnitude]]
    H = [[None] * 3 for _ in range(3)]
    for col in range(3):
        v = vectors[col]
        n = len(v)
        mapped = [None] * (n + 1)
        for k in range(n + 1):
            term = None
            if k > 0:
                term = v[k - 1] * (1.0 / SCALE)
            if k < n:
                low = v[k] * SHIFT
                term = -low if term is None else term - low
            mapped[k] = term
        image = []
        for i in range(n):
            total = G[i, 0] * mapped[0]
            for k in range(1, n + 1):
                total = total + G[i, k] * mapped[k]
            image.append(total)
        projections = []
        for vec in vectors:
            total = vec[0] * image[0]
            for k in range(1, len(vec)):
                total = total + vec[k] * image[k]
            projections.append(total)
        for k, p in enumerate(projections):
            H[k][col] = p
        if col < 2:
            rest = list(mapped)
            for p, vec in zip(projections, vectors):
                for k in range(len(vec)):
                    rest[k] = rest[k] - p * vec[k]
            square = None
            for i in range(n + 1):
                total = G[i, 0] * rest[0]
                for k in range(1, n + 1):
                    total = total + G[i, k] * rest[k]
                total = total * rest[i]
                square = total if square is None else square + total
            length = jnp.sqrt(square + EPS)
            H[col + 1][col] = length
            inverse = 1.0 / length
            vectors.append([r * inverse for r in rest])
    small = substep * (1.0 / 64.0)
    A = [[None if H[i][j] is None else H[i][j] * small for j in range(3)] for i in range(3)]
    one = jnp.ones_like(substep)
    Pm = [[one if i == j else zero for j in range(3)] for i in range(3)]
    q = [zero] * 3
    for degree in range(12, 0, -1):
        inv = 1.0 / degree
        newP = [[None] * 3 for _ in range(3)]
        newq = [None] * 3
        for i in range(3):
            ks = [k for k in range(3) if A[i][k] is not None]
            for j in range(3):
                total = A[i][ks[0]] * Pm[ks[0]][j]
                for k in ks[1:]:
                    total = total + A[i][k] * Pm[k][j]
                total = total * inv
                newP[i][j] = total + 1.0 if i == j else total
            total = A[i][ks[0]] * q[ks[0]]
            for k in ks[1:]:
                total = total + A[i][k] * q[k]
            if i == 0:
                total = total + (1.0 / 64.0)
            newq[i] = total * inv
        Pm, q = newP, newq
    for _ in range(6):
        newP = [[Pm[i][0] * Pm[0][j] + Pm[i][1] * Pm[1][j] + Pm[i][2] * Pm[2][j] for j in range(3)] for i in range(3)]
        q = [Pm[i][0] * q[0] + Pm[i][1] * q[1] + Pm[i][2] * q[2] + q[i] for i in range(3)]
        Pm = newP
    out = []
    for k in range(3):
        total = None
        for col in range(k, 3):
            term = q[col] * vectors[col][k]
            total = term if total is None else total + term
        out.append(total * (substep * magnitude))
    return out


def kernel(ndev, conc_hbm, rate_hbm, step_hbm, blocks_hbm, cols_hbm, lens_hbm, lists_hbm, result, *scratch):
    (conc_in, rate_in, conc, rate, slope8, fixed, blocks, ys, sends, gram_row, arrivals, ordered) = scratch[:12]
    (step_s, cols_s, lens_s, lists_s, index_s, place_s, row_s, pick_s) = scratch[12:20]
    xs = scratch[20 : 20 + ROUNDS]
    in_sems, block_sem, send_sem, recv_sems, ar_send, ar_recv, relay_sem, known = scratch[20 + ROUNDS :]
    me = lax.axis_index("dom")

    def near(o):
        return lax.rem(me + (o + ndev), ndev)

    my_core, my_x = lax.rem(me, 2), lax.rem(me // 2, 4)
    urgent = jnp.where(my_x < 2, 0, 3 - my_core)

    small = [
        pltpu.make_async_copy(lists_hbm, lists_s, in_sems.at[0]),
        pltpu.make_async_copy(conc_hbm, conc_in, in_sems.at[1]),
        pltpu.make_async_copy(cols_hbm, cols_s, in_sems.at[2]),
        pltpu.make_async_copy(lens_hbm, lens_s, in_sems.at[3]),
        pltpu.make_async_copy(rate_hbm, rate_in, in_sems.at[4]),
        pltpu.make_async_copy(step_hbm, step_s, in_sems.at[5]),
    ]
    for copy in small:
        copy.start()

    barrier = pltpu.get_barrier_semaphore()

    def greet(device):
        pl.semaphore_signal(barrier, inc=1, device_id=(device,), device_id_type=MESH)

    for q in ORDER:
        greet(jnp.where(me + OFFSETS[q] >= ndev, RELAY_B, near(OFFSETS[q])))

    @pl.when(me == RELAY_A)
    def _():
        greet(0)
        greet(1)

    @pl.when(me == RELAY_B)
    def _():
        greet(RELAY_A)

    greetings = (
        4
        + jnp.where(me == RELAY_B, 3, 0)
        + jnp.where(me == RELAY_A, 1, 0)
        - jnp.where(me == 0, 1, 0)
    )

    for c in range(BDEV // CHUNK):
        part = pl.ds(c * CHUNK, CHUNK)
        pltpu.make_async_copy(blocks_hbm.at[part], blocks.at[part], block_sem).start()

    def packet(r, q, source):
        offset = jnp.where(q < 2, q - 2, q - 1)
        return pltpu.make_async_remote_copy(
            src_ref=source,
            dst_ref=xs[r].at[pl.ds(pl.multiple_of(BDEV + q * GMAX, 8), GMAX), :],
            send_sem=send_sem,
            recv_sem=recv_sems.at[r],
            device_id=(lax.rem(me + offset + ndev, ndev),),
            device_id_type=MESH,
        )

    def await_ghosts(r):
        part = xs[r].at[pl.ds(BDEV, 4 * GMAX), :]
        pltpu.make_async_copy(part, part, recv_sems.at[r]).wait()

    def lane_sums(total):
        return jnp.sum(total.T, axis=0, keepdims=True)

    def own_part(r):
        source = conc if r == 0 else ys.at[r - 1]

        def group(i, carry):
            for s in range(GROUP):
                p = i * GROUP + s
                mine = source[pl.ds(p, 1), :]
                here = lane_sums(blocks[row_s[p], 0] * mine)
                if r == 0:
                    kept = rate[pl.ds(p, 1), :] * mine * (1.0 - mine)
                else:
                    kept = slope8[pl.ds(p, 1), :] * mine
                fixed[pl.ds(p, 1), :] = kept - here
            return carry

        lax.fori_loop(0, BDEV // GROUP, group, 0)

    def product(r, low, high):
        x = xs[r]
        for p in range(low, high):
            total = None
            b = row_s[p]
            for t in range(1, NNZB):
                row = x[pl.ds(index_s[p * NNZB + t], 8, stride=0), :]
                term = blocks[b, t].reshape(16, 8, BLK) * row[None]
                total = term if total is None else total + term
            whole = fixed[pl.ds(p, 1), :] - lane_sums(total.reshape(BLK, BLK))
            whole = whole if r == 0 else whole * SCALE
            ys[r, pl.ds(p, 1), :] = whole
            if r + 1 < ROUNDS:
                xs[r + 1][pl.ds(p, 1), :] = whole

    def turn(r):
        product(r, 0, GMAX)
        n = r + 1
        if n < ROUNDS:
            packet(n, urgent, ys.at[r, pl.ds(0, GMAX), :]).start()
        product(r, GMAX, BDEV)
        if n < ROUNDS:
            for k in range(1, 4):
                q = lax.rem(urgent + k, 4)
                for g in range(GMAX):
                    sends[n, k, pl.ds(g, 1), :] = ys[r, pl.ds(pick_s[q * GMAX + g], 1), :]
                packet(n, q, sends.at[n, k]).start()

    small[0].wait()
    small[1].wait()
    for q in ORDER:
        for g in range(GMAX):
            sends[0, q, pl.ds(g, 1), :] = conc_in[pl.ds(lists_s[0, q, g], 1), :]
    pl.semaphore_wait(barrier, greetings)
    for q in ORDER:
        relayed = me + OFFSETS[q] < 0
        slot = q + 2 * me
        pltpu.make_async_remote_copy(
            src_ref=sends.at[0, q],
            dst_ref=xs[0].at[
                pl.ds(
                    pl.multiple_of(
                        jnp.where(relayed, RELAY_ROW + slot * GMAX, BDEV + q * GMAX), 8
                    ),
                    GMAX,
                ),
                :,
            ],
            send_sem=send_sem,
            recv_sem=recv_sems.at[jnp.where(relayed, ROUNDS, 0)],
            device_id=(jnp.where(relayed, RELAY_A, near(OFFSETS[q])),),
            device_id_type=MESH,
        ).start()

    def forward(i):
        before_end, q = RELAYED[i]
        first = me == RELAY_A
        here = xs[0].at[pl.ds(RELAY_ROW + i * GMAX, GMAX), :]
        row = jnp.where(first, RELAY_ROW + i * GMAX, BDEV + q * GMAX)
        return pltpu.make_async_remote_copy(
            src_ref=here,
            dst_ref=xs[0].at[pl.ds(pl.multiple_of(row, 8), GMAX), :],
            send_sem=relay_sem,
            recv_sem=recv_sems.at[jnp.where(first, ROUNDS, 0)],
            device_id=(jnp.where(first, RELAY_B, ndev - before_end),),
            device_id_type=MESH,
        )

    relay_part = xs[0].at[pl.ds(RELAY_ROW, len(RELAYED) * GMAX), :]
    is_relay = (me == RELAY_A) | (me == RELAY_B)

    @pl.when(is_relay)
    def _():
        pltpu.make_async_copy(relay_part, relay_part, recv_sems.at[ROUNDS]).wait()
        for i in range(len(RELAYED)):
            forward(i).start()

    for x in xs:
        x[pl.ds(ZERO_ROW, 8), :] = jnp.zeros((8, BLK), jnp.float32)
    for copy in small[2:]:
        copy.wait()

    def find(b, others):
        found = 0
        for g in range(GMAX):
            found = jnp.where(lists_s[0, urgent, g] == b, g + 1, found)
        place_s[b] = jnp.where(found > 0, found - 1, jnp.minimum(GMAX + others, BDEV - 1))
        return others + jnp.where(found > 0, 0, 1)

    lax.fori_loop(0, BDEV, find, 0)
    for c in range(BDEV, ZERO_ROW):
        place_s[c] = c

    def settle(p, b):
        row_s[p] = b
        conc[pl.ds(p, 1), :] = conc_in[pl.ds(b, 1), :]
        rate[pl.ds(p, 1), :] = rate_in[pl.ds(b, 1), :]
        xs[0][pl.ds(p, 1), :] = conc_in[pl.ds(b, 1), :]
        length = lens_s[b]
        for t in range(1, NNZB):
            index_s[p * NNZB + t] = jnp.where(t < length, place_s[cols_s[t, b]], ZERO_ROW)

    def settle_pair(g, carry):
        settle(g, lists_s[0, urgent, g])
        b = g
        for i in range(1, GMAX + 1):
            b = jnp.where(place_s[g + i] == GMAX + g, g + i, b)
        settle(GMAX + g, b)
        return carry

    lax.fori_loop(0, GMAX, settle_pair, 0)

    def choose(g, carry):
        for q in range(4):
            pick_s[q * GMAX + g] = place_s[lists_s[0, q, g]]
        return carry

    lax.fori_loop(0, GMAX, choose, 0)
    slope8[...] = rate[...] * (1.0 - 2.0 * conc[...]) + SHIFT
    pltpu.make_async_copy(blocks, blocks, block_sem).wait()
    own_part(0)
    await_ghosts(0)
    turn(0)

    lane = lax.broadcasted_iota(jnp.int32, (1, BLK), 1)

    def sums_row(products, first, row):
        for e, p in enumerate(products, first):
            total = jnp.sum(jnp.sum(p, axis=0, keepdims=True), axis=1, keepdims=True)
            row = jnp.where(lane == e, total, row)
        return row

    def broadcast_gram(slot, row):
        gram_row[slot] = row
        for k in range(ndev - 1):
            pltpu.make_async_remote_copy(
                src_ref=gram_row.at[slot],
                dst_ref=arrivals.at[slot, me],
                send_sem=ar_send,
                recv_sem=ar_recv.at[slot],
                device_id=(jnp.where(me <= k, k + 1, k),),
                device_id_type=MESH,
            ).start()

    def collect_gram(slot):
        whole = arrivals.at[slot, pl.ds(0, ndev - 1)]
        with jax.named_scope(f"collect{slot}"):
            pltpu.make_async_copy(whole, whole, ar_recv.at[slot]).wait()
        arrivals[slot, me] = gram_row[slot]
        parts = [arrivals[slot, i] for i in range(ndev)]
        while len(parts) > 1:
            parts = [a + b for a, b in zip(parts[::2], parts[1::2])]
        total = parts[0]
        return {
            pair: jnp.broadcast_to(total[:, e : e + 1], (1, BLK)) for e, pair in enumerate(PAIRS)
        }

    def meet(step):
        for o in (2 << step, -(2 << step)):
            pl.semaphore_signal(known.at[step], inc=1, device_id=(near(o),), device_id_type=MESH)

    zero_row = jnp.zeros((1, BLK), jnp.float32)
    meet(0)
    substep = jnp.full((1, BLK), step_s[0] * 0.5, jnp.float32)
    us = None
    for r in range(1, ROUNDS):
        if r <= 4:
            pl.semaphore_wait(known.at[r - 1], 2)
            meet(r)
        own_part(r)
        if r == 4:
            pl.semaphore_wait(known.at[4], 2)
            w = [ys[k] for k in range(4)]
            broadcast_gram(0, sums_row([w[i] * w[j] for i, j in PAIRS], 0, zero_row))
        if r == ROUNDS - 1:
            w = [ys[k] for k in range(6)]
            first_weights = arnoldi_weights(collect_gram(0), substep)
            d = [None] * 4
            for k in range(4):
                term = None
                if k > 0:
                    term = first_weights[k - 1] * (1.0 / SCALE)
                if k < 3:
                    low = first_weights[k] * SHIFT
                    term = -low if term is None else term - low
                d[k] = term
            d[0] = d[0] + 1.0
            us = [d[0] * w[k] + d[1] * w[k + 1] + d[2] * w[k + 2] + d[3] * w[k + 3] for k in range(3)]
            tail = d[0] * w[3] + d[1] * w[4] + d[2] * w[5]
            partial = sums_row([us[i] * us[j] for i, j in PAIRS[:6]], 0, zero_row)
            base = (
                conc[...] + first_weights[0] * w[0] + first_weights[1] * w[1] + first_weights[2] * w[2]
            )
        await_ghosts(r)
        turn(r)
    last = tail + d[3] * ys[ROUNDS - 1]
    broadcast_gram(1, sums_row([us[i] * last for i in range(3)], 6, partial))
    second = arnoldi_weights(collect_gram(1), substep)
    ordered[...] = base + second[0] * us[0] + second[1] * us[1] + second[2] * us[2]
    for b in range(BDEV):
        result[pl.ds(b, 1), :] = ordered[pl.ds(place_s[b], 1), :]
    pltpu.make_async_copy(sends, sends, send_sem).wait()

    @pl.when(is_relay)
    def _():
        pltpu.make_async_copy(relay_part, relay_part, relay_sem).wait()

    whole = arrivals.at[:, pl.ds(0, ndev - 1)]
    pltpu.make_async_copy(whole, whole, ar_send).wait()


def solution(mesh):
    ndev = mesh.shape["dom"]

    def step(conc, rate, size, blocks, cols, lens, lists):
        f32, i32 = jnp.float32, jnp.int32
        return pl.pallas_call(
            lambda *refs: kernel(ndev, *refs),
            out_shape=pltpu.VMEM((BDEV, BLK), f32),
            in_specs=[pl.BlockSpec(memory_space=pl.ANY)] * 7,
            out_specs=pl.BlockSpec(memory_space=pltpu.VMEM),
            scratch_shapes=[
                pltpu.VMEM((BDEV, BLK), f32),
                pltpu.VMEM((BDEV, BLK), f32),
                pltpu.VMEM((BDEV, BLK), f32),
                pltpu.VMEM((BDEV, BLK), f32),
                pltpu.VMEM((BDEV, BLK), f32),
                pltpu.VMEM((BDEV, BLK), f32),
                pltpu.VMEM((BDEV, NNZB, BLK, BLK), f32),
                pltpu.VMEM((ROUNDS, BDEV, BLK), f32),
                pltpu.VMEM((ROUNDS, 4, GMAX, BLK), f32),
                pltpu.VMEM((2, 1, BLK), f32),
                pltpu.VMEM((2, ndev, 1, BLK), f32),
                pltpu.VMEM((BDEV, BLK), f32),
                pltpu.SMEM((1,), f32),
                pltpu.SMEM((NNZB, BDEV), i32),
                pltpu.SMEM((BDEV,), i32),
                pltpu.SMEM((1, 4, GMAX), i32),
                pltpu.SMEM((BDEV * NNZB,), i32),
                pltpu.SMEM((ZERO_ROW,), i32),
                pltpu.SMEM((BDEV,), i32),
                pltpu.SMEM((4 * GMAX,), i32),
            ]
            + [pltpu.VMEM((XROWS + len(RELAYED) * GMAX, BLK), f32)]
            + [pltpu.VMEM((XROWS, BLK), f32)] * (ROUNDS - 1)
            + [
                pltpu.SemaphoreType.DMA((6,)),
                pltpu.SemaphoreType.DMA,
                pltpu.SemaphoreType.DMA,
                pltpu.SemaphoreType.DMA((ROUNDS + 1,)),
                pltpu.SemaphoreType.DMA,
                pltpu.SemaphoreType.DMA((2,)),
                pltpu.SemaphoreType.DMA,
                pltpu.SemaphoreType.REGULAR((5,)),
            ],
            compiler_params=pltpu.CompilerParams(collective_id=0, has_side_effects=True),
            name="rosenbrock",
        )(conc, rate, size, blocks, cols.T, lens, lists)

    dom = "dom"
    return jax.shard_map(
        step,
        mesh=mesh,
        in_specs=(P(dom), P(dom), P(), P(dom), P(dom), P(dom), P(dom)),
        out_specs=P(dom),
        check_vma=False,
    )
```

```python
import jax
import jax.numpy as jnp
from jax import lax
from jax.experimental import pallas as pl
from jax.experimental.pallas import tpu as pltpu
from jax.sharding import PartitionSpec as P

BLK = 128
BDEV = 32
NNZB = 5
GMAX = 16
OFFSETS = (-2, -1, 1, 2)
ORDER = (0, 3, 1, 2)
EPS = 1e-6
SHIFT = 8.0
SCALE = 0.25
ROUNDS = 7
GROUP = 8
CHUNK = 4
ZERO_ROW = BDEV + 4 * GMAX
XROWS = ZERO_ROW + 8
RELAY_ROW = XROWS
RELAY_A = 7
RELAY_B = 103
RELAYED = ((2, 0), (1, 1), (1, 0))
PAIRS = ((0, 0), (0, 1), (0, 2), (1, 1), (1, 2), (2, 2), (0, 3), (1, 3), (2, 3))
MESH = pl.DeviceIdType.MESH


def arnoldi_weights(gram, substep):
    G = {}
    for (i, j), g in gram.items():
        G[i, j] = g
        G[j, i] = g
    zero = jnp.zeros_like(substep)
    magnitude = jnp.sqrt(G[0, 0] + EPS)
    vectors = [[1.0 / magnitude]]
    H = [[None] * 3 for _ in range(3)]
    for col in range(3):
        v = vectors[col]
        n = len(v)
        mapped = [None] * (n + 1)
        for k in range(n + 1):
            term = None
            if k > 0:
                term = v[k - 1] * (1.0 / SCALE)
            if k < n:
                low = v[k] * SHIFT
                term = -low if term is None else term - low
            mapped[k] = term
        image = []
        for i in range(n):
            total = G[i, 0] * mapped[0]
            for k in range(1, n + 1):
                total = total + G[i, k] * mapped[k]
            image.append(total)
        projections = []
        for vec in vectors:
            total = vec[0] * image[0]
            for k in range(1, len(vec)):
                total = total + vec[k] * image[k]
            projections.append(total)
        for k, p in enumerate(projections):
            H[k][col] = p
        if col < 2:
            rest = list(mapped)
            for p, vec in zip(projections, vectors):
                for k in range(len(vec)):
                    rest[k] = rest[k] - p * vec[k]
            square = None
            for i in range(n + 1):
                total = G[i, 0] * rest[0]
                for k in range(1, n + 1):
                    total = total + G[i, k] * rest[k]
                total = total * rest[i]
                square = total if square is None else square + total
            length = jnp.sqrt(square + EPS)
            H[col + 1][col] = length
            inverse = 1.0 / length
            vectors.append([r * inverse for r in rest])
    small = substep * (1.0 / 64.0)
    A = [[None if H[i][j] is None else H[i][j] * small for j in range(3)] for i in range(3)]
    sublane = lax.broadcasted_iota(jnp.int32, substep.shape, 0)
    unit = [jnp.where(sublane == i, 1.0, 0.0) for i in range(4)]
    rows = unit[:3]
    for degree in range(12, 0, -1):
        new = []
        for i in range(3):
            total = unit[3] * (1.0 / 64.0) if i == 0 else None
            for k in range(3):
                if A[i][k] is not None:
                    term = A[i][k] * rows[k]
                    total = term if total is None else total + term
            new.append(unit[i] + total * (1.0 / degree))
        rows = new

    def column(row, k):
        return jnp.broadcast_to(row[k : k + 1, :], substep.shape)

    for _ in range(6):
        rows = [
            column(row, 0) * rows[0]
            + column(row, 1) * rows[1]
            + (column(row, 2) * rows[2] + unit[3] * row)
            for row in rows
        ]
    q = [column(row, 3) for row in rows]
    out = []
    for k in range(3):
        total = None
        for col in range(k, 3):
            term = q[col] * vectors[col][k]
            total = term if total is None else total + term
        out.append(total * (substep * magnitude))
    return out


def kernel(ndev, conc_hbm, rate_hbm, step_hbm, blocks_hbm, cols_hbm, lens_hbm, lists_hbm, result, *scratch):
    (conc_in, rate_in, conc, rate, slope8, fixed, blocks, ys, sends, gram_row, arrivals, ordered) = scratch[:12]
    (step_s, cols_s, lens_s, lists_s, index_s, place_s, row_s, pick_s) = scratch[12:20]
    xs = scratch[20 : 20 + ROUNDS]
    in_sems, block_sem, send_sem, recv_sems, ar_send, ar_recv, relay_sem, known = scratch[20 + ROUNDS :]
    me = lax.axis_index("dom")

    def near(o):
        return lax.rem(me + (o + ndev), ndev)

    my_core, my_x = lax.rem(me, 2), lax.rem(me // 2, 4)
    urgent = jnp.where(my_x < 2, 0, 3 - my_core)

    small = [
        pltpu.make_async_copy(lists_hbm, lists_s, in_sems.at[0]),
        pltpu.make_async_copy(conc_hbm, conc_in, in_sems.at[1]),
        pltpu.make_async_copy(cols_hbm, cols_s, in_sems.at[2]),
        pltpu.make_async_copy(lens_hbm, lens_s, in_sems.at[3]),
        pltpu.make_async_copy(rate_hbm, rate_in, in_sems.at[4]),
        pltpu.make_async_copy(step_hbm, step_s, in_sems.at[5]),
    ]
    for copy in small:
        copy.start()

    barrier = pltpu.get_barrier_semaphore()

    def greet(device):
        pl.semaphore_signal(barrier, inc=1, device_id=(device,), device_id_type=MESH)

    for q in ORDER:
        greet(jnp.where(me + OFFSETS[q] >= ndev, RELAY_B, near(OFFSETS[q])))

    @pl.when(me == RELAY_A)
    def _():
        greet(0)
        greet(1)

    @pl.when(me == RELAY_B)
    def _():
        greet(RELAY_A)

    greetings = (
        4
        + jnp.where(me == RELAY_B, 3, 0)
        + jnp.where(me == RELAY_A, 1, 0)
        - jnp.where(me == 0, 1, 0)
    )

    for c in range(BDEV // CHUNK):
        part = pl.ds(c * CHUNK, CHUNK)
        pltpu.make_async_copy(blocks_hbm.at[part], blocks.at[part], block_sem).start()

    def packet(r, q, source):
        offset = jnp.where(q < 2, q - 2, q - 1)
        return pltpu.make_async_remote_copy(
            src_ref=source,
            dst_ref=xs[r].at[pl.ds(pl.multiple_of(BDEV + q * GMAX, 8), GMAX), :],
            send_sem=send_sem,
            recv_sem=recv_sems.at[r],
            device_id=(lax.rem(me + offset + ndev, ndev),),
            device_id_type=MESH,
        )

    def await_ghosts(r):
        part = xs[r].at[pl.ds(BDEV, 4 * GMAX), :]
        pltpu.make_async_copy(part, part, recv_sems.at[r]).wait()

    def lane_sums(total):
        return jnp.sum(total.T, axis=0, keepdims=True)

    def own_part(r):
        source = conc if r == 0 else ys.at[r - 1]

        def group(i, carry):
            for s in range(GROUP):
                p = i * GROUP + s
                mine = source[pl.ds(p, 1), :]
                here = lane_sums(blocks[row_s[p], 0] * mine)
                if r == 0:
                    kept = rate[pl.ds(p, 1), :] * mine * (1.0 - mine)
                else:
                    kept = slope8[pl.ds(p, 1), :] * mine
                fixed[pl.ds(p, 1), :] = kept - here
            return carry

        lax.fori_loop(0, BDEV // GROUP, group, 0)

    def product(r, low, high):
        x = xs[r]
        for p in range(low, high):
            total = None
            b = row_s[p]
            for t in range(1, NNZB):
                row = x[pl.ds(index_s[p * NNZB + t], 8, stride=0), :]
                term = blocks[b, t].reshape(16, 8, BLK) * row[None]
                total = term if total is None else total + term
            whole = fixed[pl.ds(p, 1), :] - lane_sums(total.reshape(BLK, BLK))
            whole = whole if r == 0 else whole * SCALE
            ys[r, pl.ds(p, 1), :] = whole
            if r + 1 < ROUNDS:
                xs[r + 1][pl.ds(p, 1), :] = whole

    def turn(r):
        product(r, 0, GMAX)
        n = r + 1
        if n < ROUNDS:
            packet(n, urgent, ys.at[r, pl.ds(0, GMAX), :]).start()
        product(r, GMAX, BDEV)
        if n < ROUNDS:
            for k in range(1, 4):
                q = lax.rem(urgent + k, 4)
                for g in range(GMAX):
                    sends[n, k, pl.ds(g, 1), :] = ys[r, pl.ds(pick_s[q * GMAX + g], 1), :]
                packet(n, q, sends.at[n, k]).start()

    small[0].wait()
    small[1].wait()
    for q in ORDER:
        for g in range(GMAX):
            sends[0, q, pl.ds(g, 1), :] = conc_in[pl.ds(lists_s[0, q, g], 1), :]
    pl.semaphore_wait(barrier, greetings)
    for q in ORDER:
        relayed = me + OFFSETS[q] < 0
        slot = q + 2 * me
        pltpu.make_async_remote_copy(
            src_ref=sends.at[0, q],
            dst_ref=xs[0].at[
                pl.ds(
                    pl.multiple_of(
                        jnp.where(relayed, RELAY_ROW + slot * GMAX, BDEV + q * GMAX), 8
                    ),
                    GMAX,
                ),
                :,
            ],
            send_sem=send_sem,
            recv_sem=recv_sems.at[jnp.where(relayed, ROUNDS + slot, 0)],
            device_id=(jnp.where(relayed, RELAY_A, near(OFFSETS[q])),),
            device_id_type=MESH,
        ).start()

    def forward(i):
        before_end, q = RELAYED[i]
        first = me == RELAY_A
        here = xs[0].at[pl.ds(RELAY_ROW + i * GMAX, GMAX), :]
        row = jnp.where(first, RELAY_ROW + i * GMAX, BDEV + q * GMAX)
        return pltpu.make_async_remote_copy(
            src_ref=here,
            dst_ref=xs[0].at[pl.ds(pl.multiple_of(row, 8), GMAX), :],
            send_sem=relay_sem,
            recv_sem=recv_sems.at[jnp.where(first, ROUNDS + i, 0)],
            device_id=(jnp.where(first, RELAY_B, ndev - before_end),),
            device_id_type=MESH,
        )

    relay_part = xs[0].at[pl.ds(RELAY_ROW, len(RELAYED) * GMAX), :]
    is_relay = (me == RELAY_A) | (me == RELAY_B)

    @pl.when(is_relay)
    def _():
        for i in range(len(RELAYED)):
            here = xs[0].at[pl.ds(RELAY_ROW + i * GMAX, GMAX), :]
            pltpu.make_async_copy(here, here, recv_sems.at[ROUNDS + i]).wait()
            forward(i).start()

    for x in xs:
        x[pl.ds(ZERO_ROW, 8), :] = jnp.zeros((8, BLK), jnp.float32)
    for copy in small[2:]:
        copy.wait()

    def find(b, others):
        found = 0
        for g in range(GMAX):
            found = jnp.where(lists_s[0, urgent, g] == b, g + 1, found)
        place_s[b] = jnp.where(found > 0, found - 1, jnp.minimum(GMAX + others, BDEV - 1))
        return others + jnp.where(found > 0, 0, 1)

    lax.fori_loop(0, BDEV, find, 0)
    for c in range(BDEV, ZERO_ROW):
        place_s[c] = c

    def settle(p, b):
        row_s[p] = b
        conc[pl.ds(p, 1), :] = conc_in[pl.ds(b, 1), :]
        rate[pl.ds(p, 1), :] = rate_in[pl.ds(b, 1), :]
        xs[0][pl.ds(p, 1), :] = conc_in[pl.ds(b, 1), :]
        length = lens_s[b]
        for t in range(1, NNZB):
            index_s[p * NNZB + t] = jnp.where(t < length, place_s[cols_s[t, b]], ZERO_ROW)

    def settle_pair(g, carry):
        settle(g, lists_s[0, urgent, g])
        b = g
        for i in range(1, GMAX + 1):
            b = jnp.where(place_s[g + i] == GMAX + g, g + i, b)
        settle(GMAX + g, b)
        return carry

    lax.fori_loop(0, GMAX, settle_pair, 0)

    def choose(g, carry):
        for q in range(4):
            pick_s[q * GMAX + g] = place_s[lists_s[0, q, g]]
        return carry

    lax.fori_loop(0, GMAX, choose, 0)
    slope8[...] = rate[...] * (1.0 - 2.0 * conc[...]) + SHIFT
    pltpu.make_async_copy(blocks, blocks, block_sem).wait()
    own_part(0)
    await_ghosts(0)
    turn(0)

    lane = lax.broadcasted_iota(jnp.int32, (1, BLK), 1)

    def sums_row(products, first, row):
        for e, p in enumerate(products, first):
            total = jnp.sum(jnp.sum(p, axis=0, keepdims=True), axis=1, keepdims=True)
            row = jnp.where(lane == e, total, row)
        return row

    def broadcast_gram(slot, row):
        gram_row[slot] = row
        for k in range(ndev - 1):
            pltpu.make_async_remote_copy(
                src_ref=gram_row.at[slot],
                dst_ref=arrivals.at[slot, me],
                send_sem=ar_send,
                recv_sem=ar_recv.at[slot],
                device_id=(jnp.where(me <= k, k + 1, k),),
                device_id_type=MESH,
            ).start()

    def collect_gram(slot):
        whole = arrivals.at[slot, pl.ds(0, ndev - 1)]
        with jax.named_scope(f"collect{slot}"):
            pltpu.make_async_copy(whole, whole, ar_recv.at[slot]).wait()
        arrivals[slot, me] = gram_row[slot]
        parts = [arrivals[slot, i] for i in range(ndev)]
        while len(parts) > 1:
            parts = [a + b for a, b in zip(parts[::2], parts[1::2])]
        total = parts[0]
        return {
            pair: jnp.broadcast_to(total[:, e : e + 1], (8, BLK)) for e, pair in enumerate(PAIRS)
        }

    def meet(step):
        for o in (2 << step, -(2 << step)):
            pl.semaphore_signal(known.at[step], inc=1, device_id=(near(o),), device_id_type=MESH)

    zero_row = jnp.zeros((1, BLK), jnp.float32)
    meet(0)
    substep = jnp.full((8, BLK), step_s[0] * 0.5, jnp.float32)

    def times(c, field):
        return (field.reshape(BDEV // 8, 8, BLK) * c[None]).reshape(BDEV, BLK)

    us = None
    for r in range(1, ROUNDS):
        if r <= 4:
            pl.semaphore_wait(known.at[r - 1], 2)
            meet(r)
        own_part(r)
        if r == 4:
            pl.semaphore_wait(known.at[4], 2)
            w = [ys[k] for k in range(4)]
            broadcast_gram(0, sums_row([w[i] * w[j] for i, j in PAIRS], 0, zero_row))
        if r == ROUNDS - 1:
            w = [ys[k] for k in range(6)]
            first_weights = arnoldi_weights(collect_gram(0), substep)
            d = [None] * 4
            for k in range(4):
                term = None
                if k > 0:
                    term = first_weights[k - 1] * (1.0 / SCALE)
                if k < 3:
                    low = first_weights[k] * SHIFT
                    term = -low if term is None else term - low
                d[k] = term
            d[0] = d[0] + 1.0
            us = [
                times(d[0], w[k]) + times(d[1], w[k + 1]) + times(d[2], w[k + 2]) + times(d[3], w[k + 3])
                for k in range(3)
            ]
            tail = times(d[0], w[3]) + times(d[1], w[4]) + times(d[2], w[5])
            partial = sums_row([us[i] * us[j] for i, j in PAIRS[:6]], 0, zero_row)
            base = (
                conc[...]
                + times(first_weights[0], w[0])
                + times(first_weights[1], w[1])
                + times(first_weights[2], w[2])
            )
        await_ghosts(r)
        turn(r)
    last = tail + times(d[3], ys[ROUNDS - 1])
    broadcast_gram(1, sums_row([us[i] * last for i in range(3)], 6, partial))
    second = arnoldi_weights(collect_gram(1), substep)
    ordered[...] = base + times(second[0], us[0]) + times(second[1], us[1]) + times(second[2], us[2])
    for b in range(BDEV):
        result[pl.ds(b, 1), :] = ordered[pl.ds(place_s[b], 1), :]
    pltpu.make_async_copy(sends, sends, send_sem).wait()

    @pl.when(is_relay)
    def _():
        pltpu.make_async_copy(relay_part, relay_part, relay_sem).wait()

    whole = arrivals.at[:, pl.ds(0, ndev - 1)]
    pltpu.make_async_copy(whole, whole, ar_send).wait()


def solution(mesh):
    ndev = mesh.shape["dom"]

    def step(conc, rate, size, blocks, cols, lens, lists):
        f32, i32 = jnp.float32, jnp.int32
        return pl.pallas_call(
            lambda *refs: kernel(ndev, *refs),
            out_shape=pltpu.VMEM((BDEV, BLK), f32),
            in_specs=[pl.BlockSpec(memory_space=pltpu.HBM)] * 7,
            out_specs=pl.BlockSpec(memory_space=pltpu.VMEM),
            scratch_shapes=[
                pltpu.VMEM((BDEV, BLK), f32),
                pltpu.VMEM((BDEV, BLK), f32),
                pltpu.VMEM((BDEV, BLK), f32),
                pltpu.VMEM((BDEV, BLK), f32),
                pltpu.VMEM((BDEV, BLK), f32),
                pltpu.VMEM((BDEV, BLK), f32),
                pltpu.VMEM((BDEV, NNZB, BLK, BLK), f32),
                pltpu.VMEM((ROUNDS, BDEV, BLK), f32),
                pltpu.VMEM((ROUNDS, 4, GMAX, BLK), f32),
                pltpu.VMEM((2, 1, BLK), f32),
                pltpu.VMEM((2, ndev, 1, BLK), f32),
                pltpu.VMEM((BDEV, BLK), f32),
                pltpu.SMEM((1,), f32),
                pltpu.SMEM((NNZB, BDEV), i32),
                pltpu.SMEM((BDEV,), i32),
                pltpu.SMEM((1, 4, GMAX), i32),
                pltpu.SMEM((BDEV * NNZB,), i32),
                pltpu.SMEM((ZERO_ROW,), i32),
                pltpu.SMEM((BDEV,), i32),
                pltpu.SMEM((4 * GMAX,), i32),
            ]
            + [pltpu.VMEM((XROWS + len(RELAYED) * GMAX, BLK), f32)]
            + [pltpu.VMEM((XROWS, BLK), f32)] * (ROUNDS - 1)
            + [
                pltpu.SemaphoreType.DMA((6,)),
                pltpu.SemaphoreType.DMA,
                pltpu.SemaphoreType.DMA,
                pltpu.SemaphoreType.DMA((ROUNDS + len(RELAYED),)),
                pltpu.SemaphoreType.DMA,
                pltpu.SemaphoreType.DMA((2,)),
                pltpu.SemaphoreType.DMA,
                pltpu.SemaphoreType.REGULAR((5,)),
            ],
            compiler_params=pltpu.CompilerParams(collective_id=0, has_side_effects=True),
            name="rosenbrock",
        )(conc, rate, size, blocks, cols.T, lens, lists)

    dom = "dom"
    return jax.shard_map(
        step,
        mesh=mesh,
        in_specs=(P(dom), P(dom), P(), P(dom), P(dom), P(dom), P(dom)),
        out_specs=P(dom),
        check_vma=False,
    )
```

```python
import jax
import jax.numpy as jnp
from jax import lax
from jax.experimental import pallas as pl
from jax.experimental.pallas import tpu as pltpu
from jax.sharding import PartitionSpec as P

BLK = 128
BDEV = 32
NNZB = 5
GMAX = 16
OFFSETS = (-2, -1, 1, 2)
ORDER = (0, 3, 1, 2)
EPS = 1e-6
SHIFT = 8.0
SCALE = 0.25
ROUNDS = 7
GROUP = 8
CHUNK = 4
ZERO_ROW = BDEV + 4 * GMAX
XROWS = ZERO_ROW + 8
RELAY_ROW = XROWS
RELAY_A = 7
RELAY_B = 103
RELAYED = ((2, 0), (1, 1), (1, 0))
PAIRS = ((0, 0), (0, 1), (0, 2), (1, 1), (1, 2), (2, 2), (0, 3), (1, 3), (2, 3))
MESH = pl.DeviceIdType.MESH


def arnoldi_weights(gram, substep):
    G = {}
    for (i, j), g in gram.items():
        G[i, j] = g
        G[j, i] = g
    zero = jnp.zeros_like(substep)
    magnitude = jnp.sqrt(G[0, 0] + EPS)
    vectors = [[1.0 / magnitude]]
    H = [[None] * 3 for _ in range(3)]
    for col in range(3):
        v = vectors[col]
        n = len(v)
        mapped = [None] * (n + 1)
        for k in range(n + 1):
            term = None
            if k > 0:
                term = v[k - 1] * (1.0 / SCALE)
            if k < n:
                low = v[k] * SHIFT
                term = -low if term is None else term - low
            mapped[k] = term
        image = []
        for i in range(n):
            total = G[i, 0] * mapped[0]
            for k in range(1, n + 1):
                total = total + G[i, k] * mapped[k]
            image.append(total)
        projections = []
        for vec in vectors:
            total = vec[0] * image[0]
            for k in range(1, len(vec)):
                total = total + vec[k] * image[k]
            projections.append(total)
        for k, p in enumerate(projections):
            H[k][col] = p
        if col < 2:
            rest = list(mapped)
            for p, vec in zip(projections, vectors):
                for k in range(len(vec)):
                    rest[k] = rest[k] - p * vec[k]
            square = None
            for i in range(n + 1):
                total = G[i, 0] * rest[0]
                for k in range(1, n + 1):
                    total = total + G[i, k] * rest[k]
                total = total * rest[i]
                square = total if square is None else square + total
            length = jnp.sqrt(square + EPS)
            H[col + 1][col] = length
            inverse = 1.0 / length
            vectors.append([r * inverse for r in rest])
    small = substep * (1.0 / 64.0)
    A = [[None if H[i][j] is None else H[i][j] * small for j in range(3)] for i in range(3)]
    sublane = lax.broadcasted_iota(jnp.int32, substep.shape, 0)
    unit = [jnp.where(sublane == i, 1.0, 0.0) for i in range(4)]
    rows = unit[:3]
    for degree in range(12, 0, -1):
        new = []
        for i in range(3):
            total = unit[3] * (1.0 / 64.0) if i == 0 else None
            for k in range(3):
                if A[i][k] is not None:
                    term = A[i][k] * rows[k]
                    total = term if total is None else total + term
            new.append(unit[i] + total * (1.0 / degree))
        rows = new

    def column(row, k):
        return jnp.broadcast_to(row[k : k + 1, :], substep.shape)

    for _ in range(6):
        rows = [
            column(row, 0) * rows[0]
            + column(row, 1) * rows[1]
            + (column(row, 2) * rows[2] + unit[3] * row)
            for row in rows
        ]
    q = [column(row, 3) for row in rows]
    out = []
    for k in range(3):
        total = None
        for col in range(k, 3):
            term = q[col] * vectors[col][k]
            total = term if total is None else total + term
        out.append(total * (substep * magnitude))
    return out


def kernel(ndev, conc_hbm, rate_hbm, step_hbm, blocks_hbm, cols_hbm, lens_hbm, lists_hbm, result, *scratch):
    (conc_in, rate_in, conc, rate, slope8, fixed, blocks, ys, sends, gram_row, arrivals, ordered) = scratch[:12]
    (step_s, cols_s, lens_s, lists_s, index_s, place_s, row_s, pick_s) = scratch[12:20]
    stacked, folded, us_ref = scratch[20:23]
    xs = scratch[23 : 23 + ROUNDS]
    in_sems, block_sem, send_sem, recv_sems, ar_send, ar_recv, relay_sem, known = scratch[23 + ROUNDS :]
    me = lax.axis_index("dom")

    def near(o):
        return lax.rem(me + (o + ndev), ndev)

    my_core, my_x = lax.rem(me, 2), lax.rem(me // 2, 4)
    urgent = jnp.where(my_x < 2, 0, 3 - my_core)

    small = [
        pltpu.make_async_copy(lists_hbm, lists_s, in_sems.at[0]),
        pltpu.make_async_copy(conc_hbm, conc_in, in_sems.at[1]),
        pltpu.make_async_copy(cols_hbm, cols_s, in_sems.at[2]),
        pltpu.make_async_copy(lens_hbm, lens_s, in_sems.at[3]),
        pltpu.make_async_copy(rate_hbm, rate_in, in_sems.at[4]),
        pltpu.make_async_copy(step_hbm, step_s, in_sems.at[5]),
    ]
    for copy in small:
        copy.start()

    barrier = pltpu.get_barrier_semaphore()

    def greet(device):
        pl.semaphore_signal(barrier, inc=1, device_id=(device,), device_id_type=MESH)

    for q in ORDER:
        greet(jnp.where(me + OFFSETS[q] >= ndev, RELAY_B, near(OFFSETS[q])))

    @pl.when(me == RELAY_A)
    def _():
        greet(0)
        greet(1)

    @pl.when(me == RELAY_B)
    def _():
        greet(RELAY_A)

    greetings = (
        4
        + jnp.where(me == RELAY_B, 3, 0)
        + jnp.where(me == RELAY_A, 1, 0)
        - jnp.where(me == 0, 1, 0)
    )

    for c in range(BDEV // CHUNK):
        part = pl.ds(c * CHUNK, CHUNK)
        pltpu.make_async_copy(blocks_hbm.at[part], blocks.at[part], block_sem).start()

    def packet(r, q, source):
        offset = jnp.where(q < 2, q - 2, q - 1)
        return pltpu.make_async_remote_copy(
            src_ref=source,
            dst_ref=xs[r].at[pl.ds(pl.multiple_of(BDEV + q * GMAX, 8), GMAX), :],
            send_sem=send_sem,
            recv_sem=recv_sems.at[r],
            device_id=(lax.rem(me + offset + ndev, ndev),),
            device_id_type=MESH,
        )

    def await_ghosts(r):
        part = xs[r].at[pl.ds(BDEV, 4 * GMAX), :]
        pltpu.make_async_copy(part, part, recv_sems.at[r]).wait()

    def lane_sums(total):
        return jnp.sum(total.T, axis=0, keepdims=True)

    def own_part(r):
        source = conc if r == 0 else ys.at[r - 1]

        def group(i, carry):
            for s in range(GROUP):
                p = i * GROUP + s
                mine = source[pl.ds(p, 1), :]
                here = lane_sums(blocks[row_s[p], 0] * mine)
                if r == 0:
                    kept = rate[pl.ds(p, 1), :] * mine * (1.0 - mine)
                else:
                    kept = slope8[pl.ds(p, 1), :] * mine
                fixed[pl.ds(p, 1), :] = kept - here
            return carry

        lax.fori_loop(0, BDEV // GROUP, group, 0)

    def product(r, low, high):
        x = xs[r]
        for p in range(low, high):
            total = None
            b = row_s[p]
            for t in range(1, NNZB):
                row = x[pl.ds(index_s[p * NNZB + t], 8, stride=0), :]
                term = blocks[b, t].reshape(16, 8, BLK) * row[None]
                total = term if total is None else total + term
            whole = fixed[pl.ds(p, 1), :] - lane_sums(total.reshape(BLK, BLK))
            whole = whole if r == 0 else whole * SCALE
            ys[r, pl.ds(p, 1), :] = whole
            if r + 1 < ROUNDS:
                xs[r + 1][pl.ds(p, 1), :] = whole

    def fold():
        def split(value):
            high = value.astype(jnp.bfloat16)
            return high, (value - high.astype(jnp.float32)).astype(jnp.bfloat16)

        def group(i, carry):
            for s in range(GROUP):
                p = i * GROUP + s
                left = jnp.concatenate(split(stacked[p]), axis=0)
                for t in range(1, NNZB):
                    right = jnp.concatenate(split(blocks[row_s[p], t]), axis=1)
                    both = jnp.dot(left, right, preferred_element_type=jnp.float32)
                    folded[p * NNZB + t] = (
                        both[:8, :BLK] + both[:8, BLK:] + (both[8:, :BLK] + both[8:, BLK:])
                    )
            return carry

        lax.fori_loop(0, BDEV // GROUP, group, 0)

    def turn(r):
        product(r, 0, GMAX)
        n = r + 1
        if n < ROUNDS:
            packet(n, urgent, ys.at[r, pl.ds(0, GMAX), :]).start()
        product(r, GMAX, BDEV)
        if n < ROUNDS:
            for k in range(1, 4):
                q = lax.rem(urgent + k, 4)
                for g in range(GMAX):
                    sends[n, k, pl.ds(g, 1), :] = ys[r, pl.ds(pick_s[q * GMAX + g], 1), :]
                packet(n, q, sends.at[n, k]).start()

    small[0].wait()
    small[1].wait()
    for q in ORDER:
        for g in range(GMAX):
            sends[0, q, pl.ds(g, 1), :] = conc_in[pl.ds(lists_s[0, q, g], 1), :]
    pl.semaphore_wait(barrier, greetings)
    for q in ORDER:
        relayed = me + OFFSETS[q] < 0
        slot = q + 2 * me
        pltpu.make_async_remote_copy(
            src_ref=sends.at[0, q],
            dst_ref=xs[0].at[
                pl.ds(
                    pl.multiple_of(
                        jnp.where(relayed, RELAY_ROW + slot * GMAX, BDEV + q * GMAX), 8
                    ),
                    GMAX,
                ),
                :,
            ],
            send_sem=send_sem,
            recv_sem=recv_sems.at[jnp.where(relayed, ROUNDS + slot, 0)],
            device_id=(jnp.where(relayed, RELAY_A, near(OFFSETS[q])),),
            device_id_type=MESH,
        ).start()

    def forward(i):
        before_end, q = RELAYED[i]
        first = me == RELAY_A
        here = xs[0].at[pl.ds(RELAY_ROW + i * GMAX, GMAX), :]
        row = jnp.where(first, RELAY_ROW + i * GMAX, BDEV + q * GMAX)
        return pltpu.make_async_remote_copy(
            src_ref=here,
            dst_ref=xs[0].at[pl.ds(pl.multiple_of(row, 8), GMAX), :],
            send_sem=relay_sem,
            recv_sem=recv_sems.at[jnp.where(first, ROUNDS + i, 0)],
            device_id=(jnp.where(first, RELAY_B, ndev - before_end),),
            device_id_type=MESH,
        )

    relay_part = xs[0].at[pl.ds(RELAY_ROW, len(RELAYED) * GMAX), :]
    is_relay = (me == RELAY_A) | (me == RELAY_B)

    @pl.when(is_relay)
    def _():
        for i in range(len(RELAYED)):
            here = xs[0].at[pl.ds(RELAY_ROW + i * GMAX, GMAX), :]
            pltpu.make_async_copy(here, here, recv_sems.at[ROUNDS + i]).wait()
            forward(i).start()

    for x in xs:
        x[pl.ds(ZERO_ROW, 8), :] = jnp.zeros((8, BLK), jnp.float32)
    stacked[...] = jnp.zeros_like(stacked)
    for copy in small[2:]:
        copy.wait()

    def find(b, others):
        found = 0
        for g in range(GMAX):
            found = jnp.where(lists_s[0, urgent, g] == b, g + 1, found)
        place_s[b] = jnp.where(found > 0, found - 1, jnp.minimum(GMAX + others, BDEV - 1))
        return others + jnp.where(found > 0, 0, 1)

    lax.fori_loop(0, BDEV, find, 0)
    for c in range(BDEV, ZERO_ROW):
        place_s[c] = c

    def settle(p, b):
        row_s[p] = b
        conc[pl.ds(p, 1), :] = conc_in[pl.ds(b, 1), :]
        rate[pl.ds(p, 1), :] = rate_in[pl.ds(b, 1), :]
        xs[0][pl.ds(p, 1), :] = conc_in[pl.ds(b, 1), :]
        length = lens_s[b]
        for t in range(1, NNZB):
            index_s[p * NNZB + t] = jnp.where(t < length, place_s[cols_s[t, b]], ZERO_ROW)

    def settle_pair(g, carry):
        settle(g, lists_s[0, urgent, g])
        b = g
        for i in range(1, GMAX + 1):
            b = jnp.where(place_s[g + i] == GMAX + g, g + i, b)
        settle(GMAX + g, b)
        return carry

    lax.fori_loop(0, GMAX, settle_pair, 0)

    def choose(g, carry):
        for q in range(4):
            pick_s[q * GMAX + g] = place_s[lists_s[0, q, g]]
        return carry

    lax.fori_loop(0, GMAX, choose, 0)
    slope8[...] = rate[...] * (1.0 - 2.0 * conc[...]) + SHIFT
    pltpu.make_async_copy(blocks, blocks, block_sem).wait()
    own_part(0)
    await_ghosts(0)
    turn(0)

    lane = lax.broadcasted_iota(jnp.int32, (1, BLK), 1)
    sublane = lax.broadcasted_iota(jnp.int32, (8, BLK), 0)

    def sums_row(products, first, row):
        for e, p in enumerate(products, first):
            total = jnp.sum(jnp.sum(p, axis=0, keepdims=True), axis=1, keepdims=True)
            row = jnp.where(lane == e, total, row)
        return row

    def broadcast_gram(slot, row):
        gram_row[slot] = row
        for k in range(ndev - 1):
            pltpu.make_async_remote_copy(
                src_ref=gram_row.at[slot],
                dst_ref=arrivals.at[slot, me],
                send_sem=ar_send,
                recv_sem=ar_recv.at[slot],
                device_id=(jnp.where(me <= k, k + 1, k),),
                device_id_type=MESH,
            ).start()

    def collect_gram(slot):
        whole = arrivals.at[slot, pl.ds(0, ndev - 1)]
        with jax.named_scope(f"collect{slot}"):
            pltpu.make_async_copy(whole, whole, ar_recv.at[slot]).wait()
        arrivals[slot, me] = gram_row[slot]
        parts = [arrivals[slot, i] for i in range(ndev)]
        while len(parts) > 1:
            parts = [a + b for a, b in zip(parts[::2], parts[1::2])]
        total = parts[0]
        return {
            pair: jnp.broadcast_to(total[:, e : e + 1], (8, BLK)) for e, pair in enumerate(PAIRS)
        }

    def meet(step):
        for o in (2 << step, -(2 << step)):
            pl.semaphore_signal(known.at[step], inc=1, device_id=(near(o),), device_id_type=MESH)

    zero_row = jnp.zeros((1, BLK), jnp.float32)
    meet(0)
    substep = jnp.full((8, BLK), step_s[0] * 0.5, jnp.float32)

    def times(c, field):
        return (field.reshape(BDEV // 8, 8, BLK) * c[None]).reshape(BDEV, BLK)

    us = None
    for r in range(1, ROUNDS):
        if r <= 4:
            pl.semaphore_wait(known.at[r - 1], 2)
            meet(r)
        own_part(r)
        if r == 4:
            pl.semaphore_wait(known.at[4], 2)
            w = [ys[k] for k in range(4)]
            broadcast_gram(0, sums_row([w[i] * w[j] for i, j in PAIRS], 0, zero_row))
        if r == ROUNDS - 1:
            w = [ys[k] for k in range(6)]
            first_weights = arnoldi_weights(collect_gram(0), substep)
            d = [None] * 4
            for k in range(4):
                term = None
                if k > 0:
                    term = first_weights[k - 1] * (1.0 / SCALE)
                if k < 3:
                    low = first_weights[k] * SHIFT
                    term = -low if term is None else term - low
                d[k] = term
            d[0] = d[0] + 1.0
            us = [
                times(d[0], w[k]) + times(d[1], w[k + 1]) + times(d[2], w[k + 2]) + times(d[3], w[k + 3])
                for k in range(3)
            ]
            tail = times(d[0], w[3]) + times(d[1], w[4]) + times(d[2], w[5])
            partial = sums_row([us[i] * us[j] for i, j in PAIRS[:6]], 0, zero_row)
            for k in range(3):
                us_ref[k] = us[k]
            for p in range(BDEV):
                for k in range(3):
                    stacked[p, pl.ds(k, 1), :] = us_ref[k, pl.ds(p, 1), :]
            fold()
            kept = []
            for k in range(3):
                mine = us[k] * (tail + times(d[3], fixed[...]) * SCALE)
                kept.append(jnp.sum(mine, axis=0, keepdims=True))
            known_part = jnp.concatenate(kept + [jnp.zeros((5, BLK), jnp.float32)], axis=0)
            base = (
                conc[...]
                + times(first_weights[0], w[0])
                + times(first_weights[1], w[1])
                + times(first_weights[2], w[2])
            )
        await_ghosts(r)
        if r < ROUNDS - 1:
            turn(r)
    x = xs[ROUNDS - 1]
    parts = [None] * 8
    for p in range(BDEV):
        for t in range(1, NNZB):
            term = folded[p * NNZB + t] * x[pl.ds(index_s[p * NNZB + t], 8, stride=0), :]
            i = (p * 4 + t) % 8
            parts[i] = term if parts[i] is None else parts[i] + term
    while len(parts) > 1:
        parts = [a + b for a, b in zip(parts[::2], parts[1::2])]
    late = jnp.sum(known_part - d[3] * SCALE * parts[0], axis=1, keepdims=True)
    diagonal = lax.broadcasted_iota(jnp.int32, (8, BLK), 1) == sublane + 6
    inner = jnp.where(diagonal & (sublane < 3), late, 0.0)
    broadcast_gram(1, partial + jnp.sum(inner, axis=0, keepdims=True))
    second = arnoldi_weights(collect_gram(1), substep)
    ordered[...] = base + times(second[0], us[0]) + times(second[1], us[1]) + times(second[2], us[2])
    for b in range(BDEV):
        result[pl.ds(b, 1), :] = ordered[pl.ds(place_s[b], 1), :]
    pltpu.make_async_copy(sends, sends, send_sem).wait()

    @pl.when(is_relay)
    def _():
        pltpu.make_async_copy(relay_part, relay_part, relay_sem).wait()

    whole = arrivals.at[:, pl.ds(0, ndev - 1)]
    pltpu.make_async_copy(whole, whole, ar_send).wait()


def solution(mesh):
    ndev = mesh.shape["dom"]

    def step(conc, rate, size, blocks, cols, lens, lists):
        f32, i32 = jnp.float32, jnp.int32
        return pl.pallas_call(
            lambda *refs: kernel(ndev, *refs),
            out_shape=pltpu.VMEM((BDEV, BLK), f32),
            in_specs=[pl.BlockSpec(memory_space=pltpu.HBM)] * 7,
            out_specs=pl.BlockSpec(memory_space=pltpu.VMEM),
            scratch_shapes=[
                pltpu.VMEM((BDEV, BLK), f32),
                pltpu.VMEM((BDEV, BLK), f32),
                pltpu.VMEM((BDEV, BLK), f32),
                pltpu.VMEM((BDEV, BLK), f32),
                pltpu.VMEM((BDEV, BLK), f32),
                pltpu.VMEM((BDEV, BLK), f32),
                pltpu.VMEM((BDEV, NNZB, BLK, BLK), f32),
                pltpu.VMEM((ROUNDS, BDEV, BLK), f32),
                pltpu.VMEM((ROUNDS, 4, GMAX, BLK), f32),
                pltpu.VMEM((2, 1, BLK), f32),
                pltpu.VMEM((2, ndev, 1, BLK), f32),
                pltpu.VMEM((BDEV, BLK), f32),
                pltpu.SMEM((1,), f32),
                pltpu.SMEM((NNZB, BDEV), i32),
                pltpu.SMEM((BDEV,), i32),
                pltpu.SMEM((1, 4, GMAX), i32),
                pltpu.SMEM((BDEV * NNZB,), i32),
                pltpu.SMEM((ZERO_ROW,), i32),
                pltpu.SMEM((BDEV,), i32),
                pltpu.SMEM((4 * GMAX,), i32),
            ]
            + [
                pltpu.VMEM((BDEV, 8, BLK), f32),
                pltpu.VMEM((BDEV * NNZB, 8, BLK), f32),
                pltpu.VMEM((3, BDEV, BLK), f32),
            ]
            + [pltpu.VMEM((XROWS + len(RELAYED) * GMAX, BLK), f32)]
            + [pltpu.VMEM((XROWS, BLK), f32)] * (ROUNDS - 1)
            + [
                pltpu.SemaphoreType.DMA((6,)),
                pltpu.SemaphoreType.DMA,
                pltpu.SemaphoreType.DMA,
                pltpu.SemaphoreType.DMA((ROUNDS + len(RELAYED),)),
                pltpu.SemaphoreType.DMA,
                pltpu.SemaphoreType.DMA((2,)),
                pltpu.SemaphoreType.DMA,
                pltpu.SemaphoreType.REGULAR((5,)),
            ],
            compiler_params=pltpu.CompilerParams(collective_id=0, has_side_effects=True),
            name="rosenbrock",
        )(conc, rate, size, blocks, cols.T, lens, lists)

    dom = "dom"
    return jax.shard_map(
        step,
        mesh=mesh,
        in_specs=(P(dom), P(dom), P(), P(dom), P(dom), P(dom), P(dom)),
        out_specs=P(dom),
        check_vma=False,
    )
```

```python
import jax
import jax.numpy as jnp
from jax import lax
from jax.experimental import pallas as pl
from jax.experimental.pallas import tpu as pltpu
from jax.sharding import PartitionSpec as P

BLK = 128
BDEV = 32
NNZB = 5
GMAX = 16
OFFSETS = (-2, -1, 1, 2)
ORDER = (0, 3, 1, 2)
EPS = 1e-6
SHIFT = 8.0
SCALE = 0.25
ROUNDS = 7
GROUP = 8
CHUNK = 4
ZERO_ROW = BDEV + 4 * GMAX
XROWS = ZERO_ROW + 8
MATRIX = 4
RELAY_ROW = XROWS
RELAY_A = 7
RELAY_B = 103
RELAYED = ((2, 0), (1, 1), (1, 0))
PAIRS = ((0, 0), (0, 1), (0, 2), (1, 1), (1, 2), (2, 2), (0, 3), (1, 3), (2, 3))
MESH = pl.DeviceIdType.MESH


def arnoldi_weights(gram, substep):
    G = {}
    for (i, j), g in gram.items():
        G[i, j] = g
        G[j, i] = g
    zero = jnp.zeros_like(substep)
    magnitude = jnp.sqrt(G[0, 0] + EPS)
    vectors = [[1.0 / magnitude]]
    H = [[None] * 3 for _ in range(3)]
    for col in range(3):
        v = vectors[col]
        n = len(v)
        mapped = [None] * (n + 1)
        for k in range(n + 1):
            term = None
            if k > 0:
                term = v[k - 1] * (1.0 / SCALE)
            if k < n:
                low = v[k] * SHIFT
                term = -low if term is None else term - low
            mapped[k] = term
        image = []
        for i in range(n):
            total = G[i, 0] * mapped[0]
            for k in range(1, n + 1):
                total = total + G[i, k] * mapped[k]
            image.append(total)
        projections = []
        for vec in vectors:
            total = vec[0] * image[0]
            for k in range(1, len(vec)):
                total = total + vec[k] * image[k]
            projections.append(total)
        for k, p in enumerate(projections):
            H[k][col] = p
        if col < 2:
            rest = list(mapped)
            for p, vec in zip(projections, vectors):
                for k in range(len(vec)):
                    rest[k] = rest[k] - p * vec[k]
            square = None
            for i in range(n + 1):
                total = G[i, 0] * rest[0]
                for k in range(1, n + 1):
                    total = total + G[i, k] * rest[k]
                total = total * rest[i]
                square = total if square is None else square + total
            length = jnp.sqrt(square + EPS)
            H[col + 1][col] = length
            inverse = 1.0 / length
            vectors.append([r * inverse for r in rest])
    small = substep * (1.0 / 64.0)
    A = [[None if H[i][j] is None else H[i][j] * small for j in range(3)] for i in range(3)]
    sublane = lax.broadcasted_iota(jnp.int32, substep.shape, 0)
    unit = [jnp.where(sublane == i, 1.0, 0.0) for i in range(4)]
    rows = unit[:3]
    for degree in range(12, 0, -1):
        new = []
        for i in range(3):
            total = unit[3] * (1.0 / 64.0) if i == 0 else None
            for k in range(3):
                if A[i][k] is not None:
                    term = A[i][k] * rows[k]
                    total = term if total is None else total + term
            new.append(unit[i] + total * (1.0 / degree))
        rows = new

    def column(row, k):
        return jnp.broadcast_to(row[k : k + 1, :], substep.shape)

    for _ in range(6):
        rows = [
            column(row, 0) * rows[0]
            + column(row, 1) * rows[1]
            + (column(row, 2) * rows[2] + unit[3] * row)
            for row in rows
        ]
    q = [column(row, 3) for row in rows]
    out = []
    for k in range(3):
        total = None
        for col in range(k, 3):
            term = q[col] * vectors[col][k]
            total = term if total is None else total + term
        out.append(total * (substep * magnitude))
    return out


def kernel(ndev, conc_hbm, rate_hbm, step_hbm, blocks_hbm, cols_hbm, lens_hbm, lists_hbm, result, *scratch):
    (conc_in, rate_in, conc, rate, slope8, fixed, blocks, ys, sends, gram_row, arrivals, ordered) = scratch[:12]
    (step_s, cols_s, lens_s, lists_s, index_s, place_s, row_s, pick_s) = scratch[12:20]
    stacked, folded, us_ref, weights = scratch[20:24]
    xs = scratch[24 : 24 + ROUNDS]
    in_sems, block_sem, send_sem, recv_sems, ar_send, ar_recv, relay_sem, known = scratch[24 + ROUNDS :]
    me = lax.axis_index("dom")

    def near(o):
        return lax.rem(me + (o + ndev), ndev)

    my_core, my_x = lax.rem(me, 2), lax.rem(me // 2, 4)
    urgent = jnp.where(my_x < 2, 0, 3 - my_core)

    small = [
        pltpu.make_async_copy(lists_hbm, lists_s, in_sems.at[0]),
        pltpu.make_async_copy(conc_hbm, conc_in, in_sems.at[1]),
        pltpu.make_async_copy(cols_hbm, cols_s, in_sems.at[2]),
        pltpu.make_async_copy(lens_hbm, lens_s, in_sems.at[3]),
        pltpu.make_async_copy(rate_hbm, rate_in, in_sems.at[4]),
        pltpu.make_async_copy(step_hbm, step_s, in_sems.at[5]),
    ]
    barrier = pltpu.get_barrier_semaphore()

    def greet(device):
        pl.semaphore_signal(barrier, inc=1, device_id=(device,), device_id_type=MESH)

    @pl.when(me == RELAY_A)
    def _():
        greet(0)
        greet(1)

    @pl.when(me == RELAY_B)
    def _():
        greet(RELAY_A)

    for q in ORDER:
        greet(jnp.where(me + OFFSETS[q] >= ndev, RELAY_B, near(OFFSETS[q])))

    for copy in small:
        copy.start()

    greetings = (
        4
        + jnp.where(me == RELAY_B, 3, 0)
        + jnp.where(me == RELAY_A, 1, 0)
        - jnp.where(me == 0, 1, 0)
    )

    for c in range(BDEV // CHUNK):
        part = pl.ds(c * CHUNK, CHUNK)
        pltpu.make_async_copy(blocks_hbm.at[part], blocks.at[part], block_sem).start()

    def packet(r, q, source):
        offset = jnp.where(q < 2, q - 2, q - 1)
        return pltpu.make_async_remote_copy(
            src_ref=source,
            dst_ref=xs[r].at[pl.ds(pl.multiple_of(BDEV + q * GMAX, 8), GMAX), :],
            send_sem=send_sem,
            recv_sem=recv_sems.at[r],
            device_id=(lax.rem(me + offset + ndev, ndev),),
            device_id_type=MESH,
        )

    def await_ghosts(r):
        part = xs[r].at[pl.ds(BDEV, 4 * GMAX), :]
        pltpu.make_async_copy(part, part, recv_sems.at[r]).wait()

    def lane_sums(total):
        return jnp.sum(total.T, axis=0, keepdims=True)

    def own_part(r):
        source = conc if r == 0 else ys.at[r - 1]

        def group(i, carry):
            for s in range(GROUP):
                p = i * GROUP + s
                mine = source[pl.ds(p, 1), :]
                here = lane_sums(blocks[row_s[p], 0] * mine)
                if r == 0:
                    kept = rate[pl.ds(p, 1), :] * mine * (1.0 - mine)
                else:
                    kept = slope8[pl.ds(p, 1), :] * mine
                fixed[pl.ds(p, 1), :] = kept - here
            return carry

        lax.fori_loop(0, BDEV // GROUP, group, 0)

    def split(value):
        high = value.astype(jnp.bfloat16)
        return high, (value - high.astype(jnp.float32)).astype(jnp.bfloat16)

    def load_weights():
        def one(m, carry):
            b = row_s[GMAX - MATRIX + m]
            for t in range(1, NNZB):
                weights[m, pl.ds((t - 1) * BLK, BLK), :] = jnp.concatenate(split(blocks[b, t].T), axis=1)
            return carry

        lax.fori_loop(0, MATRIX, one, 0)

    def keep(r, p, whole):
        ys[r, pl.ds(p, 1), :] = whole
        if r + 1 < ROUNDS:
            xs[r + 1][pl.ds(p, 1), :] = whole

    def matrix_product(r):
        x = xs[r]
        for m in range(MATRIX):
            p = GMAX - MATRIX + m
            wide = jnp.concatenate(
                [x[pl.ds(index_s[p * NNZB + t], 8, stride=0), :] for t in range(1, NNZB)], axis=1
            )
            both = jnp.dot(
                jnp.concatenate(split(wide), axis=0), weights[m], preferred_element_type=jnp.float32
            )
            row = both[:1, :BLK] + both[:1, BLK:] + (both[8:9, :BLK] + both[8:9, BLK:])
            keep(r, p, (fixed[pl.ds(p, 1), :] - row) * SCALE)

    def product(r, low, high):
        x = xs[r]
        for p in range(low, high):
            total = None
            b = row_s[p]
            for t in range(1, NNZB):
                row = x[pl.ds(index_s[p * NNZB + t], 8, stride=0), :]
                term = blocks[b, t].reshape(16, 8, BLK) * row[None]
                total = term if total is None else total + term
            whole = fixed[pl.ds(p, 1), :] - lane_sums(total.reshape(BLK, BLK))
            whole = whole if r == 0 else whole * SCALE
            keep(r, p, whole)

    def fold():
        def group(i, carry):
            for s in range(GROUP):
                p = i * GROUP + s
                left = jnp.concatenate(split(stacked[p]), axis=0)
                for t in range(1, NNZB):
                    right = jnp.concatenate(split(blocks[row_s[p], t]), axis=1)
                    both = jnp.dot(left, right, preferred_element_type=jnp.float32)
                    folded[p * NNZB + t] = (
                        both[:8, :BLK] + both[:8, BLK:] + (both[8:, :BLK] + both[8:, BLK:])
                    )
            return carry

        lax.fori_loop(0, BDEV // GROUP, group, 0)

    def turn(r):
        if r == 0:
            product(r, 0, GMAX)
        else:
            matrix_product(r)
            product(r, 0, GMAX - MATRIX)
        n = r + 1
        if n < ROUNDS:
            packet(n, urgent, ys.at[r, pl.ds(0, GMAX), :]).start()
        product(r, GMAX, BDEV)
        if n < ROUNDS:
            for k in range(1, 4):
                q = lax.rem(urgent + k, 4)
                for g in range(GMAX):
                    sends[n, k, pl.ds(g, 1), :] = ys[r, pl.ds(pick_s[q * GMAX + g], 1), :]
                packet(n, q, sends.at[n, k]).start()

    small[0].wait()
    small[1].wait()
    for q in ORDER:
        for g in range(GMAX):
            sends[0, q, pl.ds(g, 1), :] = conc_in[pl.ds(lists_s[0, q, g], 1), :]
    pl.semaphore_wait(barrier, greetings)
    for q in ORDER:
        relayed = me + OFFSETS[q] < 0
        slot = q + 2 * me
        pltpu.make_async_remote_copy(
            src_ref=sends.at[0, q],
            dst_ref=xs[0].at[
                pl.ds(
                    pl.multiple_of(
                        jnp.where(relayed, RELAY_ROW + slot * GMAX, BDEV + q * GMAX), 8
                    ),
                    GMAX,
                ),
                :,
            ],
            send_sem=send_sem,
            recv_sem=recv_sems.at[jnp.where(relayed, ROUNDS + slot, 0)],
            device_id=(jnp.where(relayed, RELAY_A, near(OFFSETS[q])),),
            device_id_type=MESH,
        ).start()

    def forward(i):
        before_end, q = RELAYED[i]
        first = me == RELAY_A
        here = xs[0].at[pl.ds(RELAY_ROW + i * GMAX, GMAX), :]
        row = jnp.where(first, RELAY_ROW + i * GMAX, BDEV + q * GMAX)
        return pltpu.make_async_remote_copy(
            src_ref=here,
            dst_ref=xs[0].at[pl.ds(pl.multiple_of(row, 8), GMAX), :],
            send_sem=relay_sem,
            recv_sem=recv_sems.at[jnp.where(first, ROUNDS + i, 0)],
            device_id=(jnp.where(first, RELAY_B, ndev - before_end),),
            device_id_type=MESH,
        )

    relay_part = xs[0].at[pl.ds(RELAY_ROW, len(RELAYED) * GMAX), :]
    is_relay = (me == RELAY_A) | (me == RELAY_B)

    @pl.when(is_relay)
    def _():
        for i in range(len(RELAYED)):
            here = xs[0].at[pl.ds(RELAY_ROW + i * GMAX, GMAX), :]
            pltpu.make_async_copy(here, here, recv_sems.at[ROUNDS + i]).wait()
            forward(i).start()

    for x in xs:
        x[pl.ds(ZERO_ROW, 8), :] = jnp.zeros((8, BLK), jnp.float32)
    stacked[...] = jnp.zeros_like(stacked)
    for copy in small[2:]:
        copy.wait()

    def find(b, others):
        found = 0
        for g in range(GMAX):
            found = jnp.where(lists_s[0, urgent, g] == b, g + 1, found)
        place_s[b] = jnp.where(found > 0, found - 1, jnp.minimum(GMAX + others, BDEV - 1))
        return others + jnp.where(found > 0, 0, 1)

    lax.fori_loop(0, BDEV, find, 0)
    for c in range(BDEV, ZERO_ROW):
        place_s[c] = c

    def settle(p, b):
        row_s[p] = b
        conc[pl.ds(p, 1), :] = conc_in[pl.ds(b, 1), :]
        rate[pl.ds(p, 1), :] = rate_in[pl.ds(b, 1), :]
        xs[0][pl.ds(p, 1), :] = conc_in[pl.ds(b, 1), :]
        length = lens_s[b]
        for t in range(1, NNZB):
            index_s[p * NNZB + t] = jnp.where(t < length, place_s[cols_s[t, b]], ZERO_ROW)

    def settle_pair(g, carry):
        settle(g, lists_s[0, urgent, g])
        b = g
        for i in range(1, GMAX + 1):
            b = jnp.where(place_s[g + i] == GMAX + g, g + i, b)
        settle(GMAX + g, b)
        return carry

    lax.fori_loop(0, GMAX, settle_pair, 0)

    def choose(g, carry):
        for q in range(4):
            pick_s[q * GMAX + g] = place_s[lists_s[0, q, g]]
        return carry

    lax.fori_loop(0, GMAX, choose, 0)
    slope8[...] = rate[...] * (1.0 - 2.0 * conc[...]) + SHIFT
    pltpu.make_async_copy(blocks, blocks, block_sem).wait()
    own_part(0)
    await_ghosts(0)
    turn(0)

    lane = lax.broadcasted_iota(jnp.int32, (1, BLK), 1)
    sublane = lax.broadcasted_iota(jnp.int32, (8, BLK), 0)

    def sums_row(products, first, row):
        for e, p in enumerate(products, first):
            total = jnp.sum(jnp.sum(p, axis=0, keepdims=True), axis=1, keepdims=True)
            row = jnp.where(lane == e, total, row)
        return row

    def broadcast_gram(slot, row):
        gram_row[slot] = row
        for k in range(ndev - 1):
            pltpu.make_async_remote_copy(
                src_ref=gram_row.at[slot],
                dst_ref=arrivals.at[slot, me],
                send_sem=ar_send,
                recv_sem=ar_recv.at[slot],
                device_id=(jnp.where(me <= k, k + 1, k),),
                device_id_type=MESH,
            ).start()

    def collect_gram(slot):
        whole = arrivals.at[slot, pl.ds(0, ndev - 1)]
        with jax.named_scope(f"collect{slot}"):
            pltpu.make_async_copy(whole, whole, ar_recv.at[slot]).wait()
        arrivals[slot, me] = gram_row[slot]
        parts = [arrivals[slot, i] for i in range(ndev)]
        while len(parts) > 1:
            parts = [a + b for a, b in zip(parts[::2], parts[1::2])]
        total = parts[0]
        return {
            pair: jnp.broadcast_to(total[:, e : e + 1], (8, BLK)) for e, pair in enumerate(PAIRS)
        }

    def meet(step):
        for o in (2 << step, -(2 << step)):
            pl.semaphore_signal(known.at[step], inc=1, device_id=(near(o),), device_id_type=MESH)

    zero_row = jnp.zeros((1, BLK), jnp.float32)
    meet(0)
    substep = jnp.full((8, BLK), step_s[0] * 0.5, jnp.float32)

    def times(c, field):
        return (field.reshape(BDEV // 8, 8, BLK) * c[None]).reshape(BDEV, BLK)

    us = None
    for r in range(1, ROUNDS):
        if r == 1:
            own_part(r)
            load_weights()
        if r <= 4:
            pl.semaphore_wait(known.at[r - 1], 2)
            meet(r)
        if r > 1:
            own_part(r)
        if r == 4:
            pl.semaphore_wait(known.at[4], 2)
            w = [ys[k] for k in range(4)]
            broadcast_gram(0, sums_row([w[i] * w[j] for i, j in PAIRS], 0, zero_row))
        if r == ROUNDS - 1:
            w = [ys[k] for k in range(6)]
            first_weights = arnoldi_weights(collect_gram(0), substep)
            d = [None] * 4
            for k in range(4):
                term = None
                if k > 0:
                    term = first_weights[k - 1] * (1.0 / SCALE)
                if k < 3:
                    low = first_weights[k] * SHIFT
                    term = -low if term is None else term - low
                d[k] = term
            d[0] = d[0] + 1.0
            us = [
                times(d[0], w[k]) + times(d[1], w[k + 1]) + times(d[2], w[k + 2]) + times(d[3], w[k + 3])
                for k in range(3)
            ]
            tail = times(d[0], w[3]) + times(d[1], w[4]) + times(d[2], w[5])
            partial = sums_row([us[i] * us[j] for i, j in PAIRS[:6]], 0, zero_row)
            for k in range(3):
                us_ref[k] = us[k]
            for p in range(BDEV):
                for k in range(3):
                    stacked[p, pl.ds(k, 1), :] = us_ref[k, pl.ds(p, 1), :]
            fold()
            kept = []
            for k in range(3):
                mine = us[k] * (tail + times(d[3], fixed[...]) * SCALE)
                kept.append(jnp.sum(mine, axis=0, keepdims=True))
            known_part = jnp.concatenate(kept + [jnp.zeros((5, BLK), jnp.float32)], axis=0)
            base = (
                conc[...]
                + times(first_weights[0], w[0])
                + times(first_weights[1], w[1])
                + times(first_weights[2], w[2])
            )
        await_ghosts(r)
        if r < ROUNDS - 1:
            turn(r)
    x = xs[ROUNDS - 1]
    parts = [None] * 8
    for p in range(BDEV):
        for t in range(1, NNZB):
            term = folded[p * NNZB + t] * x[pl.ds(index_s[p * NNZB + t], 8, stride=0), :]
            i = (p * 4 + t) % 8
            parts[i] = term if parts[i] is None else parts[i] + term
    while len(parts) > 1:
        parts = [a + b for a, b in zip(parts[::2], parts[1::2])]
    late = jnp.sum(known_part - d[3] * SCALE * parts[0], axis=1, keepdims=True)
    diagonal = lax.broadcasted_iota(jnp.int32, (8, BLK), 1) == sublane + 6
    inner = jnp.where(diagonal & (sublane < 3), late, 0.0)
    broadcast_gram(1, partial + jnp.sum(inner, axis=0, keepdims=True))
    second = arnoldi_weights(collect_gram(1), substep)
    ordered[...] = base + times(second[0], us[0]) + times(second[1], us[1]) + times(second[2], us[2])
    for b in range(BDEV):
        result[pl.ds(b, 1), :] = ordered[pl.ds(place_s[b], 1), :]
    pltpu.make_async_copy(sends, sends, send_sem).wait()

    @pl.when(is_relay)
    def _():
        pltpu.make_async_copy(relay_part, relay_part, relay_sem).wait()

    whole = arrivals.at[:, pl.ds(0, ndev - 1)]
    pltpu.make_async_copy(whole, whole, ar_send).wait()


def solution(mesh):
    ndev = mesh.shape["dom"]

    def step(conc, rate, size, blocks, cols, lens, lists):
        f32, i32 = jnp.float32, jnp.int32
        return pl.pallas_call(
            lambda *refs: kernel(ndev, *refs),
            out_shape=pltpu.VMEM((BDEV, BLK), f32),
            in_specs=[pl.BlockSpec(memory_space=pltpu.HBM)] * 7,
            out_specs=pl.BlockSpec(memory_space=pltpu.VMEM),
            scratch_shapes=[
                pltpu.VMEM((BDEV, BLK), f32),
                pltpu.VMEM((BDEV, BLK), f32),
                pltpu.VMEM((BDEV, BLK), f32),
                pltpu.VMEM((BDEV, BLK), f32),
                pltpu.VMEM((BDEV, BLK), f32),
                pltpu.VMEM((BDEV, BLK), f32),
                pltpu.VMEM((BDEV, NNZB, BLK, BLK), f32),
                pltpu.VMEM((ROUNDS, BDEV, BLK), f32),
                pltpu.VMEM((ROUNDS, 4, GMAX, BLK), f32),
                pltpu.VMEM((2, 1, BLK), f32),
                pltpu.VMEM((2, ndev, 1, BLK), f32),
                pltpu.VMEM((BDEV, BLK), f32),
                pltpu.SMEM((1,), f32),
                pltpu.SMEM((NNZB, BDEV), i32),
                pltpu.SMEM((BDEV,), i32),
                pltpu.SMEM((1, 4, GMAX), i32),
                pltpu.SMEM((BDEV * NNZB,), i32),
                pltpu.SMEM((ZERO_ROW,), i32),
                pltpu.SMEM((BDEV,), i32),
                pltpu.SMEM((4 * GMAX,), i32),
            ]
            + [
                pltpu.VMEM((BDEV, 8, BLK), f32),
                pltpu.VMEM((BDEV * NNZB, 8, BLK), f32),
                pltpu.VMEM((3, BDEV, BLK), f32),
                pltpu.VMEM((MATRIX, (NNZB - 1) * BLK, 2 * BLK), jnp.bfloat16),
            ]
            + [pltpu.VMEM((XROWS + len(RELAYED) * GMAX, BLK), f32)]
            + [pltpu.VMEM((XROWS, BLK), f32)] * (ROUNDS - 1)
            + [
                pltpu.SemaphoreType.DMA((6,)),
                pltpu.SemaphoreType.DMA,
                pltpu.SemaphoreType.DMA,
                pltpu.SemaphoreType.DMA((ROUNDS + len(RELAYED),)),
                pltpu.SemaphoreType.DMA,
                pltpu.SemaphoreType.DMA((2,)),
                pltpu.SemaphoreType.DMA,
                pltpu.SemaphoreType.REGULAR((5,)),
            ],
            compiler_params=pltpu.CompilerParams(collective_id=0, has_side_effects=True),
            name="rosenbrock",
        )(conc, rate, size, blocks, cols.T, lens, lists)

    dom = "dom"
    return jax.shard_map(
        step,
        mesh=mesh,
        in_specs=(P(dom), P(dom), P(), P(dom), P(dom), P(dom), P(dom)),
        out_specs=P(dom),
        check_vma=False,
    )
```

```python
import jax
import jax.numpy as jnp
from jax import lax
from jax.experimental import pallas as pl
from jax.experimental.pallas import tpu as pltpu
from jax.sharding import PartitionSpec as P

BLK = 128
BDEV = 32
NNZB = 5
GMAX = 16
OFFSETS = (-2, -1, 1, 2)
ORDER = (0, 3, 1, 2)
EPS = 1e-6
SHIFT = 8.0
SCALE = 0.25
ROUNDS = 7
GROUP = 8
CHUNK = 4
ZERO_ROW = BDEV + 4 * GMAX
XROWS = ZERO_ROW + 8
MATRIX = 4
RELAY_ROW = XROWS
RELAY_A = 7
RELAY_B = 103
RELAYED = ((2, 0), (1, 1), (1, 0))
PAIRS = ((0, 0), (0, 1), (0, 2), (1, 1), (1, 2), (2, 2), (0, 3), (1, 3), (2, 3))
MESH = pl.DeviceIdType.MESH


def arnoldi_weights(gram, substep):
    G = {}
    for (i, j), g in gram.items():
        G[i, j] = g
        G[j, i] = g
    zero = jnp.zeros_like(substep)
    magnitude = jnp.sqrt(G[0, 0] + EPS)
    vectors = [[1.0 / magnitude]]
    H = [[None] * 3 for _ in range(3)]
    for col in range(3):
        v = vectors[col]
        n = len(v)
        mapped = [None] * (n + 1)
        for k in range(n + 1):
            term = None
            if k > 0:
                term = v[k - 1] * (1.0 / SCALE)
            if k < n:
                low = v[k] * SHIFT
                term = -low if term is None else term - low
            mapped[k] = term
        image = []
        for i in range(n):
            total = G[i, 0] * mapped[0]
            for k in range(1, n + 1):
                total = total + G[i, k] * mapped[k]
            image.append(total)
        projections = []
        for vec in vectors:
            total = vec[0] * image[0]
            for k in range(1, len(vec)):
                total = total + vec[k] * image[k]
            projections.append(total)
        for k, p in enumerate(projections):
            H[k][col] = p
        if col < 2:
            rest = list(mapped)
            for p, vec in zip(projections, vectors):
                for k in range(len(vec)):
                    rest[k] = rest[k] - p * vec[k]
            square = None
            for i in range(n + 1):
                total = G[i, 0] * rest[0]
                for k in range(1, n + 1):
                    total = total + G[i, k] * rest[k]
                total = total * rest[i]
                square = total if square is None else square + total
            length = jnp.sqrt(square + EPS)
            H[col + 1][col] = length
            inverse = 1.0 / length
            vectors.append([r * inverse for r in rest])
    small = substep * (1.0 / 64.0)
    A = [[None if H[i][j] is None else H[i][j] * small for j in range(3)] for i in range(3)]
    sublane = lax.broadcasted_iota(jnp.int32, substep.shape, 0)
    unit = [jnp.where(sublane == i, 1.0, 0.0) for i in range(4)]
    rows = unit[:3]
    for degree in range(12, 0, -1):
        new = []
        for i in range(3):
            total = unit[3] * (1.0 / 64.0) if i == 0 else None
            for k in range(3):
                if A[i][k] is not None:
                    term = A[i][k] * rows[k]
                    total = term if total is None else total + term
            new.append(unit[i] + total * (1.0 / degree))
        rows = new

    def column(row, k):
        return jnp.broadcast_to(row[k : k + 1, :], substep.shape)

    for _ in range(6):
        rows = [
            column(row, 0) * rows[0]
            + column(row, 1) * rows[1]
            + (column(row, 2) * rows[2] + unit[3] * row)
            for row in rows
        ]
    q = [column(row, 3) for row in rows]
    out = []
    for k in range(3):
        total = None
        for col in range(k, 3):
            term = q[col] * vectors[col][k]
            total = term if total is None else total + term
        out.append(total * (substep * magnitude))
    return out


def kernel(ndev, conc_hbm, rate_hbm, step_hbm, blocks_hbm, cols_hbm, lens_hbm, lists_hbm, result, *scratch):
    (conc_in, rate_in, conc, rate, slope8, fixed, blocks, ys, sends, gram_row, arrivals, ordered) = scratch[:12]
    (step_s, cols_s, lens_s, lists_s, index_s, place_s, row_s, pick_s) = scratch[12:20]
    stacked, folded, us_ref, weights = scratch[20:24]
    xs = scratch[24 : 24 + ROUNDS]
    in_sems, block_sem, send_sem, recv_sems, ar_send, ar_recv, relay_sem, known = scratch[24 + ROUNDS :]
    me = lax.axis_index("dom")

    def near(o):
        return lax.rem(me + (o + ndev), ndev)

    my_core, my_x = lax.rem(me, 2), lax.rem(me // 2, 4)
    urgent = jnp.where(my_x < 2, 0, 3 - my_core)

    small = [
        pltpu.make_async_copy(lists_hbm, lists_s, in_sems.at[0]),
        pltpu.make_async_copy(conc_hbm, conc_in, in_sems.at[1]),
        pltpu.make_async_copy(cols_hbm, cols_s, in_sems.at[2]),
        pltpu.make_async_copy(lens_hbm, lens_s, in_sems.at[3]),
        pltpu.make_async_copy(rate_hbm, rate_in, in_sems.at[4]),
        pltpu.make_async_copy(step_hbm, step_s, in_sems.at[5]),
    ]
    for copy in small:
        copy.start()

    barrier = pltpu.get_barrier_semaphore()

    def greet(device):
        pl.semaphore_signal(barrier, inc=1, device_id=(device,), device_id_type=MESH)

    @pl.when(me == RELAY_A)
    def _():
        greet(0)
        greet(1)

    @pl.when(me == RELAY_B)
    def _():
        greet(RELAY_A)

    for q in ORDER:
        greet(jnp.where(me + OFFSETS[q] >= ndev, RELAY_B, near(OFFSETS[q])))

    greetings = (
        4
        + jnp.where(me == RELAY_B, 3, 0)
        + jnp.where(me == RELAY_A, 1, 0)
        - jnp.where(me == 0, 1, 0)
    )

    for c in range(BDEV // CHUNK):
        part = pl.ds(c * CHUNK, CHUNK)
        pltpu.make_async_copy(blocks_hbm.at[part], blocks.at[part], block_sem).start()

    def packet(r, q, source):
        offset = jnp.where(q < 2, q - 2, q - 1)
        return pltpu.make_async_remote_copy(
            src_ref=source,
            dst_ref=xs[r].at[pl.ds(pl.multiple_of(BDEV + q * GMAX, 8), GMAX), :],
            send_sem=send_sem,
            recv_sem=recv_sems.at[r],
            device_id=(lax.rem(me + offset + ndev, ndev),),
            device_id_type=MESH,
        )

    def await_ghosts(r):
        part = xs[r].at[pl.ds(BDEV, 4 * GMAX), :]
        pltpu.make_async_copy(part, part, recv_sems.at[r]).wait()

    def lane_sums(total):
        return jnp.sum(total.T, axis=0, keepdims=True)

    def own_part(r):
        source = conc if r == 0 else ys.at[r - 1]

        def group(i, carry):
            for s in range(GROUP):
                p = i * GROUP + s
                mine = source[pl.ds(p, 1), :]
                here = lane_sums(blocks[row_s[p], 0] * mine)
                if r == 0:
                    kept = rate[pl.ds(p, 1), :] * mine * (1.0 - mine)
                else:
                    kept = slope8[pl.ds(p, 1), :] * mine
                fixed[pl.ds(p, 1), :] = kept - here
            return carry

        lax.fori_loop(0, BDEV // GROUP, group, 0)

    def split(value):
        high = value.astype(jnp.bfloat16)
        return high, (value - high.astype(jnp.float32)).astype(jnp.bfloat16)

    def load_weights():
        def one(m, carry):
            b = row_s[GMAX - MATRIX + m]
            for t in range(1, NNZB):
                weights[m, pl.ds((t - 1) * BLK, BLK), :] = jnp.concatenate(split(blocks[b, t].T), axis=1)
            return carry

        lax.fori_loop(0, MATRIX, one, 0)

    def keep(r, p, whole):
        ys[r, pl.ds(p, 1), :] = whole
        if r + 1 < ROUNDS:
            xs[r + 1][pl.ds(p, 1), :] = whole

    def matrix_product(r):
        x = xs[r]
        for m in range(MATRIX):
            p = GMAX - MATRIX + m
            wide = jnp.concatenate(
                [x[pl.ds(index_s[p * NNZB + t], 8, stride=0), :] for t in range(1, NNZB)], axis=1
            )
            both = jnp.dot(
                jnp.concatenate(split(wide), axis=0), weights[m], preferred_element_type=jnp.float32
            )
            row = both[:1, :BLK] + both[:1, BLK:] + (both[8:9, :BLK] + both[8:9, BLK:])
            keep(r, p, (fixed[pl.ds(p, 1), :] - row) * SCALE)

    def product(r, low, high):
        x = xs[r]
        for p in range(low, high):
            total = None
            b = row_s[p]
            for t in range(1, NNZB):
                row = x[pl.ds(index_s[p * NNZB + t], 8, stride=0), :]
                term = blocks[b, t].reshape(16, 8, BLK) * row[None]
                total = term if total is None else total + term
            whole = fixed[pl.ds(p, 1), :] - lane_sums(total.reshape(BLK, BLK))
            whole = whole if r == 0 else whole * SCALE
            keep(r, p, whole)

    def fold():
        def group(i, carry):
            for s in range(GROUP):
                p = i * GROUP + s
                left = jnp.concatenate(split(stacked[p]), axis=0)
                for t in range(1, NNZB):
                    right = jnp.concatenate(split(blocks[row_s[p], t]), axis=1)
                    both = jnp.dot(left, right, preferred_element_type=jnp.float32)
                    folded[p * NNZB + t] = (
                        both[:8, :BLK] + both[:8, BLK:] + (both[8:, :BLK] + both[8:, BLK:])
                    )
            return carry

        lax.fori_loop(0, BDEV // GROUP, group, 0)

    def turn(r):
        if r == 0:
            product(r, 0, GMAX)
        else:
            matrix_product(r)
            product(r, 0, GMAX - MATRIX)
        n = r + 1
        if n < ROUNDS:
            packet(n, urgent, ys.at[r, pl.ds(0, GMAX), :]).start()
        product(r, GMAX, BDEV)
        if n < ROUNDS:
            for k in range(1, 4):
                q = lax.rem(urgent + k, 4)
                for g in range(GMAX):
                    sends[n, k, pl.ds(g, 1), :] = ys[r, pl.ds(pick_s[q * GMAX + g], 1), :]
                packet(n, q, sends.at[n, k]).start()

    small[0].wait()
    small[1].wait()
    for q in ORDER:
        for g in range(GMAX):
            sends[0, q, pl.ds(g, 1), :] = conc_in[pl.ds(lists_s[0, q, g], 1), :]
    pl.semaphore_wait(barrier, greetings)
    for q in ORDER:
        relayed = me + OFFSETS[q] < 0
        slot = q + 2 * me
        pltpu.make_async_remote_copy(
            src_ref=sends.at[0, q],
            dst_ref=xs[0].at[
                pl.ds(
                    pl.multiple_of(
                        jnp.where(relayed, RELAY_ROW + slot * GMAX, BDEV + q * GMAX), 8
                    ),
                    GMAX,
                ),
                :,
            ],
            send_sem=send_sem,
            recv_sem=recv_sems.at[jnp.where(relayed, ROUNDS + slot, 0)],
            device_id=(jnp.where(relayed, RELAY_A, near(OFFSETS[q])),),
            device_id_type=MESH,
        ).start()

    def forward(i):
        before_end, q = RELAYED[i]
        first = me == RELAY_A
        here = xs[0].at[pl.ds(RELAY_ROW + i * GMAX, GMAX), :]
        row = jnp.where(first, RELAY_ROW + i * GMAX, BDEV + q * GMAX)
        return pltpu.make_async_remote_copy(
            src_ref=here,
            dst_ref=xs[0].at[pl.ds(pl.multiple_of(row, 8), GMAX), :],
            send_sem=relay_sem,
            recv_sem=recv_sems.at[jnp.where(first, ROUNDS + i, 0)],
            device_id=(jnp.where(first, RELAY_B, ndev - before_end),),
            device_id_type=MESH,
        )

    relay_part = xs[0].at[pl.ds(RELAY_ROW, len(RELAYED) * GMAX), :]
    is_relay = (me == RELAY_A) | (me == RELAY_B)

    @pl.when(is_relay)
    def _():
        for i in range(len(RELAYED)):
            here = xs[0].at[pl.ds(RELAY_ROW + i * GMAX, GMAX), :]
            pltpu.make_async_copy(here, here, recv_sems.at[ROUNDS + i]).wait()
            forward(i).start()

    for x in xs:
        x[pl.ds(ZERO_ROW, 8), :] = jnp.zeros((8, BLK), jnp.float32)
    stacked[...] = jnp.zeros_like(stacked)
    for copy in small[2:]:
        copy.wait()

    def find(b, others):
        found = 0
        for g in range(GMAX):
            found = jnp.where(lists_s[0, urgent, g] == b, g + 1, found)
        place_s[b] = jnp.where(found > 0, found - 1, jnp.minimum(GMAX + others, BDEV - 1))
        return others + jnp.where(found > 0, 0, 1)

    lax.fori_loop(0, BDEV, find, 0)
    for c in range(BDEV, ZERO_ROW):
        place_s[c] = c

    def settle(p, b):
        row_s[p] = b
        conc[pl.ds(p, 1), :] = conc_in[pl.ds(b, 1), :]
        rate[pl.ds(p, 1), :] = rate_in[pl.ds(b, 1), :]
        xs[0][pl.ds(p, 1), :] = conc_in[pl.ds(b, 1), :]
        length = lens_s[b]
        for t in range(1, NNZB):
            index_s[p * NNZB + t] = jnp.where(t < length, place_s[cols_s[t, b]], ZERO_ROW)

    def settle_pair(g, carry):
        settle(g, lists_s[0, urgent, g])
        b = g
        for i in range(1, GMAX + 1):
            b = jnp.where(place_s[g + i] == GMAX + g, g + i, b)
        settle(GMAX + g, b)
        return carry

    lax.fori_loop(0, GMAX, settle_pair, 0)

    def choose(g, carry):
        for q in range(4):
            pick_s[q * GMAX + g] = place_s[lists_s[0, q, g]]
        return carry

    lax.fori_loop(0, GMAX, choose, 0)
    slope8[...] = rate[...] * (1.0 - 2.0 * conc[...]) + SHIFT
    pltpu.make_async_copy(blocks, blocks, block_sem).wait()
    own_part(0)
    await_ghosts(0)
    turn(0)

    lane = lax.broadcasted_iota(jnp.int32, (1, BLK), 1)
    sublane = lax.broadcasted_iota(jnp.int32, (8, BLK), 0)

    def sums_row(products, first, row):
        for e, p in enumerate(products, first):
            total = jnp.sum(jnp.sum(p, axis=0, keepdims=True), axis=1, keepdims=True)
            row = jnp.where(lane == e, total, row)
        return row

    def broadcast_gram(slot, row):
        gram_row[slot] = row
        for k in range(ndev - 1):
            pltpu.make_async_remote_copy(
                src_ref=gram_row.at[slot],
                dst_ref=arrivals.at[slot, me],
                send_sem=ar_send,
                recv_sem=ar_recv.at[slot],
                device_id=(jnp.where(me <= k, k + 1, k),),
                device_id_type=MESH,
            ).start()

    def collect_gram(slot):
        whole = arrivals.at[slot, pl.ds(0, ndev - 1)]
        with jax.named_scope(f"collect{slot}"):
            pltpu.make_async_copy(whole, whole, ar_recv.at[slot]).wait()
        arrivals[slot, me] = gram_row[slot]
        parts = [arrivals[slot, i] for i in range(ndev)]
        while len(parts) > 1:
            parts = [a + b for a, b in zip(parts[::2], parts[1::2])]
        total = parts[0]
        return {
            pair: jnp.broadcast_to(total[:, e : e + 1], (8, BLK)) for e, pair in enumerate(PAIRS)
        }

    def meet(step):
        for o in (2 << step, -(2 << step)):
            pl.semaphore_signal(known.at[step], inc=1, device_id=(near(o),), device_id_type=MESH)

    zero_row = jnp.zeros((1, BLK), jnp.float32)
    meet(0)
    substep = jnp.full((8, BLK), step_s[0] * 0.5, jnp.float32)

    def times(c, field):
        return (field.reshape(BDEV // 8, 8, BLK) * c[None]).reshape(BDEV, BLK)

    us = None
    for r in range(1, ROUNDS):
        if r == 1:
            own_part(r)
            load_weights()
        if r <= 4:
            pl.semaphore_wait(known.at[r - 1], 2)
            meet(r)
        if r > 1:
            own_part(r)
        if r == 4:
            pl.semaphore_wait(known.at[4], 2)
            w = [ys[k] for k in range(4)]
            broadcast_gram(0, sums_row([w[i] * w[j] for i, j in PAIRS], 0, zero_row))
        if r == ROUNDS - 1:
            w = [ys[k] for k in range(6)]
            first_weights = arnoldi_weights(collect_gram(0), substep)
            d = [None] * 4
            for k in range(4):
                term = None
                if k > 0:
                    term = first_weights[k - 1] * (1.0 / SCALE)
                if k < 3:
                    low = first_weights[k] * SHIFT
                    term = -low if term is None else term - low
                d[k] = term
            d[0] = d[0] + 1.0
            us = [
                times(d[0], w[k]) + times(d[1], w[k + 1]) + times(d[2], w[k + 2]) + times(d[3], w[k + 3])
                for k in range(3)
            ]
            tail = times(d[0], w[3]) + times(d[1], w[4]) + times(d[2], w[5])
            partial = sums_row([us[i] * us[j] for i, j in PAIRS[:6]], 0, zero_row)
            for k in range(3):
                us_ref[k] = us[k]
            for p in range(BDEV):
                for k in range(3):
                    stacked[p, pl.ds(k, 1), :] = us_ref[k, pl.ds(p, 1), :]
            fold()
            kept = []
            for k in range(3):
                mine = us[k] * (tail + times(d[3], fixed[...]) * SCALE)
                kept.append(jnp.sum(mine, axis=0, keepdims=True))
            known_part = jnp.concatenate(kept + [jnp.zeros((5, BLK), jnp.float32)], axis=0)
            base = (
                conc[...]
                + times(first_weights[0], w[0])
                + times(first_weights[1], w[1])
                + times(first_weights[2], w[2])
            )
        await_ghosts(r)
        if r < ROUNDS - 1:
            turn(r)
    x = xs[ROUNDS - 1]
    parts = [None] * 8
    for p in range(BDEV):
        for t in range(1, NNZB):
            term = folded[p * NNZB + t] * x[pl.ds(index_s[p * NNZB + t], 8, stride=0), :]
            i = (p * 4 + t) % 8
            parts[i] = term if parts[i] is None else parts[i] + term
    while len(parts) > 1:
        parts = [a + b for a, b in zip(parts[::2], parts[1::2])]
    late = jnp.sum(known_part - d[3] * SCALE * parts[0], axis=1, keepdims=True)
    diagonal = lax.broadcasted_iota(jnp.int32, (8, BLK), 1) == sublane + 6
    inner = jnp.where(diagonal & (sublane < 3), late, 0.0)
    broadcast_gram(1, partial + jnp.sum(inner, axis=0, keepdims=True))
    second = arnoldi_weights(collect_gram(1), substep)
    ordered[...] = base + times(second[0], us[0]) + times(second[1], us[1]) + times(second[2], us[2])
    for b in range(BDEV):
        result[pl.ds(b, 1), :] = ordered[pl.ds(place_s[b], 1), :]
    pltpu.make_async_copy(sends, sends, send_sem).wait()

    @pl.when(is_relay)
    def _():
        pltpu.make_async_copy(relay_part, relay_part, relay_sem).wait()

    whole = arrivals.at[:, pl.ds(0, ndev - 1)]
    pltpu.make_async_copy(whole, whole, ar_send).wait()


def solution(mesh):
    ndev = mesh.shape["dom"]

    def step(conc, rate, size, blocks, cols, lens, lists):
        f32, i32 = jnp.float32, jnp.int32
        return pl.pallas_call(
            lambda *refs: kernel(ndev, *refs),
            out_shape=pltpu.VMEM((BDEV, BLK), f32),
            in_specs=[pl.BlockSpec(memory_space=pltpu.HBM)] * 7,
            out_specs=pl.BlockSpec(memory_space=pltpu.VMEM),
            scratch_shapes=[
                pltpu.VMEM((BDEV, BLK), f32),
                pltpu.VMEM((BDEV, BLK), f32),
                pltpu.VMEM((BDEV, BLK), f32),
                pltpu.VMEM((BDEV, BLK), f32),
                pltpu.VMEM((BDEV, BLK), f32),
                pltpu.VMEM((BDEV, BLK), f32),
                pltpu.VMEM((BDEV, NNZB, BLK, BLK), f32),
                pltpu.VMEM((ROUNDS, BDEV, BLK), f32),
                pltpu.VMEM((ROUNDS, 4, GMAX, BLK), f32),
                pltpu.VMEM((2, 1, BLK), f32),
                pltpu.VMEM((2, ndev, 1, BLK), f32),
                pltpu.VMEM((BDEV, BLK), f32),
                pltpu.SMEM((1,), f32),
                pltpu.SMEM((NNZB, BDEV), i32),
                pltpu.SMEM((BDEV,), i32),
                pltpu.SMEM((1, 4, GMAX), i32),
                pltpu.SMEM((BDEV * NNZB,), i32),
                pltpu.SMEM((ZERO_ROW,), i32),
                pltpu.SMEM((BDEV,), i32),
                pltpu.SMEM((4 * GMAX,), i32),
            ]
            + [
                pltpu.VMEM((BDEV, 8, BLK), f32),
                pltpu.VMEM((BDEV * NNZB, 8, BLK), f32),
                pltpu.VMEM((3, BDEV, BLK), f32),
                pltpu.VMEM((MATRIX, (NNZB - 1) * BLK, 2 * BLK), jnp.bfloat16),
            ]
            + [pltpu.VMEM((XROWS + len(RELAYED) * GMAX, BLK), f32)]
            + [pltpu.VMEM((XROWS, BLK), f32)] * (ROUNDS - 1)
            + [
                pltpu.SemaphoreType.DMA((6,)),
                pltpu.SemaphoreType.DMA,
                pltpu.SemaphoreType.DMA,
                pltpu.SemaphoreType.DMA((ROUNDS + len(RELAYED),)),
                pltpu.SemaphoreType.DMA,
                pltpu.SemaphoreType.DMA((2,)),
                pltpu.SemaphoreType.DMA,
                pltpu.SemaphoreType.REGULAR((5,)),
            ],
            compiler_params=pltpu.CompilerParams(collective_id=0, has_side_effects=True),
            name="rosenbrock",
        )(conc, rate, size, blocks, cols.T, lens, lists)

    dom = "dom"
    return jax.shard_map(
        step,
        mesh=mesh,
        in_specs=(P(dom), P(dom), P(), P(dom), P(dom), P(dom), P(dom)),
        out_specs=P(dom),
        check_vma=False,
    )
```

```python
import jax
import jax.numpy as jnp
from jax import lax
from jax.experimental import pallas as pl
from jax.experimental.pallas import tpu as pltpu
from jax.sharding import PartitionSpec as P

BLK = 128
BDEV = 32
NNZB = 5
GMAX = 16
OFFSETS = (-2, -1, 1, 2)
ORDER = (0, 3, 1, 2)
EPS = 1e-6
SHIFT = 8.0
SCALE = 0.25
ROUNDS = 7
GROUP = 8
CHUNK = 4
ZERO_ROW = BDEV + 4 * GMAX
XROWS = ZERO_ROW + 8
MATRIX = 4
RELAY_ROW = XROWS
RELAY_A = 7
RELAY_B = 103
RELAYED = ((2, 0), (1, 1), (1, 0))
PAIRS = ((0, 0), (0, 1), (0, 2), (1, 1), (1, 2), (2, 2), (0, 3), (1, 3), (2, 3))
MESH = pl.DeviceIdType.MESH


def arnoldi_weights(gram, substep):
    G = {}
    for (i, j), g in gram.items():
        G[i, j] = g
        G[j, i] = g
    zero = jnp.zeros_like(substep)
    magnitude = jnp.sqrt(G[0, 0] + EPS)
    vectors = [[1.0 / magnitude]]
    H = [[None] * 3 for _ in range(3)]
    for col in range(3):
        v = vectors[col]
        n = len(v)
        mapped = [None] * (n + 1)
        for k in range(n + 1):
            term = None
            if k > 0:
                term = v[k - 1] * (1.0 / SCALE)
            if k < n:
                low = v[k] * SHIFT
                term = -low if term is None else term - low
            mapped[k] = term
        image = []
        for i in range(n):
            total = G[i, 0] * mapped[0]
            for k in range(1, n + 1):
                total = total + G[i, k] * mapped[k]
            image.append(total)
        projections = []
        for vec in vectors:
            total = vec[0] * image[0]
            for k in range(1, len(vec)):
                total = total + vec[k] * image[k]
            projections.append(total)
        for k, p in enumerate(projections):
            H[k][col] = p
        if col < 2:
            rest = list(mapped)
            for p, vec in zip(projections, vectors):
                for k in range(len(vec)):
                    rest[k] = rest[k] - p * vec[k]
            square = None
            for i in range(n + 1):
                total = G[i, 0] * rest[0]
                for k in range(1, n + 1):
                    total = total + G[i, k] * rest[k]
                total = total * rest[i]
                square = total if square is None else square + total
            length = jnp.sqrt(square + EPS)
            H[col + 1][col] = length
            inverse = 1.0 / length
            vectors.append([r * inverse for r in rest])
    small = substep * (1.0 / 64.0)
    A = [[None if H[i][j] is None else H[i][j] * small for j in range(3)] for i in range(3)]
    sublane = lax.broadcasted_iota(jnp.int32, substep.shape, 0)
    unit = [jnp.where(sublane == i, 1.0, 0.0) for i in range(4)]
    rows = unit[:3]
    for degree in range(12, 0, -1):
        new = []
        for i in range(3):
            total = unit[3] * (1.0 / 64.0) if i == 0 else None
            for k in range(3):
                if A[i][k] is not None:
                    term = A[i][k] * rows[k]
                    total = term if total is None else total + term
            new.append(unit[i] + total * (1.0 / degree))
        rows = new

    def column(row, k):
        return jnp.broadcast_to(row[k : k + 1, :], substep.shape)

    for _ in range(6):
        rows = [
            column(row, 0) * rows[0]
            + column(row, 1) * rows[1]
            + (column(row, 2) * rows[2] + unit[3] * row)
            for row in rows
        ]
    q = [column(row, 3) for row in rows]
    out = []
    for k in range(3):
        total = None
        for col in range(k, 3):
            term = q[col] * vectors[col][k]
            total = term if total is None else total + term
        out.append(total * (substep * magnitude))
    return out


def kernel(ndev, conc_hbm, rate_hbm, step_ref, blocks_hbm, cols_hbm, lens_hbm, lists_hbm, result, *scratch):
    (conc_in, rate_in, conc, rate, slope8, fixed, blocks, ys, sends, gram_row, arrivals, ordered) = scratch[:12]
    (cols_s, lens_s, lists_s, index_s, place_s, row_s, pick_s) = scratch[12:19]
    stacked, folded, us_ref, weights = scratch[19:23]
    xs = scratch[23 : 23 + ROUNDS]
    in_sems, block_sem, send_sem, recv_sems, ar_send, ar_recv, relay_sem, known = scratch[23 + ROUNDS :]
    me = lax.axis_index("dom")

    def near(o):
        return lax.rem(me + (o + ndev), ndev)

    my_core, my_x = lax.rem(me, 2), lax.rem(me // 2, 4)
    urgent = jnp.where(my_x < 2, 0, 3 - my_core)

    small = [
        pltpu.make_async_copy(lists_hbm, lists_s, in_sems.at[0]),
        pltpu.make_async_copy(conc_hbm, conc_in, in_sems.at[1]),
        pltpu.make_async_copy(cols_hbm, cols_s, in_sems.at[2]),
        pltpu.make_async_copy(lens_hbm, lens_s, in_sems.at[3]),
        pltpu.make_async_copy(rate_hbm, rate_in, in_sems.at[4]),
    ]
    barrier = pltpu.get_barrier_semaphore()

    def greet(device):
        pl.semaphore_signal(barrier, inc=1, device_id=(device,), device_id_type=MESH)

    @pl.when(me == RELAY_A)
    def _():
        greet(0)
        greet(1)

    @pl.when(me == RELAY_B)
    def _():
        greet(RELAY_A)

    for copy in small:
        copy.start()

    for q in ORDER:
        greet(jnp.where(me + OFFSETS[q] >= ndev, RELAY_B, near(OFFSETS[q])))

    greetings = (
        4
        + jnp.where(me == RELAY_B, 3, 0)
        + jnp.where(me == RELAY_A, 1, 0)
        - jnp.where(me == 0, 1, 0)
    )

    for c in range(BDEV // CHUNK):
        part = pl.ds(c * CHUNK, CHUNK)
        pltpu.make_async_copy(blocks_hbm.at[part], blocks.at[part], block_sem).start()

    def packet(r, q, source):
        offset = jnp.where(q < 2, q - 2, q - 1)
        return pltpu.make_async_remote_copy(
            src_ref=source,
            dst_ref=xs[r].at[pl.ds(pl.multiple_of(BDEV + q * GMAX, 8), GMAX), :],
            send_sem=send_sem,
            recv_sem=recv_sems.at[r],
            device_id=(lax.rem(me + offset + ndev, ndev),),
            device_id_type=MESH,
        )

    def await_ghosts(r):
        part = xs[r].at[pl.ds(BDEV, 4 * GMAX), :]
        pltpu.make_async_copy(part, part, recv_sems.at[r]).wait()

    def lane_sums(total):
        return jnp.sum(total.T, axis=0, keepdims=True)

    def own_part(r):
        source = conc if r == 0 else ys.at[r - 1]

        def group(i, carry):
            for s in range(GROUP):
                p = i * GROUP + s
                mine = source[pl.ds(p, 1), :]
                here = lane_sums(blocks[row_s[p], 0] * mine)
                if r == 0:
                    kept = rate[pl.ds(p, 1), :] * mine * (1.0 - mine)
                else:
                    kept = slope8[pl.ds(p, 1), :] * mine
                fixed[pl.ds(p, 1), :] = kept - here
            return carry

        lax.fori_loop(0, BDEV // GROUP, group, 0)

    def split(value):
        high = value.astype(jnp.bfloat16)
        return high, (value - high.astype(jnp.float32)).astype(jnp.bfloat16)

    def load_weights():
        def one(m, carry):
            b = row_s[GMAX - MATRIX + m]
            for t in range(1, NNZB):
                weights[m, pl.ds((t - 1) * BLK, BLK), :] = jnp.concatenate(split(blocks[b, t].T), axis=1)
            return carry

        lax.fori_loop(0, MATRIX, one, 0)

    def keep(r, p, whole):
        ys[r, pl.ds(p, 1), :] = whole
        if r + 1 < ROUNDS:
            xs[r + 1][pl.ds(p, 1), :] = whole

    def matrix_product(r):
        x = xs[r]
        for m in range(MATRIX):
            p = GMAX - MATRIX + m
            wide = jnp.concatenate(
                [x[pl.ds(index_s[p * NNZB + t], 8, stride=0), :] for t in range(1, NNZB)], axis=1
            )
            both = jnp.dot(
                jnp.concatenate(split(wide), axis=0), weights[m], preferred_element_type=jnp.float32
            )
            row = both[:1, :BLK] + both[:1, BLK:] + (both[8:9, :BLK] + both[8:9, BLK:])
            keep(r, p, (fixed[pl.ds(p, 1), :] - row) * SCALE)

    def product(r, low, high):
        x = xs[r]
        for p in range(low, high):
            total = None
            b = row_s[p]
            for t in range(1, NNZB):
                row = x[pl.ds(index_s[p * NNZB + t], 8, stride=0), :]
                term = blocks[b, t].reshape(16, 8, BLK) * row[None]
                total = term if total is None else total + term
            whole = fixed[pl.ds(p, 1), :] - lane_sums(total.reshape(BLK, BLK))
            whole = whole if r == 0 else whole * SCALE
            keep(r, p, whole)

    def fold():
        def group(i, carry):
            for s in range(GROUP):
                p = i * GROUP + s
                left = jnp.concatenate(split(stacked[p]), axis=0)
                for t in range(1, NNZB):
                    right = jnp.concatenate(split(blocks[row_s[p], t]), axis=1)
                    both = jnp.dot(left, right, preferred_element_type=jnp.float32)
                    folded[p * NNZB + t] = (
                        both[:8, :BLK] + both[:8, BLK:] + (both[8:, :BLK] + both[8:, BLK:])
                    )
            return carry

        lax.fori_loop(0, BDEV // GROUP, group, 0)

    def turn(r):
        if r == 0:
            product(r, 0, GMAX)
        else:
            matrix_product(r)
            product(r, 0, GMAX - MATRIX)
        n = r + 1
        if n < ROUNDS:
            packet(n, urgent, ys.at[r, pl.ds(0, GMAX), :]).start()
        product(r, GMAX, BDEV)
        if n < ROUNDS:
            for k in range(1, 4):
                q = lax.rem(urgent + k, 4)
                for g in range(GMAX):
                    sends[n, k, pl.ds(g, 1), :] = ys[r, pl.ds(pick_s[q * GMAX + g], 1), :]
                packet(n, q, sends.at[n, k]).start()

    small[0].wait()
    small[1].wait()
    for q in ORDER:
        for g in range(GMAX):
            sends[0, q, pl.ds(g, 1), :] = conc_in[pl.ds(lists_s[0, q, g], 1), :]
    pl.semaphore_wait(barrier, greetings)
    for q in ORDER:
        relayed = me + OFFSETS[q] < 0
        slot = q + 2 * me
        pltpu.make_async_remote_copy(
            src_ref=sends.at[0, q],
            dst_ref=xs[0].at[
                pl.ds(
                    pl.multiple_of(
                        jnp.where(relayed, RELAY_ROW + slot * GMAX, BDEV + q * GMAX), 8
                    ),
                    GMAX,
                ),
                :,
            ],
            send_sem=send_sem,
            recv_sem=recv_sems.at[jnp.where(relayed, ROUNDS + slot, 0)],
            device_id=(jnp.where(relayed, RELAY_A, near(OFFSETS[q])),),
            device_id_type=MESH,
        ).start()

    def forward(i):
        before_end, q = RELAYED[i]
        first = me == RELAY_A
        here = xs[0].at[pl.ds(RELAY_ROW + i * GMAX, GMAX), :]
        row = jnp.where(first, RELAY_ROW + i * GMAX, BDEV + q * GMAX)
        return pltpu.make_async_remote_copy(
            src_ref=here,
            dst_ref=xs[0].at[pl.ds(pl.multiple_of(row, 8), GMAX), :],
            send_sem=relay_sem,
            recv_sem=recv_sems.at[jnp.where(first, ROUNDS + i, 0)],
            device_id=(jnp.where(first, RELAY_B, ndev - before_end),),
            device_id_type=MESH,
        )

    relay_part = xs[0].at[pl.ds(RELAY_ROW, len(RELAYED) * GMAX), :]
    is_relay = (me == RELAY_A) | (me == RELAY_B)

    @pl.when(is_relay)
    def _():
        for i in range(len(RELAYED)):
            here = xs[0].at[pl.ds(RELAY_ROW + i * GMAX, GMAX), :]
            pltpu.make_async_copy(here, here, recv_sems.at[ROUNDS + i]).wait()
            forward(i).start()

    for x in xs:
        x[pl.ds(ZERO_ROW, 8), :] = jnp.zeros((8, BLK), jnp.float32)
    stacked[...] = jnp.zeros_like(stacked)
    for copy in small[2:]:
        copy.wait()

    def find(b, others):
        found = 0
        for g in range(GMAX):
            found = jnp.where(lists_s[0, urgent, g] == b, g + 1, found)
        place_s[b] = jnp.where(found > 0, found - 1, jnp.minimum(GMAX + others, BDEV - 1))
        return others + jnp.where(found > 0, 0, 1)

    lax.fori_loop(0, BDEV, find, 0)
    for c in range(BDEV, ZERO_ROW):
        place_s[c] = c

    def settle(p, b):
        row_s[p] = b
        conc[pl.ds(p, 1), :] = conc_in[pl.ds(b, 1), :]
        rate[pl.ds(p, 1), :] = rate_in[pl.ds(b, 1), :]
        xs[0][pl.ds(p, 1), :] = conc_in[pl.ds(b, 1), :]
        length = lens_s[b]
        for t in range(1, NNZB):
            index_s[p * NNZB + t] = jnp.where(t < length, place_s[cols_s[t, b]], ZERO_ROW)

    def settle_pair(g, carry):
        settle(g, lists_s[0, urgent, g])
        b = g
        for i in range(1, GMAX + 1):
            b = jnp.where(place_s[g + i] == GMAX + g, g + i, b)
        settle(GMAX + g, b)
        return carry

    lax.fori_loop(0, GMAX, settle_pair, 0)

    def choose(g, carry):
        for q in range(4):
            pick_s[q * GMAX + g] = place_s[lists_s[0, q, g]]
        return carry

    lax.fori_loop(0, GMAX, choose, 0)
    slope8[...] = rate[...] * (1.0 - 2.0 * conc[...]) + SHIFT
    pltpu.make_async_copy(blocks, blocks, block_sem).wait()
    own_part(0)
    await_ghosts(0)
    turn(0)

    lane = lax.broadcasted_iota(jnp.int32, (1, BLK), 1)
    sublane = lax.broadcasted_iota(jnp.int32, (8, BLK), 0)

    def sums_row(products, first, row):
        for e, p in enumerate(products, first):
            total = jnp.sum(jnp.sum(p, axis=0, keepdims=True), axis=1, keepdims=True)
            row = jnp.where(lane == e, total, row)
        return row

    def broadcast_gram(slot, row):
        gram_row[slot] = row
        for k in range(ndev - 1):
            pltpu.make_async_remote_copy(
                src_ref=gram_row.at[slot],
                dst_ref=arrivals.at[slot, me],
                send_sem=ar_send,
                recv_sem=ar_recv.at[slot],
                device_id=(jnp.where(me <= k, k + 1, k),),
                device_id_type=MESH,
            ).start()

    def collect_gram(slot):
        whole = arrivals.at[slot, pl.ds(0, ndev - 1)]
        with jax.named_scope(f"collect{slot}"):
            pltpu.make_async_copy(whole, whole, ar_recv.at[slot]).wait()
        arrivals[slot, me] = gram_row[slot]
        parts = [arrivals[slot, i] for i in range(ndev)]
        while len(parts) > 1:
            parts = [a + b for a, b in zip(parts[::2], parts[1::2])]
        total = parts[0]
        return {
            pair: jnp.broadcast_to(total[:, e : e + 1], (8, BLK)) for e, pair in enumerate(PAIRS)
        }

    def meet(step):
        for o in (2 << step, -(2 << step)):
            pl.semaphore_signal(known.at[step], inc=1, device_id=(near(o),), device_id_type=MESH)

    zero_row = jnp.zeros((1, BLK), jnp.float32)
    meet(0)
    substep = jnp.full((8, BLK), step_ref[0] * 0.5, jnp.float32)

    def times(c, field):
        return (field.reshape(BDEV // 8, 8, BLK) * c[None]).reshape(BDEV, BLK)

    us = None
    for r in range(1, ROUNDS):
        if r == 1:
            own_part(r)
            load_weights()
        if r <= 4:
            pl.semaphore_wait(known.at[r - 1], 2)
            meet(r)
        if r > 1:
            own_part(r)
        if r == 4:
            pl.semaphore_wait(known.at[4], 2)
            w = [ys[k] for k in range(4)]
            broadcast_gram(0, sums_row([w[i] * w[j] for i, j in PAIRS], 0, zero_row))
        if r == ROUNDS - 1:
            w = [ys[k] for k in range(6)]
            first_weights = arnoldi_weights(collect_gram(0), substep)
            d = [None] * 4
            for k in range(4):
                term = None
                if k > 0:
                    term = first_weights[k - 1] * (1.0 / SCALE)
                if k < 3:
                    low = first_weights[k] * SHIFT
                    term = -low if term is None else term - low
                d[k] = term
            d[0] = d[0] + 1.0
            us = [
                times(d[0], w[k]) + times(d[1], w[k + 1]) + times(d[2], w[k + 2]) + times(d[3], w[k + 3])
                for k in range(3)
            ]
            tail = times(d[0], w[3]) + times(d[1], w[4]) + times(d[2], w[5])
            partial = sums_row([us[i] * us[j] for i, j in PAIRS[:6]], 0, zero_row)
            for k in range(3):
                us_ref[k] = us[k]
            for p in range(BDEV):
                for k in range(3):
                    stacked[p, pl.ds(k, 1), :] = us_ref[k, pl.ds(p, 1), :]
            fold()
            kept = []
            for k in range(3):
                mine = us[k] * (tail + times(d[3], fixed[...]) * SCALE)
                kept.append(jnp.sum(mine, axis=0, keepdims=True))
            known_part = jnp.concatenate(kept + [jnp.zeros((5, BLK), jnp.float32)], axis=0)
            base = (
                conc[...]
                + times(first_weights[0], w[0])
                + times(first_weights[1], w[1])
                + times(first_weights[2], w[2])
            )
        await_ghosts(r)
        if r < ROUNDS - 1:
            turn(r)
    x = xs[ROUNDS - 1]
    parts = [None] * 8
    for p in range(BDEV):
        for t in range(1, NNZB):
            term = folded[p * NNZB + t] * x[pl.ds(index_s[p * NNZB + t], 8, stride=0), :]
            i = (p * 4 + t) % 8
            parts[i] = term if parts[i] is None else parts[i] + term
    while len(parts) > 1:
        parts = [a + b for a, b in zip(parts[::2], parts[1::2])]
    late = jnp.sum(known_part - d[3] * SCALE * parts[0], axis=1, keepdims=True)
    diagonal = lax.broadcasted_iota(jnp.int32, (8, BLK), 1) == sublane + 6
    inner = jnp.where(diagonal & (sublane < 3), late, 0.0)
    broadcast_gram(1, partial + jnp.sum(inner, axis=0, keepdims=True))
    second = arnoldi_weights(collect_gram(1), substep)
    ordered[...] = base + times(second[0], us[0]) + times(second[1], us[1]) + times(second[2], us[2])
    for b in range(BDEV):
        result[pl.ds(b, 1), :] = ordered[pl.ds(place_s[b], 1), :]
    pltpu.make_async_copy(sends, sends, send_sem).wait()

    @pl.when(is_relay)
    def _():
        pltpu.make_async_copy(relay_part, relay_part, relay_sem).wait()

    whole = arrivals.at[:, pl.ds(0, ndev - 1)]
    pltpu.make_async_copy(whole, whole, ar_send).wait()


def solution(mesh):
    ndev = mesh.shape["dom"]

    def step(conc, rate, size, blocks, cols, lens, lists):
        f32, i32 = jnp.float32, jnp.int32
        return pl.pallas_call(
            lambda *refs: kernel(ndev, *refs),
            out_shape=pltpu.VMEM((BDEV, BLK), f32),
            in_specs=[pl.BlockSpec(memory_space=pltpu.HBM)] * 2
            + [pl.BlockSpec(memory_space=pltpu.SMEM)]
            + [pl.BlockSpec(memory_space=pltpu.HBM)] * 4,
            out_specs=pl.BlockSpec(memory_space=pltpu.VMEM),
            scratch_shapes=[
                pltpu.VMEM((BDEV, BLK), f32),
                pltpu.VMEM((BDEV, BLK), f32),
                pltpu.VMEM((BDEV, BLK), f32),
                pltpu.VMEM((BDEV, BLK), f32),
                pltpu.VMEM((BDEV, BLK), f32),
                pltpu.VMEM((BDEV, BLK), f32),
                pltpu.VMEM((BDEV, NNZB, BLK, BLK), f32),
                pltpu.VMEM((ROUNDS, BDEV, BLK), f32),
                pltpu.VMEM((ROUNDS, 4, GMAX, BLK), f32),
                pltpu.VMEM((2, 1, BLK), f32),
                pltpu.VMEM((2, ndev, 1, BLK), f32),
                pltpu.VMEM((BDEV, BLK), f32),
                pltpu.SMEM((NNZB, BDEV), i32),
                pltpu.SMEM((BDEV,), i32),
                pltpu.SMEM((1, 4, GMAX), i32),
                pltpu.SMEM((BDEV * NNZB,), i32),
                pltpu.SMEM((ZERO_ROW,), i32),
                pltpu.SMEM((BDEV,), i32),
                pltpu.SMEM((4 * GMAX,), i32),
            ]
            + [
                pltpu.VMEM((BDEV, 8, BLK), f32),
                pltpu.VMEM((BDEV * NNZB, 8, BLK), f32),
                pltpu.VMEM((3, BDEV, BLK), f32),
                pltpu.VMEM((MATRIX, (NNZB - 1) * BLK, 2 * BLK), jnp.bfloat16),
            ]
            + [pltpu.VMEM((XROWS + len(RELAYED) * GMAX, BLK), f32)]
            + [pltpu.VMEM((XROWS, BLK), f32)] * (ROUNDS - 1)
            + [
                pltpu.SemaphoreType.DMA((5,)),
                pltpu.SemaphoreType.DMA,
                pltpu.SemaphoreType.DMA,
                pltpu.SemaphoreType.DMA((ROUNDS + len(RELAYED),)),
                pltpu.SemaphoreType.DMA,
                pltpu.SemaphoreType.DMA((2,)),
                pltpu.SemaphoreType.DMA,
                pltpu.SemaphoreType.REGULAR((5,)),
            ],
            compiler_params=pltpu.CompilerParams(collective_id=0, has_side_effects=True),
            name="rosenbrock",
        )(conc, rate, size, blocks, cols.T, lens, lists)

    dom = "dom"
    return jax.shard_map(
        step,
        mesh=mesh,
        in_specs=(P(dom), P(dom), P(), P(dom), P(dom), P(dom), P(dom)),
        out_specs=P(dom),
        check_vma=False,
    )
```

```python
import jax
import jax.numpy as jnp
from jax import lax
from jax.experimental import pallas as pl
from jax.experimental.pallas import tpu as pltpu
from jax.sharding import PartitionSpec as P

BLK = 128
BDEV = 32
NNZB = 5
GMAX = 16
OFFSETS = (-2, -1, 1, 2)
ORDER = (0, 3, 1, 2)
EPS = 1e-6
SHIFT = 8.0
SCALE = 0.25
ROUNDS = 7
GROUP = 8
CHUNK = 4
ZERO_ROW = BDEV + 4 * GMAX
XROWS = ZERO_ROW + 8
MATRIX = 4
RELAY_ROW = XROWS
RELAY_A = 7
RELAY_B = 103
RELAYED = ((2, 0), (1, 1), (1, 0))
PAIRS = ((0, 0), (0, 1), (0, 2), (1, 1), (1, 2), (2, 2), (0, 3), (1, 3), (2, 3))
MESH = pl.DeviceIdType.MESH


def arnoldi_weights(gram, substep):
    G = {}
    for (i, j), g in gram.items():
        G[i, j] = g
        G[j, i] = g
    zero = jnp.zeros_like(substep)
    magnitude = jnp.sqrt(G[0, 0] + EPS)
    vectors = [[1.0 / magnitude]]
    H = [[None] * 3 for _ in range(3)]
    for col in range(3):
        v = vectors[col]
        n = len(v)
        mapped = [None] * (n + 1)
        for k in range(n + 1):
            term = None
            if k > 0:
                term = v[k - 1] * (1.0 / SCALE)
            if k < n:
                low = v[k] * SHIFT
                term = -low if term is None else term - low
            mapped[k] = term
        image = []
        for i in range(n):
            total = G[i, 0] * mapped[0]
            for k in range(1, n + 1):
                total = total + G[i, k] * mapped[k]
            image.append(total)
        projections = []
        for vec in vectors:
            total = vec[0] * image[0]
            for k in range(1, len(vec)):
                total = total + vec[k] * image[k]
            projections.append(total)
        for k, p in enumerate(projections):
            H[k][col] = p
        if col < 2:
            rest = list(mapped)
            for p, vec in zip(projections, vectors):
                for k in range(len(vec)):
                    rest[k] = rest[k] - p * vec[k]
            square = None
            for i in range(n + 1):
                total = G[i, 0] * rest[0]
                for k in range(1, n + 1):
                    total = total + G[i, k] * rest[k]
                total = total * rest[i]
                square = total if square is None else square + total
            length = jnp.sqrt(square + EPS)
            H[col + 1][col] = length
            inverse = 1.0 / length
            vectors.append([r * inverse for r in rest])
    small = substep * (1.0 / 64.0)
    A = [[None if H[i][j] is None else H[i][j] * small for j in range(3)] for i in range(3)]
    sublane = lax.broadcasted_iota(jnp.int32, substep.shape, 0)
    unit = [jnp.where(sublane == i, 1.0, 0.0) for i in range(4)]
    rows = unit[:3]
    for degree in range(12, 0, -1):
        new = []
        for i in range(3):
            total = unit[3] * (1.0 / 64.0) if i == 0 else None
            for k in range(3):
                if A[i][k] is not None:
                    term = A[i][k] * rows[k]
                    total = term if total is None else total + term
            new.append(unit[i] + total * (1.0 / degree))
        rows = new

    def column(row, k):
        return jnp.broadcast_to(row[k : k + 1, :], substep.shape)

    for _ in range(6):
        rows = [
            column(row, 0) * rows[0]
            + column(row, 1) * rows[1]
            + (column(row, 2) * rows[2] + unit[3] * row)
            for row in rows
        ]
    q = [column(row, 3) for row in rows]
    out = []
    for k in range(3):
        total = None
        for col in range(k, 3):
            term = q[col] * vectors[col][k]
            total = term if total is None else total + term
        out.append(total * (substep * magnitude))
    return out


def kernel(ndev, conc_hbm, rate_hbm, step_hbm, blocks_hbm, cols_hbm, lens_hbm, lists_hbm, result, *scratch):
    (conc_in, rate_in, conc, rate, slope8, fixed, blocks, ys, sends, gram_row, arrivals, ordered) = scratch[:12]
    (step_s, cols_s, lens_s, lists_s, index_s, place_s, row_s, pick_s) = scratch[12:20]
    stacked, folded, us_ref, weights = scratch[20:24]
    xs = scratch[24 : 24 + ROUNDS]
    in_sems, block_sem, send_sem, recv_sems, ar_send, ar_recv, relay_sem, known = scratch[24 + ROUNDS :]
    me = lax.axis_index("dom")

    def near(o):
        return lax.rem(me + (o + ndev), ndev)

    my_core, my_x = lax.rem(me, 2), lax.rem(me // 2, 4)
    urgent = jnp.where(my_x < 2, 0, 3 - my_core)

    small = [
        pltpu.make_async_copy(lists_hbm, lists_s, in_sems.at[0]),
        pltpu.make_async_copy(conc_hbm, conc_in, in_sems.at[1]),
        pltpu.make_async_copy(cols_hbm, cols_s, in_sems.at[2]),
        pltpu.make_async_copy(lens_hbm, lens_s, in_sems.at[3]),
        pltpu.make_async_copy(rate_hbm, rate_in, in_sems.at[4]),
        pltpu.make_async_copy(step_hbm, step_s, in_sems.at[5]),
    ]
    for copy in small:
        copy.start()

    barrier = pltpu.get_barrier_semaphore()

    def greet(device):
        pl.semaphore_signal(barrier, inc=1, device_id=(device,), device_id_type=MESH)

    @pl.when(me == RELAY_A)
    def _():
        greet(0)
        greet(1)

    @pl.when(me == RELAY_B)
    def _():
        greet(RELAY_A)

    for q in ORDER:
        greet(jnp.where(me + OFFSETS[q] >= ndev, RELAY_B, near(OFFSETS[q])))

    greetings = (
        4
        + jnp.where(me == RELAY_B, 3, 0)
        + jnp.where(me == RELAY_A, 1, 0)
        - jnp.where(me == 0, 1, 0)
    )

    for c in range(BDEV // CHUNK):
        part = pl.ds(c * CHUNK, CHUNK)
        pltpu.make_async_copy(blocks_hbm.at[part], blocks.at[part], block_sem).start()

    def packet(r, q, source):
        offset = jnp.where(q < 2, q - 2, q - 1)
        return pltpu.make_async_remote_copy(
            src_ref=source,
            dst_ref=xs[r].at[pl.ds(pl.multiple_of(BDEV + q * GMAX, 8), GMAX), :],
            send_sem=send_sem,
            recv_sem=recv_sems.at[r % 2],
            device_id=(lax.rem(me + offset + ndev, ndev),),
            device_id_type=MESH,
        )

    def await_ghosts(r):
        part = xs[r].at[pl.ds(BDEV, 4 * GMAX), :]
        pltpu.make_async_copy(part, part, recv_sems.at[r % 2]).wait()

    def lane_sums(total):
        return jnp.sum(total.T, axis=0, keepdims=True)

    def own_part(r):
        source = conc if r == 0 else ys.at[r - 1]

        def group(i, carry):
            for s in range(GROUP):
                p = i * GROUP + s
                mine = source[pl.ds(p, 1), :]
                here = lane_sums(blocks[row_s[p], 0] * mine)
                if r == 0:
                    kept = rate[pl.ds(p, 1), :] * mine * (1.0 - mine)
                else:
                    kept = slope8[pl.ds(p, 1), :] * mine
                fixed[pl.ds(p, 1), :] = kept - here
            return carry

        lax.fori_loop(0, BDEV // GROUP, group, 0)

    def split(value):
        high = value.astype(jnp.bfloat16)
        return high, (value - high.astype(jnp.float32)).astype(jnp.bfloat16)

    def load_weights():
        def one(m, carry):
            b = row_s[GMAX - MATRIX + m]
            for t in range(1, NNZB):
                weights[m, pl.ds((t - 1) * BLK, BLK), :] = jnp.concatenate(split(blocks[b, t].T), axis=1)
            return carry

        lax.fori_loop(0, MATRIX, one, 0)

    def keep(r, p, whole):
        ys[r, pl.ds(p, 1), :] = whole
        if r + 1 < ROUNDS:
            xs[r + 1][pl.ds(p, 1), :] = whole

    def matrix_product(r):
        x = xs[r]
        for m in range(MATRIX):
            p = GMAX - MATRIX + m
            wide = jnp.concatenate(
                [x[pl.ds(index_s[p * NNZB + t], 8, stride=0), :] for t in range(1, NNZB)], axis=1
            )
            both = jnp.dot(
                jnp.concatenate(split(wide), axis=0), weights[m], preferred_element_type=jnp.float32
            )
            row = both[:1, :BLK] + both[:1, BLK:] + (both[8:9, :BLK] + both[8:9, BLK:])
            keep(r, p, (fixed[pl.ds(p, 1), :] - row) * SCALE)

    def product(r, low, high):
        x = xs[r]
        for p in range(low, high):
            total = None
            b = row_s[p]
            for t in range(1, NNZB):
                row = x[pl.ds(index_s[p * NNZB + t], 8, stride=0), :]
                term = blocks[b, t].reshape(16, 8, BLK) * row[None]
                total = term if total is None else total + term
            whole = fixed[pl.ds(p, 1), :] - lane_sums(total.reshape(BLK, BLK))
            whole = whole if r == 0 else whole * SCALE
            keep(r, p, whole)

    def fold():
        def group(i, carry):
            for s in range(GROUP):
                p = i * GROUP + s
                left = jnp.concatenate(split(stacked[p]), axis=0)
                for t in range(1, NNZB):
                    right = jnp.concatenate(split(blocks[row_s[p], t]), axis=1)
                    both = jnp.dot(left, right, preferred_element_type=jnp.float32)
                    folded[p * NNZB + t] = (
                        both[:8, :BLK] + both[:8, BLK:] + (both[8:, :BLK] + both[8:, BLK:])
                    )
            return carry

        lax.fori_loop(0, BDEV // GROUP, group, 0)

    def turn(r):
        if r == 0:
            product(r, 0, GMAX)
        else:
            matrix_product(r)
            product(r, 0, GMAX - MATRIX)
        n = r + 1
        if n < ROUNDS:
            packet(n, urgent, ys.at[r, pl.ds(0, GMAX), :]).start()
        product(r, GMAX, BDEV)
        if n < ROUNDS:
            for k in range(1, 4):
                q = lax.rem(urgent + k, 4)
                for g in range(GMAX):
                    sends[n, k, pl.ds(g, 1), :] = ys[r, pl.ds(pick_s[q * GMAX + g], 1), :]
                packet(n, q, sends.at[n, k]).start()

    small[0].wait()
    small[1].wait()
    for q in ORDER:
        for g in range(GMAX):
            sends[0, q, pl.ds(g, 1), :] = conc_in[pl.ds(lists_s[0, q, g], 1), :]
    pl.semaphore_wait(barrier, greetings)
    for q in ORDER:
        relayed = me + OFFSETS[q] < 0
        slot = q + 2 * me
        pltpu.make_async_remote_copy(
            src_ref=sends.at[0, q],
            dst_ref=xs[0].at[
                pl.ds(
                    pl.multiple_of(
                        jnp.where(relayed, RELAY_ROW + slot * GMAX, BDEV + q * GMAX), 8
                    ),
                    GMAX,
                ),
                :,
            ],
            send_sem=send_sem,
            recv_sem=recv_sems.at[jnp.where(relayed, 2 + slot, 0)],
            device_id=(jnp.where(relayed, RELAY_A, near(OFFSETS[q])),),
            device_id_type=MESH,
        ).start()

    def forward(i):
        before_end, q = RELAYED[i]
        first = me == RELAY_A
        here = xs[0].at[pl.ds(RELAY_ROW + i * GMAX, GMAX), :]
        row = jnp.where(first, RELAY_ROW + i * GMAX, BDEV + q * GMAX)
        return pltpu.make_async_remote_copy(
            src_ref=here,
            dst_ref=xs[0].at[pl.ds(pl.multiple_of(row, 8), GMAX), :],
            send_sem=relay_sem,
            recv_sem=recv_sems.at[jnp.where(first, 2 + i, 0)],
            device_id=(jnp.where(first, RELAY_B, ndev - before_end),),
            device_id_type=MESH,
        )

    relay_part = xs[0].at[pl.ds(RELAY_ROW, len(RELAYED) * GMAX), :]
    is_relay = (me == RELAY_A) | (me == RELAY_B)

    @pl.when(is_relay)
    def _():
        for i in range(len(RELAYED)):
            here = xs[0].at[pl.ds(RELAY_ROW + i * GMAX, GMAX), :]
            pltpu.make_async_copy(here, here, recv_sems.at[2 + i]).wait()
            forward(i).start()

    for x in xs:
        x[pl.ds(ZERO_ROW, 8), :] = jnp.zeros((8, BLK), jnp.float32)
    stacked[...] = jnp.zeros_like(stacked)
    for copy in small[2:]:
        copy.wait()

    def find(b, others):
        found = 0
        for g in range(GMAX):
            found = jnp.where(lists_s[0, urgent, g] == b, g + 1, found)
        place_s[b] = jnp.where(found > 0, found - 1, jnp.minimum(GMAX + others, BDEV - 1))
        return others + jnp.where(found > 0, 0, 1)

    lax.fori_loop(0, BDEV, find, 0)
    for c in range(BDEV, ZERO_ROW):
        place_s[c] = c

    def settle(p, b):
        row_s[p] = b
        conc[pl.ds(p, 1), :] = conc_in[pl.ds(b, 1), :]
        rate[pl.ds(p, 1), :] = rate_in[pl.ds(b, 1), :]
        xs[0][pl.ds(p, 1), :] = conc_in[pl.ds(b, 1), :]
        length = lens_s[b]
        for t in range(1, NNZB):
            index_s[p * NNZB + t] = jnp.where(t < length, place_s[cols_s[t, b]], ZERO_ROW)

    def settle_pair(g, carry):
        settle(g, lists_s[0, urgent, g])
        b = g
        for i in range(1, GMAX + 1):
            b = jnp.where(place_s[g + i] == GMAX + g, g + i, b)
        settle(GMAX + g, b)
        return carry

    lax.fori_loop(0, GMAX, settle_pair, 0)

    def choose(g, carry):
        for q in range(4):
            pick_s[q * GMAX + g] = place_s[lists_s[0, q, g]]
        return carry

    lax.fori_loop(0, GMAX, choose, 0)
    slope8[...] = rate[...] * (1.0 - 2.0 * conc[...]) + SHIFT
    pltpu.make_async_copy(blocks, blocks, block_sem).wait()
    own_part(0)
    await_ghosts(0)
    turn(0)

    lane = lax.broadcasted_iota(jnp.int32, (1, BLK), 1)
    sublane = lax.broadcasted_iota(jnp.int32, (8, BLK), 0)

    def sums_row(products, first, row):
        for e, p in enumerate(products, first):
            total = jnp.sum(jnp.sum(p, axis=0, keepdims=True), axis=1, keepdims=True)
            row = jnp.where(lane == e, total, row)
        return row

    def broadcast_gram(slot, row):
        gram_row[slot] = row
        for k in range(ndev - 1):
            pltpu.make_async_remote_copy(
                src_ref=gram_row.at[slot],
                dst_ref=arrivals.at[slot, me],
                send_sem=ar_send,
                recv_sem=ar_recv.at[slot],
                device_id=(jnp.where(me <= k, k + 1, k),),
                device_id_type=MESH,
            ).start()

    def collect_gram(slot):
        whole = arrivals.at[slot, pl.ds(0, ndev - 1)]
        with jax.named_scope(f"collect{slot}"):
            pltpu.make_async_copy(whole, whole, ar_recv.at[slot]).wait()
        arrivals[slot, me] = gram_row[slot]
        parts = [arrivals[slot, i] for i in range(ndev)]
        while len(parts) > 1:
            parts = [a + b for a, b in zip(parts[::2], parts[1::2])]
        total = parts[0]
        return {
            pair: jnp.broadcast_to(total[:, e : e + 1], (8, BLK)) for e, pair in enumerate(PAIRS)
        }

    def meet(step):
        for o in (2 << step, -(2 << step)):
            pl.semaphore_signal(known.at[step], inc=1, device_id=(near(o),), device_id_type=MESH)

    zero_row = jnp.zeros((1, BLK), jnp.float32)
    meet(0)
    substep = jnp.full((8, BLK), step_s[0] * 0.5, jnp.float32)

    def times(c, field):
        return (field.reshape(BDEV // 8, 8, BLK) * c[None]).reshape(BDEV, BLK)

    us = None
    for r in range(1, ROUNDS):
        if r == 1:
            own_part(r)
            load_weights()
        if r <= 4:
            pl.semaphore_wait(known.at[r - 1], 2)
            meet(r)
        if r > 1:
            own_part(r)
        if r == 4:
            pl.semaphore_wait(known.at[4], 2)
            w = [ys[k] for k in range(4)]
            broadcast_gram(0, sums_row([w[i] * w[j] for i, j in PAIRS], 0, zero_row))
        if r == ROUNDS - 1:
            w = [ys[k] for k in range(6)]
            first_weights = arnoldi_weights(collect_gram(0), substep)
            d = [None] * 4
            for k in range(4):
                term = None
                if k > 0:
                    term = first_weights[k - 1] * (1.0 / SCALE)
                if k < 3:
                    low = first_weights[k] * SHIFT
                    term = -low if term is None else term - low
                d[k] = term
            d[0] = d[0] + 1.0
            us = [
                times(d[0], w[k]) + times(d[1], w[k + 1]) + times(d[2], w[k + 2]) + times(d[3], w[k + 3])
                for k in range(3)
            ]
            tail = times(d[0], w[3]) + times(d[1], w[4]) + times(d[2], w[5])
            partial = sums_row([us[i] * us[j] for i, j in PAIRS[:6]], 0, zero_row)
            for k in range(3):
                us_ref[k] = us[k]
            for p in range(BDEV):
                for k in range(3):
                    stacked[p, pl.ds(k, 1), :] = us_ref[k, pl.ds(p, 1), :]
            fold()
            kept = []
            for k in range(3):
                mine = us[k] * (tail + times(d[3], fixed[...]) * SCALE)
                kept.append(jnp.sum(mine, axis=0, keepdims=True))
            known_part = jnp.concatenate(kept + [jnp.zeros((5, BLK), jnp.float32)], axis=0)
            base = (
                conc[...]
                + times(first_weights[0], w[0])
                + times(first_weights[1], w[1])
                + times(first_weights[2], w[2])
            )
        await_ghosts(r)
        if r < ROUNDS - 1:
            turn(r)
    x = xs[ROUNDS - 1]
    parts = [None] * 8
    for p in range(BDEV):
        for t in range(1, NNZB):
            term = folded[p * NNZB + t] * x[pl.ds(index_s[p * NNZB + t], 8, stride=0), :]
            i = (p * 4 + t) % 8
            parts[i] = term if parts[i] is None else parts[i] + term
    while len(parts) > 1:
        parts = [a + b for a, b in zip(parts[::2], parts[1::2])]
    late = jnp.sum(known_part - d[3] * SCALE * parts[0], axis=1, keepdims=True)
    diagonal = lax.broadcasted_iota(jnp.int32, (8, BLK), 1) == sublane + 6
    inner = jnp.where(diagonal & (sublane < 3), late, 0.0)
    broadcast_gram(1, partial + jnp.sum(inner, axis=0, keepdims=True))
    second = arnoldi_weights(collect_gram(1), substep)
    ordered[...] = base + times(second[0], us[0]) + times(second[1], us[1]) + times(second[2], us[2])
    for b in range(BDEV):
        result[pl.ds(b, 1), :] = ordered[pl.ds(place_s[b], 1), :]
    pltpu.make_async_copy(sends, sends, send_sem).wait()

    @pl.when(is_relay)
    def _():
        pltpu.make_async_copy(relay_part, relay_part, relay_sem).wait()

    whole = arrivals.at[:, pl.ds(0, ndev - 1)]
    pltpu.make_async_copy(whole, whole, ar_send).wait()


def solution(mesh):
    ndev = mesh.shape["dom"]

    def step(conc, rate, size, blocks, cols, lens, lists):
        f32, i32 = jnp.float32, jnp.int32
        return pl.pallas_call(
            lambda *refs: kernel(ndev, *refs),
            out_shape=pltpu.VMEM((BDEV, BLK), f32),
            in_specs=[pl.BlockSpec(memory_space=pltpu.HBM)] * 7,
            out_specs=pl.BlockSpec(memory_space=pltpu.VMEM),
            scratch_shapes=[
                pltpu.VMEM((BDEV, BLK), f32),
                pltpu.VMEM((BDEV, BLK), f32),
                pltpu.VMEM((BDEV, BLK), f32),
                pltpu.VMEM((BDEV, BLK), f32),
                pltpu.VMEM((BDEV, BLK), f32),
                pltpu.VMEM((BDEV, BLK), f32),
                pltpu.VMEM((BDEV, NNZB, BLK, BLK), f32),
                pltpu.VMEM((ROUNDS, BDEV, BLK), f32),
                pltpu.VMEM((ROUNDS, 4, GMAX, BLK), f32),
                pltpu.VMEM((2, 1, BLK), f32),
                pltpu.VMEM((2, ndev, 1, BLK), f32),
                pltpu.VMEM((BDEV, BLK), f32),
                pltpu.SMEM((1,), f32),
                pltpu.SMEM((NNZB, BDEV), i32),
                pltpu.SMEM((BDEV,), i32),
                pltpu.SMEM((1, 4, GMAX), i32),
                pltpu.SMEM((BDEV * NNZB,), i32),
                pltpu.SMEM((ZERO_ROW,), i32),
                pltpu.SMEM((BDEV,), i32),
                pltpu.SMEM((4 * GMAX,), i32),
            ]
            + [
                pltpu.VMEM((BDEV, 8, BLK), f32),
                pltpu.VMEM((BDEV * NNZB, 8, BLK), f32),
                pltpu.VMEM((3, BDEV, BLK), f32),
                pltpu.VMEM((MATRIX, (NNZB - 1) * BLK, 2 * BLK), jnp.bfloat16),
            ]
            + [pltpu.VMEM((XROWS + len(RELAYED) * GMAX, BLK), f32)]
            + [pltpu.VMEM((XROWS, BLK), f32)] * (ROUNDS - 1)
            + [
                pltpu.SemaphoreType.DMA((6,)),
                pltpu.SemaphoreType.DMA,
                pltpu.SemaphoreType.DMA,
                pltpu.SemaphoreType.DMA((2 + len(RELAYED),)),
                pltpu.SemaphoreType.DMA,
                pltpu.SemaphoreType.DMA((2,)),
                pltpu.SemaphoreType.DMA,
                pltpu.SemaphoreType.REGULAR((5,)),
            ],
            compiler_params=pltpu.CompilerParams(collective_id=0, has_side_effects=True),
            name="rosenbrock",
        )(conc, rate, size, blocks, cols.T, lens, lists)

    dom = "dom"
    return jax.shard_map(
        step,
        mesh=mesh,
        in_specs=(P(dom), P(dom), P(), P(dom), P(dom), P(dom), P(dom)),
        out_specs=P(dom),
        check_vma=False,
    )
```
